32 devices in a mesh: grp: 4 (over y, x), tile: 8 (over z, core).
Axes of the slice: x: 2, y: 2, z: 4, core: 2. Of those that a mesh axis runs over, the one named last changes fastest.
Arguments:
- base_rhs: float32 [1024, 4096], P('grp', 'tile'), may hold values from -6 to 6
- depth: float32 [1024, 4096], P('grp', 'tile'), may hold values from 0.25 to 2
- ssh_prev: float32 [1024, 4096], P('grp', 'tile'), may hold values from -6 to 6
- currents: float32 [2, 1024, 4096], P(None, 'grp', 'tile'), may hold values from -3 to 3
- land_blocks: int32 [128, 512], P('grp', 'tile'), may hold values 0 or 1
- ice_thick: float32 [2, 256, 4096], P(None, 'grp', 'tile'), may hold values from 0.25 to 4
- ice_blocks: int32 [2, 32, 512], P(None, 'grp', 'tile'), may hold values 0 or 1
- ice_vel: float32 [2, 2, 256, 4096], P(None, None, 'grp', 'tile'), may hold values from -3 to 3
- ice_stress: float32 [3, 2, 256, 4096], P(None, None, 'grp', 'tile'), may hold values from -5 to 5
- wind: float32 [2, 2, 256, 4096], P(None, None, 'grp', 'tile'), may hold values from -6 to 6
Outputs:
- ssh: float32 [1024, 4096], P('grp', 'tile')
- ice_vel_out: float32 [2, 2, 256, 4096], P(None, None, 'grp', 'tile')
- ice_stress_out: float32 [3, 2, 256, 4096], P(None, None, 'grp', 'tile')
The draws below stay inside these ranges and needn't reach their ends.
All inputs are finite; a program needn't handle non-finite values. No bound on the sum of `land_blocks` or of `ice_blocks` on one device may be relied on, other than what follows from the above.
Results may differ from the reference program's by a relative error of at most 0.0001.
Values sent between devices are 32-bit elements; how exact they have to be, the bound alone decides.
No kernel may reach another device: no remote copies, remote signals or barrier semaphores. Data moves between devices by JAX's collectives and lax.ppermute only.
A program may use at most 64 MiB of HBM per device.

```python
import math
import jax
import jax.numpy as jnp

BS = 8
NSUB = 8
ITERS = 3
NX = 1024
NY = 4096
NXI = 256


def set_ends(values, own_key, least, largest):
    index_at = [jax.random.randint(jax.random.fold_in(own_key, axis), (), 0, length) for axis, length in enumerate(values.shape)]
    widest = values.shape.index(max(values.shape))
    beside = index_at[:widest] + [(index_at[widest] + 1) % values.shape[widest]] + index_at[widest + 1:]
    return values.at[tuple(index_at)].set(least).at[tuple(beside)].set(largest)


def level_of(key, extent, split, smallest, high):
    loudness = 1.0
    for position, shards_of in split:
        heights = jax.random.uniform(jax.random.fold_in(jax.random.fold_in(key, 6), position), (shards_of,), jnp.float32, smallest / len(split), high / len(split))
        loudness = loudness * jnp.repeat(jnp.exp(heights), extent[position] // shards_of).reshape((-1,) + (1,) * (len(extent) - 1 - position))
    return loudness


def bell_draw(rng, dims, scale, reach, pieces=(), held_as=jnp.bfloat16):
    level = level_of(rng, dims, pieces, -0.22, 0.18) if pieces else 1.0
    entries = jax.random.normal(rng, dims, jnp.float32) * scale * level
    return jnp.minimum(jnp.maximum(entries, -reach), reach).astype(held_as)


def setup_inputs(seed: int = 0) -> dict:
    key_list = jax.random.split(jax.random.key(seed), 11)
    base_rhs = bell_draw(key_list[0], (NX, NY), 1.0, 6.0, ((0, 4), (1, 8)), jnp.float32)
    depth = jnp.clip(jnp.exp(math.log(2.0) - 2.0794415 * jax.random.uniform(key_list[1], (NX, NY), jnp.float32) ** level_of(key_list[1], (NX, NY), ((0, 4), (1, 8)), -0.2, 0.2)), 0.25, 2.0)
    ssh_prev = bell_draw(key_list[2], (NX, NY), 1.0, 6.0, ((0, 4), (1, 8)), jnp.float32)
    currents = bell_draw(key_list[3], (2, NX, NY), 0.5, 3.0, ((1, 4), (2, 8)), jnp.float32)
    land_blocks = set_ends((jax.random.randint(key_list[4], (NX // BS, NY // BS), 0, 4) < 3).astype(jnp.int32), jax.random.fold_in(key_list[4], 1), 0, 1)
    ice_thick = jnp.clip(jnp.exp(math.log(4.0) - 2.7725887 * jax.random.uniform(key_list[5], (2, NXI, NY), jnp.float32) ** level_of(key_list[5], (2, NXI, NY), ((1, 4), (2, 8)), -0.2, 0.2)), 0.25, 4.0)
    ice_blocks = set_ends((jax.random.randint(key_list[6], (2, NXI // BS, NY // BS), 0, 4) < 3).astype(jnp.int32), jax.random.fold_in(key_list[6], 1), 0, 1)
    ice_vel = bell_draw(key_list[7], (2, 2, NXI, NY), 0.5, 3.0, ((2, 4), (3, 8)), jnp.float32)
    ice_stress = bell_draw(key_list[8], (3, 2, NXI, NY), 1.0, 5.0, ((2, 4), (3, 8)), jnp.float32)
    wind = bell_draw(key_list[9], (2, 2, NXI, NY), 1.0, 6.0, ((2, 4), (3, 8)), jnp.float32)
    return dict(base_rhs=base_rhs, depth=depth, ssh_prev=ssh_prev, currents=currents, land_blocks=land_blocks, ice_thick=ice_thick, ice_blocks=ice_blocks, ice_vel=ice_vel, ice_stress=ice_stress, wind=wind)


DAMP = 0.05
RELAX = 0.2
STRENGTH = 0.5
DRAG = 1.0
STEP = 0.5

def strain_rates(u_pad, v_pad):
    du_dx = u_pad[..., 1:, :-1] - u_pad[..., :-1, :-1]
    du_dy = u_pad[..., :-1, 1:] - u_pad[..., :-1, :-1]
    dv_dx = v_pad[..., 1:, :-1] - v_pad[..., :-1, :-1]
    dv_dy = v_pad[..., :-1, 1:] - v_pad[..., :-1, :-1]
    return (du_dx + dv_dy, du_dx - dv_dy, du_dy + dv_dx)

def relax_stress(previous, strength, div_rate, tens_rate, shear_rate):
    deformation = jnp.sqrt(div_rate * div_rate + tens_rate * tens_rate + shear_rate * shear_rate + 1.0)
    relax_scale = 1.0 / (1.0 + RELAX)
    div_part = (previous[0] + RELAX * strength * (div_rate / deformation - 1.0)) * relax_scale
    tens_part = (previous[1] + RELAX * strength * tens_rate / deformation) * relax_scale
    shear_part = (previous[2] + RELAX * strength * shear_rate / deformation) * relax_scale
    return jnp.stack([div_part, tens_part, shear_part])

def along_rows(field):
    return field[..., 1:, 1:] - field[..., :-1, 1:]

def along_cols(field):
    return field[..., 1:, 1:] - field[..., 1:, :-1]

def stress_force(stress_pad):
    force_x = 0.5 * along_rows(stress_pad[0] + stress_pad[1]) + along_cols(stress_pad[2])
    force_y = 0.5 * along_cols(stress_pad[0] - stress_pad[1]) + along_rows(stress_pad[2])
    return jnp.stack([force_x, force_y])

def momentum(velocity, force, ice_mass, ice_cover, wind, ocean_flow):
    return ice_cover * (ice_mass * velocity + STEP * (force + wind + DRAG * ocean_flow)) / (ice_mass + STEP * DRAG)

def face_weights(depth_pad):
    centre = depth_pad[1:-1, 1:-1]
    return (centre * depth_pad[2:, 1:-1], centre * depth_pad[:-2, 1:-1], centre * depth_pad[1:-1, 2:], centre * depth_pad[1:-1, :-2])

def apply_operator(field_pad, weights):
    field = field_pad[1:-1, 1:-1]
    north_weight, south_weight, east_weight, west_weight = weights
    return DAMP * field + north_weight * (field - field_pad[2:, 1:-1]) + south_weight * (field - field_pad[:-2, 1:-1]) + east_weight * (field - field_pad[1:-1, 2:]) + west_weight * (field - field_pad[1:-1, :-2])

def expand(blocks):
    return jnp.repeat(jnp.repeat(blocks, BS, axis=-2), BS, axis=-1).astype(jnp.float32)

def reference(base_rhs, depth, ssh_prev, currents, land_blocks, ice_thick, ice_blocks, ice_vel, ice_stress, wind):
    wet_cells = expand(land_blocks)
    ice_cover = expand(ice_blocks)
    strength = STRENGTH * ice_thick * ice_cover
    ice_mass = ice_thick * ice_cover + 1.0
    ocean_flow = jnp.stack([currents[:, :NXI], currents[:, NX - NXI:]], axis=1)
    velocity = ice_vel
    stress = ice_stress
    for subcycle in range(NSUB):
        vel_pad = jnp.pad(velocity, ((0, 0), (0, 0), (1, 1), (1, 1)))
        strain = strain_rates(vel_pad[0], vel_pad[1])
        div_rate = strain[0][:, 1:, 1:]
        tens_rate = strain[1][:, 1:, 1:]
        shear_rate = strain[2][:, 1:, 1:]
        stress = relax_stress(stress, strength, div_rate, tens_rate, shear_rate)
        stress_pad = jnp.pad(stress, ((0, 0), (0, 0), (1, 0), (1, 0)))
        velocity = momentum(velocity, stress_force(stress_pad), ice_mass, ice_cover, wind, ocean_flow)
    ice_drag = DRAG * ice_cover * (velocity - ocean_flow)
    ocean_drag = jnp.zeros((2, NX, NY), jnp.float32)
    ocean_drag = ocean_drag.at[:, :NXI].set(ice_drag[:, 0]).at[:, NX - NXI:].set(ice_drag[:, 1])
    forcing_pad = jnp.pad(jnp.stack([ocean_drag[0], ocean_drag[1], depth * wet_cells]), ((0, 0), (1, 1), (1, 1)))
    spread = forcing_pad[0, 1:-1, 1:-1] - forcing_pad[0, :-2, 1:-1] + (forcing_pad[1, 1:-1, 1:-1] - forcing_pad[1, 1:-1, :-2])
    forcing = wet_cells * (base_rhs + spread)
    weights = face_weights(forcing_pad[2])
    diagonal = DAMP + weights[0] + weights[1] + weights[2] + weights[3]
    solution = ssh_prev
    residual = forcing - apply_operator(jnp.pad(solution, 1), weights)
    precond = residual / diagonal
    direction = precond
    precond_norm = jnp.sum(residual * precond)
    for iteration in range(ITERS):
        applied = apply_operator(jnp.pad(direction, 1), weights)
        step_size = precond_norm / jnp.sum(direction * applied)
        solution = solution + step_size * direction
        residual = residual - step_size * applied
        precond = residual / diagonal
        norm_next = jnp.sum(residual * precond)
        direction = precond + norm_next / precond_norm * direction
        precond_norm = norm_next
    return (solution, velocity, stress)
```

```python
import functools

import jax
import jax.numpy as jnp
from jax import lax
from jax.experimental import pallas as pl
from jax.experimental.pallas import tpu as pltpu
from jax.sharding import PartitionSpec as P

BS = 8
NSUB = 8
ITERS = 3

DAMP = 0.05
RELAX = 0.2
STRENGTH = 0.5
DRAG = 1.0
STEP = 0.5

F32 = jnp.float32
SUB = 8
LANES = 128
EDGE = 16
SLOTS = LANES // EDGE
NICE = 8
NEXT = NICE + 2
NOC = 3


def vmem():
    return pl.BlockSpec(memory_space=pltpu.VMEM)


def smem():
    return pl.BlockSpec(memory_space=pltpu.SMEM)


def call(body, name, outs, ins, scratch=(), mib=24, flops=1000000):
    shapes = tuple(jax.ShapeDtypeStruct(s, F32) for s in outs)
    specs = [smem() if i == 0 else vmem() for i in range(len(ins))]
    return pl.pallas_call(
        body,
        name=name,
        out_shape=shapes,
        in_specs=specs,
        out_specs=tuple(vmem() for _ in outs),
        scratch_shapes=[pltpu.VMEM(s, F32) for s in scratch],
        cost_estimate=pl.CostEstimate(flops=flops, bytes_accessed=4000000, transcendentals=0),
        compiler_params=pltpu.CompilerParams(vmem_limit_bytes=mib * 1024 * 1024),
    )(*ins)


def tile(k):
    return slice(k * SUB, k * SUB + SUB)


def expanded_cols(blocks):
    count = blocks.shape[-1]
    row = lax.broadcasted_iota(jnp.int32, (count, count * BS), 0) * BS
    col = lax.broadcasted_iota(jnp.int32, (count, count * BS), 1)
    spread = ((col >= row) & (col < row + BS)).astype(F32)
    return jnp.dot(blocks.astype(F32), spread, preferred_element_type=F32)


def row_iota(cols):
    return lax.broadcasted_iota(jnp.int32, (SUB, cols), 0)


def lane_iota():
    return lax.broadcasted_iota(jnp.int32, (SUB, LANES), 1)


def from_next_row(here, after, row):
    return pltpu.roll(jnp.where(row == 0, after, here), SUB - 1, 0)


def from_prev_row(here, before, row):
    return pltpu.roll(jnp.where(row == SUB - 1, before, here), 1, 0)


def from_next_col(here):
    return pltpu.roll(here, here.shape[1] - 1, 1)


def from_prev_col(here):
    return pltpu.roll(here, 1, 1)


def own_tile(cur, comp, first, j):
    last = cur.shape[1] // SUB - 1
    t = jnp.clip(first + j, 0, last)
    return cur[comp, pl.ds(pl.multiple_of(t * SUB, SUB), SUB), :]


def pack_rows(groups, g_ref, base, depth, x0, cur, land, thick, iceb, vel, stress, wind,
              gf, h, a, b, c, d):
    g = g_ref[0]
    rows, ice_rows = base.shape[0], thick.shape[1]
    slab_tiles = ice_rows // SUB
    wet = expanded_cols(land[...])
    for k in range(rows // SUB):
        gf[tile(k), :] = depth[tile(k), :] * wet[k : k + 1, :]
    for cap in range(2):
        cover = expanded_cols(iceb[cap])
        for k in range(slab_tiles):
            h[cap, tile(k), :] = thick[cap, tile(k), :] * cover[k : k + 1, :]

    def halo(out, last):
        r = slice(ice_rows - SUB, ice_rows) if last else slice(0, SUB)
        ro = slice(rows - SUB, rows) if last else slice(0, SUB)
        n = 0
        for cap in range(2):
            pieces = [h[cap, r, :], vel[0, cap, r, :], vel[1, cap, r, :]]
            pieces += [stress[i, cap, r, :] for i in range(3)]
            pieces += [wind[i, cap, r, :] for i in range(2)]
            for piece in pieces:
                out[tile(n), :] = piece
                n += 1
        for field in (base, gf, x0):
            out[tile(n), :] = field[ro, :]
            n += 1
        for k in range(n, out.shape[0] // SUB):
            out[tile(k), :] = jnp.zeros((SUB, out.shape[1]), F32)

    def slab(out, dest):
        for comp in range(2):
            for j in range(slab_tiles + 2):
                out[tile(comp * (slab_tiles + 2) + j), :] = own_tile(cur, comp, slab_tiles * dest - 1, j)

    @pl.when((g == 0) | (g == 3))
    def _():
        slab(a, g ^ 1)
        slab(b, g ^ 2)
        slab(c, g ^ 3)

    @pl.when(g == 0)
    def _():
        halo(d, True)

    @pl.when(g == 3)
    def _():
        halo(d, False)

    @pl.when(g == 1)
    def _():
        halo(a, False)
        halo(c, True)

    @pl.when(g == 2)
    def _():
        halo(a, True)
        halo(c, False)


def pack_cols(g_ref, ra, rb, rc, rd, cur, h, vel, stress, wind, base, gf, x0, ice, ocean, left, right):
    g = g_ref[0]
    cols = base.shape[1]
    slab_tiles = h.shape[1] // SUB
    ext = slab_tiles + 2
    rows = base.shape[0] // SUB
    lane = lane_iota()
    zero = jnp.zeros((SUB, cols), F32)
    state = {"n": 0, "l": None, "r": None}

    def emit(value):
        n = state["n"]
        s = n % SLOTS
        first, last = value[:, :LANES], value[:, cols - LANES :]
        first = pltpu.roll(first, EDGE * s, 1) if s else first
        shift = EDGE * (s + 1) % LANES
        last = pltpu.roll(last, shift, 1) if shift else last
        if s == 0:
            state["l"], state["r"] = first, last
        else:
            state["l"] = jnp.where(lane >= EDGE * s, first, state["l"])
            state["r"] = jnp.where(lane >= EDGE * s, last, state["r"])
        if s == SLOTS - 1:
            k = n // SLOTS
            left[tile(k), :] = state["l"]
            right[tile(k), :] = state["r"]
        state["n"] = n + 1

    def low(k):
        r = tile(k)
        return jnp.where(g == 1, rd[r, :], jnp.where(g == 2, rc[r, :], jnp.where(g == 3, ra[r, :], zero)))

    def high(k):
        r = tile(k)
        return jnp.where(g == 0, ra[r, :], jnp.where(g == 1, rc[r, :], jnp.where(g == 2, rd[r, :], zero)))

    for cap in range(2):
        own = [h.at[cap], vel.at[0, cap], vel.at[1, cap], stress.at[0, cap], stress.at[1, cap],
               stress.at[2, cap], wind.at[0, cap], wind.at[1, cap]]
        for f in range(NICE):
            for j in range(ext):
                if j == 0:
                    value = low(cap * NICE + f)
                elif j == ext - 1:
                    value = high(cap * NICE + f)
                else:
                    value = own[f][tile(j - 1), :]
                ice[cap, f, tile(j), :] = value
                emit(value)
        for comp in range(2):
            for j in range(ext):
                r = tile(comp * ext + j)
                mine = own_tile(cur, comp, slab_tiles * g - 1, j)
                if cap == 0:
                    value = jnp.where(g == 0, mine, jnp.where(g == 1, ra[r, :], jnp.where(g == 2, rb[r, :], rc[r, :])))
                else:
                    value = jnp.where(g == 3, mine, jnp.where(g == 2, ra[r, :], jnp.where(g == 1, rb[r, :], rc[r, :])))
                ice[cap, NICE + comp, tile(j), :] = value
                emit(value)
    for i, field in enumerate((base, gf, x0)):
        for j in range(rows + 2):
            if j == 0:
                value = low(2 * NICE + i)
            elif j == rows + 1:
                value = high(2 * NICE + i)
            else:
                value = field[tile(j - 1), :]
            ocean[i, tile(j), :] = value
            emit(value)
    while state["n"] % SLOTS:
        emit(zero)


def widened(value, from_left, from_right, n, lane):
    s = n % SLOTS
    k = n // SLOTS
    after, before = from_right[tile(k), :], from_left[tile(k), :]
    after = pltpu.roll(after, LANES - EDGE * s, 1) if s else after
    shift = (LANES - EDGE * (s + 1)) % LANES
    before = pltpu.roll(before, shift, 1) if shift else before
    outer = jnp.where(lane < EDGE, after, jnp.where(lane >= LANES - EDGE, before, 0.0))
    return jnp.concatenate([value, outer], axis=1)


def ice_steps(g_ref, ice, from_left, from_right, vel_out, stress_out, p1, p2, p3, mine,
              u_s, v_s, s0_s, s1_s, s2_s, a_s, m_s, q_s, fx_s, fy_s, f0_s, f1_s):
    g = g_ref[0]
    cols = ice.shape[3]
    wide = cols + LANES
    ext = ice.shape[2] // SUB
    lane = lane_iota()
    row = row_iota(wide)
    zero = jnp.zeros((SUB, wide), F32)
    keep = 1.0 / (1.0 + RELAX)
    for cap in range(2):
        for j in range(ext):
            t = tile(j)

            def field(f):
                return widened(ice[cap, f, t, :], from_left, from_right, (cap * NEXT + f) * ext + j, lane)

            hh = field(0)
            u_s[cap, t, :] = field(1)
            v_s[cap, t, :] = field(2)
            s0_s[cap, t, :] = field(3)
            s1_s[cap, t, :] = field(4)
            s2_s[cap, t, :] = field(5)
            w0, w1, f0, f1 = field(6), field(7), field(8), field(9)
            inv = jnp.where(hh > 0.0, 1.0 / (hh + (1.0 + STEP * DRAG)), 0.0)
            quick = STEP * inv
            a_s[cap, t, :] = hh * (RELAX * STRENGTH * keep)
            m_s[cap, t, :] = (hh + 1.0) * inv
            q_s[cap, t, :] = quick
            fx_s[cap, t, :] = quick * (w0 + DRAG * f0)
            fy_s[cap, t, :] = quick * (w1 + DRAG * f1)
            f0_s[cap, t, :] = f0
            f1_s[cap, t, :] = f1

    def subcycle(_, carry):
        for cap in range(2):
            p_prev, s2_prev = zero, zero
            u, v = u_s[cap, tile(0), :], v_s[cap, tile(0), :]
            for j in range(ext):
                t = tile(j)
                if j + 1 < ext:
                    u_next, v_next = u_s[cap, tile(j + 1), :], v_s[cap, tile(j + 1), :]
                else:
                    u_next, v_next = zero, zero
                ux = from_next_row(u, u_next, row) - u
                vx = from_next_row(v, v_next, row) - v
                uy = from_next_col(u) - u
                vy = from_next_col(v) - v
                ed, et, es = ux + vy, ux - vy, uy + vx
                a = a_s[cap, t, :]
                ratio = a * lax.rsqrt(ed * ed + et * et + es * es + 1.0)
                s0 = s0_s[cap, t, :] * keep + (ratio * ed - a)
                s1 = s1_s[cap, t, :] * keep + ratio * et
                s2 = s2_s[cap, t, :] * keep + ratio * es
                s0_s[cap, t, :] = s0
                s1_s[cap, t, :] = s1
                s2_s[cap, t, :] = s2
                p = 0.5 * (s0 + s1)
                q = 0.5 * (s0 - s1)
                force_x = (p - from_prev_row(p, p_prev, row)) + (s2 - from_prev_col(s2))
                force_y = (q - from_prev_col(q)) + (s2 - from_prev_row(s2, s2_prev, row))
                m, quick = m_s[cap, t, :], q_s[cap, t, :]
                u_s[cap, t, :] = m * u + (quick * force_x + fx_s[cap, t, :])
                v_s[cap, t, :] = m * v + (quick * force_y + fy_s[cap, t, :])
                p_prev, s2_prev = p, s2
                u, v = u_next, v_next
        return carry

    lax.fori_loop(0, NSUB, subcycle, 0)
    spreads = []
    for cap in range(2):
        parts = []
        d0_prev = zero
        for j in range(1, ext):
            t = tile(j)
            if j < ext - 1:
                out = tile(j - 1)
                u, v = u_s[cap, t, :], v_s[cap, t, :]
                vel_out[0, cap, out, :] = u[:, :cols]
                vel_out[1, cap, out, :] = v[:, :cols]
                stress_out[0, cap, out, :] = s0_s[cap, t, :][:, :cols]
                stress_out[1, cap, out, :] = s1_s[cap, t, :][:, :cols]
                stress_out[2, cap, out, :] = s2_s[cap, t, :][:, :cols]
                iced = m_s[cap, t, :] > 0.0
                d0 = jnp.where(iced, DRAG * (u - f0_s[cap, t, :]), 0.0)
                d1 = jnp.where(iced, DRAG * (v - f1_s[cap, t, :]), 0.0)
            else:
                d0 = d1 = zero
            parts.append((d0 - from_prev_row(d0, d0_prev, row)) + (d1 - from_prev_col(d1)))
            d0_prev = d0
        spreads.append(parts)
    for k, (north, south) in enumerate(zip(*spreads)):
        t = tile(k)
        p1[t, :] = jnp.where((g == 1) | (g == 3), north, south)
        p2[t, :] = jnp.where(g == 2, north, south)
        p3[t, :] = jnp.where(g == 3, north, south)
        mine[t, :] = jnp.where(g == 0, north, south)


def neighbour_sum(ref, k, row):
    here, before, after = ref[tile(k), :], ref[tile(k - 1), :], ref[tile(k + 1), :]
    along = from_prev_row(here, before, row) + from_next_row(here, after, row)
    return along + (from_prev_col(here) + from_next_col(here))


def ocean_before(first, g_ref, ocean, from_left, from_right, gw, invd, ra, g_s, gx_s, x_s, b_s):
    cols = ocean.shape[2]
    wide = cols + LANES
    ext = ocean.shape[1] // SUB
    lane = lane_iota()
    row = row_iota(wide)
    zero = jnp.zeros((SUB, wide), F32)
    for ref in (g_s, gx_s):
        ref[tile(0), :] = zero
        ref[tile(ext + 1), :] = zero
    for j in range(ext):
        t = tile(j + 1)

        def field(i):
            return widened(ocean[i, tile(j), :], from_left, from_right, first + i * ext + j, lane)

        b_s[tile(j), :] = field(0)
        depth = field(1)
        x = field(2)
        g_s[t, :] = depth
        gx_s[t, :] = depth * x
        x_s[tile(j), :] = x
        gw[tile(j), :] = depth
    for j in range(ext):
        t = tile(j)
        depth = g_s[tile(j + 1), :]
        diag = DAMP + depth * neighbour_sum(g_s, j + 1, row)
        invd[t, :] = 1.0 / diag
        around = depth * neighbour_sum(gx_s, j + 1, row)
        ra[t, :] = jnp.where(depth > 0.0, b_s[t, :], 0.0) - (diag * x_s[t, :] - around)


def ocean_basis(g_ref, gw, invd, ra, r1, r2, r3, mine, y0_out, y1_out, y2_out, sums,
                sp, u0_s, u1_s, u2_s):
    g = g_ref[0]
    wide = gw.shape[1]
    ext = gw.shape[0] // SUB
    cols = y0_out.shape[1]
    slab = r1.shape[0] // SUB - 1
    row = row_iota(wide)
    zero = jnp.zeros((SUB, wide), F32)
    for ref in (u0_s, u1_s, u2_s):
        ref[tile(0), :] = zero
        ref[tile(ext + 1), :] = zero

    def clear(which):
        for j in which:
            sp[tile(j), :] = zero

    def whole(slabs):
        clear([0])
        for k, ref in enumerate(slabs):
            for t in range(slab):
                value = ref[tile(t), :]
                if t == 0 and k > 0:
                    value = value + slabs[k - 1][tile(slab), :]
                sp[tile(1 + slab * k + t), :] = value
        sp[tile(1 + slab * len(slabs)), :] = slabs[-1][tile(slab), :]

    @pl.when(g == 0)
    def _():
        whole([mine, r1, r2, r3])

    @pl.when(g == 3)
    def _():
        whole([r3, r2, r1, mine])

    @pl.when(g == 1)
    def _():
        clear(range(2, ext))
        sp[tile(0), :] = r1[tile(slab - 1), :]
        sp[tile(1), :] = r1[tile(slab), :]

    @pl.when(g == 2)
    def _():
        clear(range(ext - 1))
        sp[tile(ext - 1), :] = r1[tile(0), :]

    acc = [jnp.zeros((SUB, cols), F32) for _ in range(6)]

    def add(k, left, right, j):
        if 0 < j < ext - 1:
            acc[k] = acc[k] + left[:, :cols] * right[:, :cols]

    for j in range(ext):
        t = tile(j)
        depth = gw[t, :]
        r0 = ra[t, :] + jnp.where(depth > 0.0, sp[t, :], 0.0)
        y0 = r0 * invd[t, :]
        u0_s[tile(j + 1), :] = depth * y0
        if 0 < j < ext - 1:
            y0_out[tile(j - 1), :] = y0[:, :cols]
        add(0, r0, y0, j)
    for j in range(ext):
        t = tile(j)
        depth = gw[t, :]
        w = depth * neighbour_sum(u0_s, j + 1, row)
        y1 = w * invd[t, :]
        u1_s[tile(j + 1), :] = depth * y1
        if 0 < j < ext - 1:
            y1_out[tile(j - 1), :] = y1[:, :cols]
            acc[1] = acc[1] + y0_out[tile(j - 1), :] * w[:, :cols]
        add(2, w, y1, j)
    for j in range(ext):
        t = tile(j)
        depth = gw[t, :]
        w = depth * neighbour_sum(u1_s, j + 1, row)
        y2 = w * invd[t, :]
        u2_s[tile(j + 1), :] = depth * y2
        if 0 < j < ext - 1:
            y2_out[tile(j - 1), :] = y2[:, :cols]
            acc[3] = acc[3] + y1_out[tile(j - 1), :] * w[:, :cols]
        add(4, w, y2, j)
    for j in range(1, ext - 1):
        w = neighbour_sum(u2_s, j + 1, row)[:, :cols] * u2_s[tile(j + 1), :][:, :cols]
        acc[5] = acc[5] + w
    for k in range(6):
        total = acc[k][:, :LANES]
        for c in range(1, cols // LANES):
            total = total + acc[k][:, c * LANES : (c + 1) * LANES]
        sums[k : k + 1, :] = jnp.sum(total, axis=0, keepdims=True)
    sums[6:8, :] = jnp.zeros((2, LANES), F32)


def combine(g_ref, parts, x0, y0, y1, y2, out):
    total = jnp.sum(jnp.sum(parts[...], axis=0), axis=1, keepdims=True)
    total = jnp.broadcast_to(total, (SUB, LANES))
    m = [jnp.broadcast_to(total[k : k + 1, :], (SUB, LANES)) for k in range(6)]

    def dot(left, right, image):
        value = None
        for i, a in enumerate(left):
            for j, b in enumerate(right):
                moment = m[i + j] - m[i + j + 1] if image else m[i + j]
                term = a * b * moment
                value = term if value is None else value + term
        return value

    z = [jnp.ones((SUB, LANES), F32)]
    p = z
    rz = m[0]
    coef = [0.0, 0.0, 0.0]
    for step in range(ITERS):
        alpha = rz / dot(p, p, True)
        for i, a in enumerate(p):
            coef[i] = coef[i] + alpha * a
        if step + 1 < ITERS:
            image = [a for a in p] + [jnp.zeros((SUB, LANES), F32)]
            for i, a in enumerate(p):
                image[i + 1] = image[i + 1] - a
            z = [(z[i] if i < len(z) else 0.0) - alpha * image[i] for i in range(len(image))]
            fresh = dot(z, z, False)
            beta = fresh / rz
            p = [z[i] + beta * p[i] if i < len(p) else z[i] for i in range(len(z))]
            rz = fresh
    reps = x0.shape[1] // LANES
    wide = [jnp.concatenate([c] * reps, axis=1) for c in coef]
    for k in range(x0.shape[0] // SUB):
        t = tile(k)
        out[t, :] = x0[t, :] + (wide[0] * y0[t, :] + wide[1] * y1[t, :] + wide[2] * y2[t, :])


def shards(
    base_rhs,
    depth,
    ssh_prev,
    currents,
    land_blocks,
    ice_thick,
    ice_blocks,
    ice_vel,
    ice_stress,
    wind,
):
    groups = lax.axis_size("grp")
    tiles = lax.axis_size("tile")
    assert groups == 4
    g = lax.axis_index("grp").astype(jnp.int32).reshape(1)
    rows, cols = base_rhs.shape
    ice_rows = ice_thick.shape[1]
    assert rows == groups * ice_rows
    slab = ice_rows + 2 * SUB
    wide = cols + LANES

    strip = (2 * slab, cols)
    gf, h, a, b, c, d = call(
        functools.partial(pack_rows, groups), "pack_rows",
        [(rows, cols), (2, ice_rows, cols), strip, strip, strip, strip],
        [g, base_rhs, depth, ssh_prev, currents, land_blocks, ice_thick, ice_blocks, ice_vel, ice_stress, wind],
    )
    ra = lax.ppermute(a, "grp", [(0, 1), (1, 0), (2, 3), (3, 2)])
    rc = lax.ppermute(c, "grp", [(0, 3), (3, 0), (1, 2), (2, 1)])
    rb = lax.ppermute(b, "grp", [(0, 2), (3, 1)])
    rd = lax.ppermute(d, "grp", [(0, 1), (3, 2)])

    ice_tiles = 2 * NEXT * (slab // SUB)
    ocean_rows = rows + 2 * SUB
    count = ice_tiles + NOC * (ocean_rows // SUB)
    packed = (-(-count // SLOTS) * SUB, LANES)
    ice, ocean, left, right = call(
        pack_cols, "pack_cols",
        [(2, NEXT, slab, cols), (NOC, ocean_rows, cols), packed, packed],
        [g, ra, rb, rc, rd, currents, h, ice_vel, ice_stress, wind, base_rhs, gf, ssh_prev],
    )
    from_left = lax.ppermute(right, "tile", [(i, i + 1) for i in range(tiles - 1)])
    from_right = lax.ppermute(left, "tile", [(i + 1, i) for i in range(tiles - 1)])

    back = (ice_rows + SUB, wide)
    velocity, stress, p1, p2, p3, mine = call(
        ice_steps, "ice_steps",
        [ice_vel.shape, ice_stress.shape, back, back, back, back],
        [g, ice, from_left, from_right],
        scratch=[(2, slab, wide)] * 12,
        mib=32,
    )
    r1 = lax.ppermute(p1, "grp", [(1, 0), (2, 3), (3, 1), (0, 2)])
    r2 = lax.ppermute(p2, "grp", [(2, 0), (1, 3)])
    r3 = lax.ppermute(p3, "grp", [(3, 0), (0, 3)])

    field = (ocean_rows, wide)
    padded = (ocean_rows + 2 * SUB, wide)
    gw, invd, known = call(
        functools.partial(ocean_before, ice_tiles), "ocean_before",
        [field] * 3,
        [g, ocean, from_left, from_right],
        scratch=[padded, padded, field, field],
        flops=20000000,
    )
    y0, y1, y2, sums = call(
        ocean_basis, "ocean_basis",
        [(rows, cols)] * 3 + [(SUB, LANES)],
        [g, gw, invd, known, r1, r2, r3, mine],
        scratch=[field, padded, padded, padded],
    )
    devices = groups * tiles
    shared = lax.all_to_all(
        jnp.broadcast_to(sums[None], (devices, SUB, LANES)), ("grp", "tile"), 0, 0, tiled=True
    )
    (ssh,) = call(combine, "combine", [(rows, cols)], [g, shared, ssh_prev, y0, y1, y2])
    return ssh, velocity, stress


def solution(mesh):
    return jax.shard_map(
        shards,
        mesh=mesh,
        in_specs=(
            P("grp", "tile"),
            P("grp", "tile"),
            P("grp", "tile"),
            P(None, "grp", "tile"),
            P("grp", "tile"),
            P(None, "grp", "tile"),
            P(None, "grp", "tile"),
            P(None, None, "grp", "tile"),
            P(None, None, "grp", "tile"),
            P(None, None, "grp", "tile"),
        ),
        out_specs=(P("grp", "tile"), P(None, None, "grp", "tile"), P(None, None, "grp", "tile")),
        check_vma=False,
    )
```

```python
import functools

import jax
import jax.numpy as jnp
from jax import lax
from jax.experimental import pallas as pl
from jax.experimental.pallas import tpu as pltpu
from jax.sharding import PartitionSpec as P

BS = 8
NSUB = 8
ITERS = 3

DAMP = 0.05
RELAX = 0.2
STRENGTH = 0.5
DRAG = 1.0
STEP = 0.5

F32 = jnp.float32
SUB = 8
LANES = 128
EDGE = 16
SLOTS = LANES // EDGE
GROUP = 4
SKEW = 2
NICE = 8
NEXT = NICE + 2
NOC = 3


def vmem():
    return pl.BlockSpec(memory_space=pltpu.VMEM)


def smem():
    return pl.BlockSpec(memory_space=pltpu.SMEM)


def call(body, name, outs, ins, scratch=(), sems=0, hbm=False, mib=24, flops=1000000):
    shapes = tuple(jax.ShapeDtypeStruct(s, F32) for s in outs)
    other = pl.BlockSpec(memory_space=pltpu.HBM) if hbm else vmem()
    specs = [smem() if i == 0 else other for i in range(len(ins))]
    held = [pltpu.VMEM(*s) if isinstance(s[0], tuple) else pltpu.VMEM(s, F32) for s in scratch]
    if sems:
        held.append(pltpu.SemaphoreType.DMA((sems,)))
    return pl.pallas_call(
        body,
        name=name,
        out_shape=shapes,
        in_specs=specs,
        out_specs=tuple(vmem() for _ in outs),
        scratch_shapes=held,
        cost_estimate=pl.CostEstimate(flops=flops, bytes_accessed=4000000, transcendentals=0),
        compiler_params=pltpu.CompilerParams(vmem_limit_bytes=mib * 1024 * 1024),
    )(*ins)


def tile(k):
    return slice(k * SUB, k * SUB + SUB)


def expanded_cols(blocks):
    count = blocks.shape[-1]
    row = lax.broadcasted_iota(jnp.int32, (count, count * BS), 0) * BS
    col = lax.broadcasted_iota(jnp.int32, (count, count * BS), 1)
    spread = ((col >= row) & (col < row + BS)).astype(F32)
    return jnp.dot(blocks.astype(F32), spread, preferred_element_type=F32)


def row_iota(cols):
    return lax.broadcasted_iota(jnp.int32, (SUB, cols), 0)


def lane_iota():
    return lax.broadcasted_iota(jnp.int32, (SUB, LANES), 1)


def from_next_row(here, after, row):
    return pltpu.roll(jnp.where(row == 0, after, here), SUB - 1, 0)


def from_prev_row(here, before, row):
    return pltpu.roll(jnp.where(row == SUB - 1, before, here), 1, 0)


def from_next_col(here):
    return pltpu.roll(here, here.shape[1] - 1, 1)


def from_prev_col(here):
    return pltpu.roll(here, 1, 1)


def own_tile(cur, comp, first, j):
    last = cur.shape[1] // SUB - 1
    t = jnp.clip(first + j, 0, last)
    return cur[comp, pl.ds(pl.multiple_of(t * SUB, SUB), SUB), :]


def pack_rows(g_ref, base, depth, x0, cur, land, thick, iceb, vel, stress, wind,
              a, b, c, d, thick_s, depth_s, land_s, iceb_s, sems):
    g = g_ref[0]
    rows, cols = base.shape
    ice_rows = thick.shape[1]
    slab = ice_rows + 2 * SUB

    def run(slabs, halos):
        copies = []

        def copy(src, dst):
            made = pltpu.make_async_copy(src, dst, sems.at[len(copies)])
            made.start()
            copies.append(made)

        for out, dest in slabs:
            start = ice_rows * dest - SUB
            first, last = max(start, 0), min(start + slab, rows)
            for comp in range(2):
                at = comp * slab + first - start
                copy(cur.at[comp, first:last, :], out.at[at : at + last - first, :])
                if first > start:
                    out[comp * slab : at, :] = jnp.zeros((first - start, cols), F32)
                if last < start + slab:
                    out[at + last - first : (comp + 1) * slab, :] = jnp.zeros((start + slab - last, cols), F32)
        if halos:
            copy(land, land_s)
            copy(iceb, iceb_s)
        for i, (out, last) in enumerate(halos):
            r = slice(ice_rows - SUB, ice_rows) if last else slice(0, SUB)
            ro = slice(rows - SUB, rows) if last else slice(0, SUB)
            for cap in range(2):
                copy(thick.at[cap, r, :], thick_s.at[i, cap])
                n = cap * NICE + 1
                pieces = [vel.at[0, cap, r, :], vel.at[1, cap, r, :]]
                pieces += [stress.at[k, cap, r, :] for k in range(3)]
                pieces += [wind.at[k, cap, r, :] for k in range(2)]
                for piece in pieces:
                    copy(piece, out.at[tile(n), :])
                    n += 1
            copy(depth.at[ro, :], depth_s.at[i])
            copy(base.at[ro, :], out.at[tile(2 * NICE), :])
            copy(x0.at[ro, :], out.at[tile(2 * NICE + 2), :])
            out[tile(2 * NICE + 3), :] = jnp.zeros((SUB, cols), F32)
        for made in copies:
            made.wait()
        if halos:
            wet = expanded_cols(land_s[...])
            covers = [expanded_cols(iceb_s[cap]) for cap in range(2)]
        for i, (out, last) in enumerate(halos):
            for cap in range(2):
                k = covers[cap].shape[0] - 1 if last else 0
                out[tile(cap * NICE), :] = thick_s[i, cap] * covers[cap][k : k + 1, :]
            k = wet.shape[0] - 1 if last else 0
            out[tile(2 * NICE + 1), :] = depth_s[i] * wet[k : k + 1, :]

    @pl.when(g == 0)
    def _():
        run([(c, 3), (a, 1), (b, 2)], [(d, True)])

    @pl.when(g == 3)
    def _():
        run([(c, 0), (a, 2), (b, 1)], [(d, False)])

    @pl.when(g == 1)
    def _():
        run([], [(a, False), (c, True)])

    @pl.when(g == 2)
    def _():
        run([], [(a, True), (c, False)])


def masks(g_ref, depth, land, thick, iceb, gf, h):
    wet = expanded_cols(land[...])
    for k in range(depth.shape[0] // SUB):
        gf[tile(k), :] = depth[tile(k), :] * wet[k : k + 1, :]
    for cap in range(2):
        cover = expanded_cols(iceb[cap])
        for k in range(thick.shape[1] // SUB):
            h[cap, tile(k), :] = thick[cap, tile(k), :] * cover[k : k + 1, :]


def pack_cols(g_ref, ra, rb, rc, rd, cur, h, vel, stress, wind, base, gf, x0, ice, ocean, left, right):
    g = g_ref[0]
    cols = base.shape[1]
    slab_tiles = h.shape[1] // SUB
    ext = slab_tiles + 2
    rows = base.shape[0] // SUB
    lane = lane_iota()
    slot = lane // EDGE
    zero = jnp.zeros((SUB, cols), F32)
    state = {"n": 0, "l": None, "r": None}

    def emit(value):
        n = state["n"]
        s = n % SLOTS
        both = jnp.where(lane < EDGE, value[:, :LANES], value[:, cols - LANES :])
        both = pltpu.roll(both, EDGE * s, 1) if s else both
        before = (s - 1) % SLOTS
        if s == 0:
            state["l"] = state["r"] = both
        else:
            state["l"] = jnp.where(slot == s, both, state["l"])
            state["r"] = jnp.where(slot == before, both, state["r"])
        if s == SLOTS - 1:
            k = n // SLOTS
            left[tile(k), :] = state["l"]
            right[tile(k), :] = state["r"]
        state["n"] = n + 1

    def low(k):
        r = tile(k)
        return jnp.where(g == 1, rd[r, :], jnp.where(g == 2, rc[r, :], jnp.where(g == 3, ra[r, :], zero)))

    def high(k):
        r = tile(k)
        return jnp.where(g == 0, ra[r, :], jnp.where(g == 1, rc[r, :], jnp.where(g == 2, rd[r, :], zero)))

    for cap in range(2):
        own = [h.at[cap], vel.at[0, cap], vel.at[1, cap], stress.at[0, cap], stress.at[1, cap],
               stress.at[2, cap], wind.at[0, cap], wind.at[1, cap]]
        for f in range(NICE):
            for j in range(ext):
                if j == 0:
                    value = low(cap * NICE + f)
                elif j == ext - 1:
                    value = high(cap * NICE + f)
                else:
                    value = own[f][tile(j - 1), :]
                ice[cap, f, tile(j), :] = value
                emit(value)
        for comp in range(2):
            for j in range(ext):
                r = tile(comp * ext + j)
                mine = own_tile(cur, comp, slab_tiles * g - 1, j)
                if cap == 0:
                    value = jnp.where(g == 0, mine, jnp.where(g == 1, ra[r, :], jnp.where(g == 2, rb[r, :], rc[r, :])))
                else:
                    value = jnp.where(g == 3, mine, jnp.where(g == 2, ra[r, :], jnp.where(g == 1, rb[r, :], rc[r, :])))
                ice[cap, NICE + comp, tile(j), :] = value
                emit(value)
    for i, field in enumerate((base, gf, x0)):
        for j in range(rows + 2):
            if j == 0:
                value = low(2 * NICE + i)
            elif j == rows + 1:
                value = high(2 * NICE + i)
            else:
                value = field[tile(j - 1), :]
            ocean[i, tile(j), :] = value
            emit(value)
    while state["n"] % SLOTS:
        emit(zero)


def outer_columns(from_left, from_right, n, lane):
    s, k = n % SLOTS, n // SLOTS
    both = jnp.where(lane // EDGE == s, from_right[tile(k), :], from_left[tile(k), :])
    both = pltpu.roll(both, LANES - EDGE * s, 1) if s else both
    return jnp.where((lane < EDGE) | (lane >= LANES - EDGE), both, 0.0)


def split(value):
    return [value[:, c * LANES : (c + 1) * LANES] for c in range(value.shape[1] // LANES)]


def turned_next(regs, lane):
    n = len(regs)
    return [pltpu.roll(jnp.where(lane == 0, regs[(c + 1) % n], regs[c]), LANES - 1, 1) for c in range(n)]


def turned_prev(regs, lane):
    n = len(regs)
    return [pltpu.roll(jnp.where(lane == LANES - 1, regs[c - 1], regs[c]), 1, 1) for c in range(n)]


def ice_steps(g_ref, ice, from_left, from_right, vel_out, stress_out, p1, p2, p3, mine,
              u_s, v_s, p_s, q_s, s_s, un_s, vn_s, qp_s, sp_s, a_s, m_s, w_s, fx_s, fy_s, f0_s, f1_s):
    g = g_ref[0]
    cols = ice.shape[3]
    regs = cols // LANES + 1
    ext = ice.shape[2] // SUB
    lane = lane_iota()
    zero = jnp.zeros((SUB, LANES), F32)
    keep = 1.0 / (1.0 + RELAX)

    def at(j, shift=0):
        return slice(SUB * (j + 1) + shift, SUB * (j + 2) + shift)

    for cap in range(2):
        for c in range(regs):
            for ref in (p_s, s_s):
                ref[cap, c, at(-1), :] = zero
            for ref in (u_s, v_s):
                ref[cap, c, at(ext), :] = zero
        outers = []
        for j in range(ext):
            if j % GROUP == 0:
                outers = [
                    [outer_columns(from_left, from_right, (cap * NEXT + f) * ext + i, lane) for f in range(NEXT)]
                    for i in range(j, min(j + GROUP, ext))
                ]
            fields = [split(ice[cap, f, tile(j), :]) + [outers[j % GROUP][f]] for f in range(NEXT)]
            for c in range(regs):
                hh, u, v, s0, s1, s2, w0, w1, f0, f1 = (f[c] for f in fields)
                u_s[cap, c, at(j), :] = u
                v_s[cap, c, at(j), :] = v
                p_s[cap, c, at(j), :] = 0.5 * (s0 + s1)
                q_s[cap, c, at(j), :] = 0.5 * (s0 - s1)
                s_s[cap, c, at(j), :] = s2
                inv = jnp.where(hh > 0.0, 1.0 / (hh + (1.0 + STEP * DRAG)), 0.0)
                quick = STEP * inv
                a_s[cap, c, at(j), :] = hh * (RELAX * STRENGTH * keep)
                m_s[cap, c, at(j), :] = (hh + 1.0) * inv
                w_s[cap, c, at(j), :] = quick
                fx_s[cap, c, at(j), :] = quick * (w0 + DRAG * f0)
                fy_s[cap, c, at(j), :] = quick * (w1 + DRAG * f1)
                f0_s[cap, c, at(j), :] = f0
                f1_s[cap, c, at(j), :] = f1
    for j in range(ext):
        for cap in range(2):
            for ref, source in ((un_s, u_s), (vn_s, v_s)):
                turned = turned_next([source[cap, c, at(j), :] for c in range(regs)], lane)
                for c in range(regs):
                    ref[cap, c, at(j), :] = turned[c]

    def stress_tile(cap, j):
        qs, ss = [], []
        for c in range(regs):
            u, v = u_s[cap, c, at(j), :], v_s[cap, c, at(j), :]
            ux = u_s[cap, c, at(j, 1), :] - u
            vx = v_s[cap, c, at(j, 1), :] - v
            uy = un_s[cap, c, at(j), :] - u
            vy = vn_s[cap, c, at(j), :] - v
            es = uy + vx
            half = ux * ux + vy * vy
            a = a_s[cap, c, at(j), :]
            ratio = a * lax.rsqrt((half + half) + (es * es + 1.0))
            low = 0.5 * a
            q = q_s[cap, c, at(j), :] * keep + (ratio * vy - low)
            s = s_s[cap, c, at(j), :] * keep + ratio * es
            p_s[cap, c, at(j), :] = p_s[cap, c, at(j), :] * keep + (ratio * ux - low)
            q_s[cap, c, at(j), :] = q
            s_s[cap, c, at(j), :] = s
            qs.append(q)
            ss.append(s)
        for ref, turned in ((qp_s, turned_prev(qs, lane)), (sp_s, turned_prev(ss, lane))):
            for c in range(regs):
                ref[cap, c, at(j), :] = turned[c]

    def velocity_tile(cap, j):
        us, vs = [], []
        for c in range(regs):
            s = s_s[cap, c, at(j), :]
            force_x = (p_s[cap, c, at(j), :] - p_s[cap, c, at(j, -1), :]) + (s - sp_s[cap, c, at(j), :])
            force_y = (q_s[cap, c, at(j), :] - qp_s[cap, c, at(j), :]) + (s - s_s[cap, c, at(j, -1), :])
            m, quick = m_s[cap, c, at(j), :], w_s[cap, c, at(j), :]
            u = m * u_s[cap, c, at(j), :] + (quick * force_x + fx_s[cap, c, at(j), :])
            v = m * v_s[cap, c, at(j), :] + (quick * force_y + fy_s[cap, c, at(j), :])
            u_s[cap, c, at(j), :] = u
            v_s[cap, c, at(j), :] = v
            us.append(u)
            vs.append(v)
        for ref, turned in ((un_s, turned_next(us, lane)), (vn_s, turned_next(vs, lane))):
            for c in range(regs):
                ref[cap, c, at(j), :] = turned[c]

    def subcycle(_, carry):
        for j in range(ext + SKEW):
            for cap in range(2):
                if j < ext:
                    stress_tile(cap, j)
                if j >= SKEW:
                    velocity_tile(cap, j - SKEW)
        return carry

    lax.fori_loop(0, NSUB, subcycle, 0)
    spreads = []
    for cap in range(2):
        for c in range(regs):
            q_s[cap, c, at(0), :] = zero
            q_s[cap, c, at(ext - 1), :] = zero
        parts = []
        across = [[zero] * regs]
        for j in range(1, ext - 1):
            d1s = []
            for c in range(regs):
                u, v = u_s[cap, c, at(j), :], v_s[cap, c, at(j), :]
                p, q = p_s[cap, c, at(j), :], q_s[cap, c, at(j), :]
                if c + 1 < regs:
                    block = (tile(j - 1), slice(c * LANES, (c + 1) * LANES))
                    vel_out[(0, cap) + block] = u
                    vel_out[(1, cap) + block] = v
                    stress_out[(0, cap) + block] = p + q
                    stress_out[(1, cap) + block] = p - q
                    stress_out[(2, cap) + block] = s_s[cap, c, at(j), :]
                iced = m_s[cap, c, at(j), :] > 0.0
                q_s[cap, c, at(j), :] = jnp.where(iced, DRAG * (u - f0_s[cap, c, at(j), :]), 0.0)
                d1s.append(jnp.where(iced, DRAG * (v - f1_s[cap, c, at(j), :]), 0.0))
            turned = turned_prev(d1s, lane)
            across.append([d1s[c] - turned[c] for c in range(regs)])
        across.append([zero] * regs)
        for j in range(1, ext):
            parts.append([
                (q_s[cap, c, at(j), :] - q_s[cap, c, at(j, -1), :]) + across[j][c] for c in range(regs)
            ])
        spreads.append(parts)
    for k, (norths, souths) in enumerate(zip(*spreads)):
        for c, (north, south) in enumerate(zip(norths, souths)):
            block = (tile(k), slice(c * LANES, (c + 1) * LANES))
            p1[block] = jnp.where((g == 1) | (g == 3), north, south)
            p2[block] = jnp.where(g == 2, north, south)
            p3[block] = jnp.where(g == 3, north, south)
            mine[block] = jnp.where(g == 0, north, south)


def neighbour_sum(ref, k, row):
    here, before, after = ref[tile(k), :], ref[tile(k - 1), :], ref[tile(k + 1), :]
    along = from_prev_row(here, before, row) + from_next_row(here, after, row)
    return along + (from_prev_col(here) + from_next_col(here))


def ocean_before(first, g_ref, ocean, from_left, from_right, gw, invd, ra, g_s, gx_s, x_s, b_s):
    cols = ocean.shape[2]
    wide = cols + LANES
    ext = ocean.shape[1] // SUB
    lane = lane_iota()
    row = row_iota(wide)
    zero = jnp.zeros((SUB, wide), F32)
    for ref in (g_s, gx_s):
        ref[tile(0), :] = zero
        ref[tile(ext + 1), :] = zero
    for j in range(ext):
        t = tile(j + 1)

        def field(i):
            outer = outer_columns(from_left, from_right, first + i * ext + j, lane)
            return jnp.concatenate([ocean[i, tile(j), :], outer], axis=1)

        b_s[tile(j), :] = field(0)
        depth = field(1)
        x = field(2)
        g_s[t, :] = depth
        gx_s[t, :] = depth * x
        x_s[tile(j), :] = x
        gw[tile(j), :] = depth
    for j in range(ext):
        t = tile(j)
        depth = g_s[tile(j + 1), :]
        diag = DAMP + depth * neighbour_sum(g_s, j + 1, row)
        invd[t, :] = 1.0 / diag
        around = depth * neighbour_sum(gx_s, j + 1, row)
        ra[t, :] = jnp.where(depth > 0.0, b_s[t, :], 0.0) - (diag * x_s[t, :] - around)


def ocean_basis(g_ref, gw, invd, ra, r1, r2, r3, mine, y0_out, y1_out, y2_out, sums,
                sp, u0_s, u1_s, u2_s):
    g = g_ref[0]
    wide = gw.shape[1]
    ext = gw.shape[0] // SUB
    cols = y0_out.shape[1]
    slab = r1.shape[0] // SUB - 1
    row = row_iota(wide)
    zero = jnp.zeros((SUB, wide), F32)
    for ref in (u0_s, u1_s, u2_s):
        ref[tile(0), :] = zero
        ref[tile(ext + 1), :] = zero

    def clear(which):
        for j in which:
            sp[tile(j), :] = zero

    def whole(slabs):
        clear([0])
        for k, ref in enumerate(slabs):
            for t in range(slab):
                value = ref[tile(t), :]
                if t == 0 and k > 0:
                    value = value + slabs[k - 1][tile(slab), :]
                sp[tile(1 + slab * k + t), :] = value
        sp[tile(1 + slab * len(slabs)), :] = slabs[-1][tile(slab), :]

    @pl.when(g == 0)
    def _():
        whole([mine, r1, r2, r3])

    @pl.when(g == 3)
    def _():
        whole([r3, r2, r1, mine])

    @pl.when(g == 1)
    def _():
        clear(range(2, ext))
        sp[tile(0), :] = r1[tile(slab - 1), :]
        sp[tile(1), :] = r1[tile(slab), :]

    @pl.when(g == 2)
    def _():
        clear(range(ext - 1))
        sp[tile(ext - 1), :] = r1[tile(0), :]

    acc = [jnp.zeros((SUB, cols), F32) for _ in range(6)]

    def add(k, left, right, j):
        if 0 < j < ext - 1:
            acc[k] = acc[k] + left[:, :cols] * right[:, :cols]

    for j in range(ext):
        t = tile(j)
        depth = gw[t, :]
        r0 = ra[t, :] + jnp.where(depth > 0.0, sp[t, :], 0.0)
        y0 = r0 * invd[t, :]
        u0_s[tile(j + 1), :] = depth * y0
        if 0 < j < ext - 1:
            y0_out[tile(j - 1), :] = y0[:, :cols]
        add(0, r0, y0, j)
    for j in range(ext):
        t = tile(j)
        depth = gw[t, :]
        w = depth * neighbour_sum(u0_s, j + 1, row)
        y1 = w * invd[t, :]
        u1_s[tile(j + 1), :] = depth * y1
        if 0 < j < ext - 1:
            y1_out[tile(j - 1), :] = y1[:, :cols]
            acc[1] = acc[1] + y0_out[tile(j - 1), :] * w[:, :cols]
        add(2, w, y1, j)
    for j in range(ext):
        t = tile(j)
        depth = gw[t, :]
        w = depth * neighbour_sum(u1_s, j + 1, row)
        y2 = w * invd[t, :]
        u2_s[tile(j + 1), :] = depth * y2
        if 0 < j < ext - 1:
            y2_out[tile(j - 1), :] = y2[:, :cols]
            acc[3] = acc[3] + y1_out[tile(j - 1), :] * w[:, :cols]
        add(4, w, y2, j)
    for j in range(1, ext - 1):
        w = neighbour_sum(u2_s, j + 1, row)[:, :cols] * u2_s[tile(j + 1), :][:, :cols]
        acc[5] = acc[5] + w
    for k in range(6):
        total = acc[k][:, :LANES]
        for c in range(1, cols // LANES):
            total = total + acc[k][:, c * LANES : (c + 1) * LANES]
        sums[k : k + 1, :] = jnp.sum(total, axis=0, keepdims=True)
    sums[6:8, :] = jnp.zeros((2, LANES), F32)


def combine(g_ref, parts, x0, y0, y1, y2, out):
    total = jnp.sum(jnp.sum(parts[...], axis=0), axis=1, keepdims=True)
    total = jnp.broadcast_to(total, (SUB, LANES))
    m = [jnp.broadcast_to(total[k : k + 1, :], (SUB, LANES)) for k in range(6)]

    def dot(left, right, image):
        value = None
        for i, a in enumerate(left):
            for j, b in enumerate(right):
                moment = m[i + j] - m[i + j + 1] if image else m[i + j]
                term = a * b * moment
                value = term if value is None else value + term
        return value

    z = [jnp.ones((SUB, LANES), F32)]
    p = z
    rz = m[0]
    coef = [0.0, 0.0, 0.0]
    for step in range(ITERS):
        alpha = rz / dot(p, p, True)
        for i, a in enumerate(p):
            coef[i] = coef[i] + alpha * a
        if step + 1 < ITERS:
            image = [a for a in p] + [jnp.zeros((SUB, LANES), F32)]
            for i, a in enumerate(p):
                image[i + 1] = image[i + 1] - a
            z = [(z[i] if i < len(z) else 0.0) - alpha * image[i] for i in range(len(image))]
            fresh = dot(z, z, False)
            beta = fresh / rz
            p = [z[i] + beta * p[i] if i < len(p) else z[i] for i in range(len(z))]
            rz = fresh
    reps = x0.shape[1] // LANES
    wide = [jnp.concatenate([c] * reps, axis=1) for c in coef]
    for k in range(x0.shape[0] // SUB):
        t = tile(k)
        out[t, :] = x0[t, :] + (wide[0] * y0[t, :] + wide[1] * y1[t, :] + wide[2] * y2[t, :])


def shards(
    base_rhs,
    depth,
    ssh_prev,
    currents,
    land_blocks,
    ice_thick,
    ice_blocks,
    ice_vel,
    ice_stress,
    wind,
):
    groups = lax.axis_size("grp")
    tiles = lax.axis_size("tile")
    assert groups == 4
    g = lax.axis_index("grp").astype(jnp.int32).reshape(1)
    rows, cols = base_rhs.shape
    ice_rows = ice_thick.shape[1]
    assert rows == groups * ice_rows
    slab = ice_rows + 2 * SUB
    wide = cols + LANES

    strip = (2 * slab, cols)
    a, b, c, d = call(
        pack_rows, "pack_rows",
        [strip] * 4,
        [g, base_rhs, depth, ssh_prev, currents, land_blocks, ice_thick, ice_blocks, ice_vel, ice_stress, wind],
        scratch=[
            (2, 2, SUB, cols), (2, SUB, cols),
            (land_blocks.shape, jnp.int32), (ice_blocks.shape, jnp.int32),
        ],
        sems=48,
        hbm=True,
    )
    gf, h = call(
        masks, "masks",
        [(rows, cols), (2, ice_rows, cols)],
        [g, depth, land_blocks, ice_thick, ice_blocks],
        flops=10000000,
    )
    rc = lax.ppermute(c, "grp", [(0, 3), (3, 0), (1, 2), (2, 1)])
    ra = lax.ppermute(a, "grp", [(0, 1), (1, 0), (2, 3), (3, 2)])
    rb = lax.ppermute(b, "grp", [(0, 2), (3, 1)])
    rd = lax.ppermute(d, "grp", [(0, 1), (3, 2)])

    ice_tiles = 2 * NEXT * (slab // SUB)
    ocean_rows = rows + 2 * SUB
    count = ice_tiles + NOC * (ocean_rows // SUB)
    packed = (-(-count // SLOTS) * SUB, LANES)
    ice, ocean, left, right = call(
        pack_cols, "pack_cols",
        [(2, NEXT, slab, cols), (NOC, ocean_rows, cols), packed, packed],
        [g, ra, rb, rc, rd, currents, h, ice_vel, ice_stress, wind, base_rhs, gf, ssh_prev],
    )
    from_left = lax.ppermute(right, "tile", [(i, i + 1) for i in range(tiles - 1)])
    from_right = lax.ppermute(left, "tile", [(i + 1, i) for i in range(tiles - 1)])

    back = (ice_rows + SUB, wide)
    velocity, stress, p1, p2, p3, mine = call(
        ice_steps, "ice_steps",
        [ice_vel.shape, ice_stress.shape, back, back, back, back],
        [g, ice, from_left, from_right],
        scratch=[(2, cols // LANES + 1, slab + 2 * SUB, LANES)] * 16,
        mib=32,
    )
    r1 = lax.ppermute(p1, "grp", [(1, 0), (2, 3), (3, 1), (0, 2)])
    r2 = lax.ppermute(p2, "grp", [(2, 0), (1, 3)])
    r3 = lax.ppermute(p3, "grp", [(3, 0), (0, 3)])

    field = (ocean_rows, wide)
    padded = (ocean_rows + 2 * SUB, wide)
    gw, invd, known = call(
        functools.partial(ocean_before, ice_tiles), "ocean_before",
        [field] * 3,
        [g, ocean, from_left, from_right],
        scratch=[padded, padded, field, field],
        flops=20000000,
    )
    y0, y1, y2, sums = call(
        ocean_basis, "ocean_basis",
        [(rows, cols)] * 3 + [(SUB, LANES)],
        [g, gw, invd, known, r1, r2, r3, mine],
        scratch=[field, padded, padded, padded],
    )
    devices = groups * tiles
    shared = lax.all_to_all(
        jnp.broadcast_to(sums[None], (devices, SUB, LANES)), ("grp", "tile"), 0, 0, tiled=True
    )
    (ssh,) = call(combine, "combine", [(rows, cols)], [g, shared, ssh_prev, y0, y1, y2])
    return ssh, velocity, stress


def solution(mesh):
    return jax.shard_map(
        shards,
        mesh=mesh,
        in_specs=(
            P("grp", "tile"),
            P("grp", "tile"),
            P("grp", "tile"),
            P(None, "grp", "tile"),
            P("grp", "tile"),
            P(None, "grp", "tile"),
            P(None, "grp", "tile"),
            P(None, None, "grp", "tile"),
            P(None, None, "grp", "tile"),
            P(None, None, "grp", "tile"),
        ),
        out_specs=(P("grp", "tile"), P(None, None, "grp", "tile"), P(None, None, "grp", "tile")),
        check_vma=False,
    )
```

```python
import functools

import jax
import jax.numpy as jnp
from jax import lax
from jax.experimental import pallas as pl
from jax.experimental.pallas import tpu as pltpu
from jax.sharding import PartitionSpec as P

BS = 8
NSUB = 8
ITERS = 3

DAMP = 0.05
RELAX = 0.2
STRENGTH = 0.5
DRAG = 1.0
STEP = 0.5

F32 = jnp.float32
SUB = 8
LANES = 128
EDGE = 16
SLOTS = LANES // EDGE
GROUP = 4
SKEW = 1
NICE = 8
NEXT = NICE + 2
NOC = 3


def vmem():
    return pl.BlockSpec(memory_space=pltpu.VMEM)


def smem():
    return pl.BlockSpec(memory_space=pltpu.SMEM)


def call(body, name, outs, ins, scratch=(), sems=0, hbm=False, mib=24, flops=1000000):
    shapes = tuple(jax.ShapeDtypeStruct(s, F32) for s in outs)
    other = pl.BlockSpec(memory_space=pltpu.HBM) if hbm else vmem()
    specs = [smem() if i == 0 else other for i in range(len(ins))]
    held = [pltpu.VMEM(*s) if isinstance(s[0], tuple) else pltpu.VMEM(s, F32) for s in scratch]
    if sems:
        held.append(pltpu.SemaphoreType.DMA((sems,)))
    return pl.pallas_call(
        body,
        name=name,
        out_shape=shapes,
        in_specs=specs,
        out_specs=tuple(vmem() for _ in outs),
        scratch_shapes=held,
        cost_estimate=pl.CostEstimate(flops=flops, bytes_accessed=4000000, transcendentals=0),
        compiler_params=pltpu.CompilerParams(vmem_limit_bytes=mib * 1024 * 1024),
    )(*([ins[0]] + [pltpu.with_memory_space_constraint(x, pltpu.HBM) for x in ins[1:]] if hbm else ins))


def tile(k):
    return slice(k * SUB, k * SUB + SUB)


def expanded_cols(blocks):
    count = blocks.shape[-1]
    row = lax.broadcasted_iota(jnp.int32, (count, count * BS), 0) * BS
    col = lax.broadcasted_iota(jnp.int32, (count, count * BS), 1)
    spread = ((col >= row) & (col < row + BS)).astype(F32)
    return jnp.dot(blocks.astype(F32), spread, preferred_element_type=F32)


def row_iota(cols):
    return lax.broadcasted_iota(jnp.int32, (SUB, cols), 0)


def lane_iota():
    return lax.broadcasted_iota(jnp.int32, (SUB, LANES), 1)


def from_next_row(here, after, row):
    return pltpu.roll(jnp.where(row == 0, after, here), SUB - 1, 0)


def from_prev_row(here, before, row):
    return pltpu.roll(jnp.where(row == SUB - 1, before, here), 1, 0)


def from_next_col(here):
    return pltpu.roll(here, here.shape[1] - 1, 1)


def from_prev_col(here):
    return pltpu.roll(here, 1, 1)


def own_tile(cur, comp, first, j):
    last = cur.shape[1] // SUB - 1
    t = jnp.clip(first + j, 0, last)
    return cur[comp, pl.ds(pl.multiple_of(t * SUB, SUB), SUB), :]


def pack_rows(g_ref, base, depth, x0, cur, land, thick, iceb, vel, stress, wind,
              a, b, c, d, thick_s, depth_s, land_s, iceb_s, sems):
    g = g_ref[0]
    rows, cols = base.shape
    ice_rows = thick.shape[1]
    slab = ice_rows + 2 * SUB

    def run(slabs, halos):
        copies = []

        def copy(src, dst):
            made = pltpu.make_async_copy(src, dst, sems.at[len(copies)])
            made.start()
            copies.append(made)

        for out, dest in slabs:
            start = ice_rows * dest - SUB
            first, last = max(start, 0), min(start + slab, rows)
            for comp in range(2):
                at = comp * slab + first - start
                copy(cur.at[comp, first:last, :], out.at[at : at + last - first, :])
                if first > start:
                    out[comp * slab : at, :] = jnp.zeros((first - start, cols), F32)
                if last < start + slab:
                    out[at + last - first : (comp + 1) * slab, :] = jnp.zeros((start + slab - last, cols), F32)
        if halos:
            copy(land, land_s)
            copy(iceb, iceb_s)
        for i, (out, last) in enumerate(halos):
            r = slice(ice_rows - SUB, ice_rows) if last else slice(0, SUB)
            ro = slice(rows - SUB, rows) if last else slice(0, SUB)
            for cap in range(2):
                copy(thick.at[cap, r, :], thick_s.at[i, cap])
                n = cap * NICE + 1
                pieces = [vel.at[0, cap, r, :], vel.at[1, cap, r, :]]
                pieces += [stress.at[k, cap, r, :] for k in range(3)]
                pieces += [wind.at[k, cap, r, :] for k in range(2)]
                for piece in pieces:
                    copy(piece, out.at[tile(n), :])
                    n += 1
            copy(depth.at[ro, :], depth_s.at[i])
            copy(base.at[ro, :], out.at[tile(2 * NICE), :])
            copy(x0.at[ro, :], out.at[tile(2 * NICE + 2), :])
            out[tile(2 * NICE + 3), :] = jnp.zeros((SUB, cols), F32)
        for made in copies:
            made.wait()
        if halos:
            wet = expanded_cols(land_s[...])
            covers = [expanded_cols(iceb_s[cap]) for cap in range(2)]
        for i, (out, last) in enumerate(halos):
            for cap in range(2):
                k = covers[cap].shape[0] - 1 if last else 0
                out[tile(cap * NICE), :] = thick_s[i, cap] * covers[cap][k : k + 1, :]
            k = wet.shape[0] - 1 if last else 0
            out[tile(2 * NICE + 1), :] = depth_s[i] * wet[k : k + 1, :]

    @pl.when(g == 0)
    def _():
        run([(c, 3), (a, 1), (b, 2)], [(d, True)])

    @pl.when(g == 3)
    def _():
        run([(c, 0), (a, 2), (b, 1)], [(d, False)])

    @pl.when(g == 1)
    def _():
        run([], [(a, False), (c, True)])

    @pl.when(g == 2)
    def _():
        run([], [(a, True), (c, False)])


def masks(g_ref, depth, land, thick, iceb, gf, h):
    wet = expanded_cols(land[...])
    for k in range(depth.shape[0] // SUB):
        gf[tile(k), :] = depth[tile(k), :] * wet[k : k + 1, :]
    for cap in range(2):
        cover = expanded_cols(iceb[cap])
        for k in range(thick.shape[1] // SUB):
            h[cap, tile(k), :] = thick[cap, tile(k), :] * cover[k : k + 1, :]


def pack_cols(g_ref, ra, rb, rc, rd, cur, h, vel, stress, wind, base, gf, x0, ice, ocean, left, right):
    g = g_ref[0]
    cols = base.shape[1]
    slab_tiles = h.shape[1] // SUB
    ext = slab_tiles + 2
    rows = base.shape[0] // SUB
    lane = lane_iota()
    slot = lane // EDGE
    zero = jnp.zeros((SUB, cols), F32)
    state = {"n": 0, "l": None, "r": None}

    def emit(value):
        n = state["n"]
        s = n % SLOTS
        both = jnp.where(lane < EDGE, value[:, :LANES], value[:, cols - LANES :])
        both = pltpu.roll(both, EDGE * s, 1) if s else both
        before = (s - 1) % SLOTS
        if s == 0:
            state["l"] = state["r"] = both
        else:
            state["l"] = jnp.where(slot == s, both, state["l"])
            state["r"] = jnp.where(slot == before, both, state["r"])
        if s == SLOTS - 1:
            k = n // SLOTS
            left[tile(k), :] = state["l"]
            right[tile(k), :] = state["r"]
        state["n"] = n + 1

    def low(k):
        r = tile(k)
        return jnp.where(g == 1, rd[r, :], jnp.where(g == 2, rc[r, :], jnp.where(g == 3, ra[r, :], zero)))

    def high(k):
        r = tile(k)
        return jnp.where(g == 0, ra[r, :], jnp.where(g == 1, rc[r, :], jnp.where(g == 2, rd[r, :], zero)))

    for cap in range(2):
        own = [h.at[cap], vel.at[0, cap], vel.at[1, cap], stress.at[0, cap], stress.at[1, cap],
               stress.at[2, cap], wind.at[0, cap], wind.at[1, cap]]
        for f in range(NICE):
            for j in range(ext):
                if j == 0:
                    value = low(cap * NICE + f)
                elif j == ext - 1:
                    value = high(cap * NICE + f)
                else:
                    value = own[f][tile(j - 1), :]
                ice[cap, f, tile(j), :] = value
                emit(value)
        for comp in range(2):
            for j in range(ext):
                r = tile(comp * ext + j)
                mine = own_tile(cur, comp, slab_tiles * g - 1, j)
                if cap == 0:
                    value = jnp.where(g == 0, mine, jnp.where(g == 1, ra[r, :], jnp.where(g == 2, rb[r, :], rc[r, :])))
                else:
                    value = jnp.where(g == 3, mine, jnp.where(g == 2, ra[r, :], jnp.where(g == 1, rb[r, :], rc[r, :])))
                ice[cap, NICE + comp, tile(j), :] = value
                emit(value)
    for i, field in enumerate((base, gf, x0)):
        for j in range(rows + 2):
            if j == 0:
                value = low(2 * NICE + i)
            elif j == rows + 1:
                value = high(2 * NICE + i)
            else:
                value = field[tile(j - 1), :]
            ocean[i, tile(j), :] = value
            emit(value)
    while state["n"] % SLOTS:
        emit(zero)


def outer_columns(from_left, from_right, n, lane):
    s, k = n % SLOTS, n // SLOTS
    both = jnp.where(lane // EDGE == s, from_right[tile(k), :], from_left[tile(k), :])
    both = pltpu.roll(both, LANES - EDGE * s, 1) if s else both
    return jnp.where((lane < EDGE) | (lane >= LANES - EDGE), both, 0.0)


def split(value):
    return [value[:, c * LANES : (c + 1) * LANES] for c in range(value.shape[1] // LANES)]


def turned_next(regs, lane):
    n = len(regs)
    return [pltpu.roll(jnp.where(lane == 0, regs[(c + 1) % n], regs[c]), LANES - 1, 1) for c in range(n)]


def turned_prev(regs, lane):
    n = len(regs)
    return [pltpu.roll(jnp.where(lane == LANES - 1, regs[c - 1], regs[c]), 1, 1) for c in range(n)]


def ice_steps(g_ref, ice, from_left, from_right, vel_out, stress_out, p1, p2, p3, mine,
              u_s, v_s, p_s, q_s, s_s, un_s, vn_s, qp_s, sp_s, a_s, m_s, w_s, fx_s, fy_s, f0_s, f1_s):
    g = g_ref[0]
    cols = ice.shape[3]
    regs = cols // LANES + 1
    ext = ice.shape[2] // SUB
    lane = lane_iota()
    zero = jnp.zeros((SUB, LANES), F32)
    keep = 1.0 / (1.0 + RELAX)

    def at(j, shift=0):
        return slice(SUB * (j + 1) + shift, SUB * (j + 2) + shift)

    for cap in range(2):
        for c in range(regs):
            for ref in (p_s, s_s):
                ref[cap, c, at(-1), :] = zero
            for ref in (u_s, v_s):
                ref[cap, c, at(ext), :] = zero
        outers = []
        for j in range(ext):
            if j % GROUP == 0:
                outers = [
                    [outer_columns(from_left, from_right, (cap * NEXT + f) * ext + i, lane) for f in range(NEXT)]
                    for i in range(j, min(j + GROUP, ext))
                ]
            fields = [split(ice[cap, f, tile(j), :]) + [outers[j % GROUP][f]] for f in range(NEXT)]
            for c in range(regs):
                hh, u, v, s0, s1, s2, w0, w1, f0, f1 = (f[c] for f in fields)
                u_s[cap, c, at(j), :] = u
                v_s[cap, c, at(j), :] = v
                p_s[cap, c, at(j), :] = 0.5 * (s0 + s1)
                q_s[cap, c, at(j), :] = 0.5 * (s0 - s1)
                s_s[cap, c, at(j), :] = s2
                inv = jnp.where(hh > 0.0, 1.0 / (hh + (1.0 + STEP * DRAG)), 0.0)
                quick = STEP * inv
                a_s[cap, c, at(j), :] = hh * (RELAX * STRENGTH * keep)
                m_s[cap, c, at(j), :] = (hh + 1.0) * inv
                w_s[cap, c, at(j), :] = quick
                fx_s[cap, c, at(j), :] = quick * (w0 + DRAG * f0)
                fy_s[cap, c, at(j), :] = quick * (w1 + DRAG * f1)
                f0_s[cap, c, at(j), :] = f0
                f1_s[cap, c, at(j), :] = f1
    for j in range(ext):
        for cap in range(2):
            for ref, source in ((un_s, u_s), (vn_s, v_s)):
                turned = turned_next([source[cap, c, at(j), :] for c in range(regs)], lane)
                for c in range(regs):
                    ref[cap, c, at(j), :] = turned[c]

    def stress_tile(cap, j):
        qs, ss = [], []
        for c in range(regs):
            u, v = u_s[cap, c, at(j), :], v_s[cap, c, at(j), :]
            ux = u_s[cap, c, at(j, 1), :] - u
            vx = v_s[cap, c, at(j, 1), :] - v
            uy = un_s[cap, c, at(j), :] - u
            vy = vn_s[cap, c, at(j), :] - v
            es = uy + vx
            half = ux * ux + vy * vy
            a = a_s[cap, c, at(j), :]
            ratio = a * lax.rsqrt((half + half) + (es * es + 1.0))
            low = 0.5 * a
            q = q_s[cap, c, at(j), :] * keep + (ratio * vy - low)
            s = s_s[cap, c, at(j), :] * keep + ratio * es
            p_s[cap, c, at(j), :] = p_s[cap, c, at(j), :] * keep + (ratio * ux - low)
            q_s[cap, c, at(j), :] = q
            s_s[cap, c, at(j), :] = s
            qs.append(q)
            ss.append(s)
        for ref, turned in ((qp_s, turned_prev(qs, lane)), (sp_s, turned_prev(ss, lane))):
            for c in range(regs):
                ref[cap, c, at(j), :] = turned[c]

    def velocity_tile(cap, j):
        us, vs = [], []
        for c in range(regs):
            s = s_s[cap, c, at(j), :]
            force_x = (p_s[cap, c, at(j), :] - p_s[cap, c, at(j, -1), :]) + (s - sp_s[cap, c, at(j), :])
            force_y = (q_s[cap, c, at(j), :] - qp_s[cap, c, at(j), :]) + (s - s_s[cap, c, at(j, -1), :])
            m, quick = m_s[cap, c, at(j), :], w_s[cap, c, at(j), :]
            u = m * u_s[cap, c, at(j), :] + (quick * force_x + fx_s[cap, c, at(j), :])
            v = m * v_s[cap, c, at(j), :] + (quick * force_y + fy_s[cap, c, at(j), :])
            u_s[cap, c, at(j), :] = u
            v_s[cap, c, at(j), :] = v
            us.append(u)
            vs.append(v)
        for ref, turned in ((un_s, turned_next(us, lane)), (vn_s, turned_next(vs, lane))):
            for c in range(regs):
                ref[cap, c, at(j), :] = turned[c]

    def subcycle(_, carry):
        for j in range(ext + SKEW):
            for cap in range(2):
                if j < ext:
                    stress_tile(cap, j)
                if j >= SKEW:
                    velocity_tile(cap, j - SKEW)
        return carry

    lax.fori_loop(0, NSUB, subcycle, 0)
    spreads = []
    for cap in range(2):
        for c in range(regs):
            q_s[cap, c, at(0), :] = zero
            q_s[cap, c, at(ext - 1), :] = zero
        parts = []
        across = [[zero] * regs]
        for j in range(1, ext - 1):
            d1s = []
            for c in range(regs):
                u, v = u_s[cap, c, at(j), :], v_s[cap, c, at(j), :]
                p, q = p_s[cap, c, at(j), :], q_s[cap, c, at(j), :]
                if c + 1 < regs:
                    block = (tile(j - 1), slice(c * LANES, (c + 1) * LANES))
                    vel_out[(0, cap) + block] = u
                    vel_out[(1, cap) + block] = v
                    stress_out[(0, cap) + block] = p + q
                    stress_out[(1, cap) + block] = p - q
                    stress_out[(2, cap) + block] = s_s[cap, c, at(j), :]
                iced = m_s[cap, c, at(j), :] > 0.0
                q_s[cap, c, at(j), :] = jnp.where(iced, DRAG * (u - f0_s[cap, c, at(j), :]), 0.0)
                d1s.append(jnp.where(iced, DRAG * (v - f1_s[cap, c, at(j), :]), 0.0))
            turned = turned_prev(d1s, lane)
            across.append([d1s[c] - turned[c] for c in range(regs)])
        across.append([zero] * regs)
        for j in range(1, ext):
            parts.append([
                (q_s[cap, c, at(j), :] - q_s[cap, c, at(j, -1), :]) + across[j][c] for c in range(regs)
            ])
        spreads.append(parts)
    for k, (norths, souths) in enumerate(zip(*spreads)):
        for c, (north, south) in enumerate(zip(norths, souths)):
            block = (tile(k), slice(c * LANES, (c + 1) * LANES))
            p1[block] = jnp.where((g == 1) | (g == 3), north, south)
            p2[block] = jnp.where(g == 2, north, south)
            p3[block] = jnp.where(g == 3, north, south)
            mine[block] = jnp.where(g == 0, north, south)


def neighbour_sum(ref, k, row):
    here, before, after = ref[tile(k), :], ref[tile(k - 1), :], ref[tile(k + 1), :]
    along = from_prev_row(here, before, row) + from_next_row(here, after, row)
    return along + (from_prev_col(here) + from_next_col(here))


def ocean_before(first, g_ref, ocean, from_left, from_right, gw, invd, ra, g_s, gx_s, x_s, b_s):
    cols = ocean.shape[2]
    wide = cols + LANES
    ext = ocean.shape[1] // SUB
    lane = lane_iota()
    row = row_iota(wide)
    zero = jnp.zeros((SUB, wide), F32)
    for ref in (g_s, gx_s):
        ref[tile(0), :] = zero
        ref[tile(ext + 1), :] = zero
    for j in range(ext):
        t = tile(j + 1)

        def field(i):
            outer = outer_columns(from_left, from_right, first + i * ext + j, lane)
            return jnp.concatenate([ocean[i, tile(j), :], outer], axis=1)

        b_s[tile(j), :] = field(0)
        depth = field(1)
        x = field(2)
        g_s[t, :] = depth
        gx_s[t, :] = depth * x
        x_s[tile(j), :] = x
        gw[tile(j), :] = depth
    for j in range(ext):
        t = tile(j)
        depth = g_s[tile(j + 1), :]
        diag = DAMP + depth * neighbour_sum(g_s, j + 1, row)
        invd[t, :] = 1.0 / diag
        around = depth * neighbour_sum(gx_s, j + 1, row)
        ra[t, :] = jnp.where(depth > 0.0, b_s[t, :], 0.0) - (diag * x_s[t, :] - around)


def ocean_basis(g_ref, gw, invd, ra, r1, r2, r3, mine, y0_out, y1_out, y2_out, sums,
                sp, u0_s, u1_s, u2_s):
    g = g_ref[0]
    wide = gw.shape[1]
    ext = gw.shape[0] // SUB
    cols = y0_out.shape[1]
    slab = r1.shape[0] // SUB - 1
    row = row_iota(wide)
    zero = jnp.zeros((SUB, wide), F32)
    for ref in (u0_s, u1_s, u2_s):
        ref[tile(0), :] = zero
        ref[tile(ext + 1), :] = zero

    def clear(which):
        for j in which:
            sp[tile(j), :] = zero

    def whole(slabs):
        clear([0])
        for k, ref in enumerate(slabs):
            for t in range(slab):
                value = ref[tile(t), :]
                if t == 0 and k > 0:
                    value = value + slabs[k - 1][tile(slab), :]
                sp[tile(1 + slab * k + t), :] = value
        sp[tile(1 + slab * len(slabs)), :] = slabs[-1][tile(slab), :]

    @pl.when(g == 0)
    def _():
        whole([mine, r1, r2, r3])

    @pl.when(g == 3)
    def _():
        whole([r3, r2, r1, mine])

    @pl.when(g == 1)
    def _():
        clear(range(2, ext))
        sp[tile(0), :] = r1[tile(slab - 1), :]
        sp[tile(1), :] = r1[tile(slab), :]

    @pl.when(g == 2)
    def _():
        clear(range(ext - 1))
        sp[tile(ext - 1), :] = r1[tile(0), :]

    acc = [jnp.zeros((SUB, cols), F32) for _ in range(6)]

    def add(k, left, right, j):
        if 0 < j < ext - 1:
            acc[k] = acc[k] + left[:, :cols] * right[:, :cols]

    for j in range(ext):
        t = tile(j)
        depth = gw[t, :]
        r0 = ra[t, :] + jnp.where(depth > 0.0, sp[t, :], 0.0)
        y0 = r0 * invd[t, :]
        u0_s[tile(j + 1), :] = depth * y0
        if 0 < j < ext - 1:
            y0_out[tile(j - 1), :] = y0[:, :cols]
        add(0, r0, y0, j)
    for j in range(ext):
        t = tile(j)
        depth = gw[t, :]
        w = depth * neighbour_sum(u0_s, j + 1, row)
        y1 = w * invd[t, :]
        u1_s[tile(j + 1), :] = depth * y1
        if 0 < j < ext - 1:
            y1_out[tile(j - 1), :] = y1[:, :cols]
            acc[1] = acc[1] + y0_out[tile(j - 1), :] * w[:, :cols]
        add(2, w, y1, j)
    for j in range(ext):
        t = tile(j)
        depth = gw[t, :]
        w = depth * neighbour_sum(u1_s, j + 1, row)
        y2 = w * invd[t, :]
        u2_s[tile(j + 1), :] = depth * y2
        if 0 < j < ext - 1:
            y2_out[tile(j - 1), :] = y2[:, :cols]
            acc[3] = acc[3] + y1_out[tile(j - 1), :] * w[:, :cols]
        add(4, w, y2, j)
    for j in range(1, ext - 1):
        w = neighbour_sum(u2_s, j + 1, row)[:, :cols] * u2_s[tile(j + 1), :][:, :cols]
        acc[5] = acc[5] + w
    for k in range(6):
        total = acc[k][:, :LANES]
        for c in range(1, cols // LANES):
            total = total + acc[k][:, c * LANES : (c + 1) * LANES]
        sums[k : k + 1, :] = jnp.sum(total, axis=0, keepdims=True)
    sums[6:8, :] = jnp.zeros((2, LANES), F32)


def combine(g_ref, parts, x0, y0, y1, y2, out):
    total = jnp.sum(jnp.sum(parts[...], axis=0), axis=1, keepdims=True)
    total = jnp.broadcast_to(total, (SUB, LANES))
    m = [jnp.broadcast_to(total[k : k + 1, :], (SUB, LANES)) for k in range(6)]

    def dot(left, right, image):
        value = None
        for i, a in enumerate(left):
            for j, b in enumerate(right):
                moment = m[i + j] - m[i + j + 1] if image else m[i + j]
                term = a * b * moment
                value = term if value is None else value + term
        return value

    z = [jnp.ones((SUB, LANES), F32)]
    p = z
    rz = m[0]
    coef = [0.0, 0.0, 0.0]
    for step in range(ITERS):
        alpha = rz / dot(p, p, True)
        for i, a in enumerate(p):
            coef[i] = coef[i] + alpha * a
        if step + 1 < ITERS:
            image = [a for a in p] + [jnp.zeros((SUB, LANES), F32)]
            for i, a in enumerate(p):
                image[i + 1] = image[i + 1] - a
            z = [(z[i] if i < len(z) else 0.0) - alpha * image[i] for i in range(len(image))]
            fresh = dot(z, z, False)
            beta = fresh / rz
            p = [z[i] + beta * p[i] if i < len(p) else z[i] for i in range(len(z))]
            rz = fresh
    reps = x0.shape[1] // LANES
    wide = [jnp.concatenate([c] * reps, axis=1) for c in coef]
    for k in range(x0.shape[0] // SUB):
        t = tile(k)
        out[t, :] = x0[t, :] + (wide[0] * y0[t, :] + wide[1] * y1[t, :] + wide[2] * y2[t, :])


def shards(
    base_rhs,
    depth,
    ssh_prev,
    currents,
    land_blocks,
    ice_thick,
    ice_blocks,
    ice_vel,
    ice_stress,
    wind,
):
    groups = lax.axis_size("grp")
    tiles = lax.axis_size("tile")
    assert groups == 4
    g = lax.axis_index("grp").astype(jnp.int32).reshape(1)
    rows, cols = base_rhs.shape
    ice_rows = ice_thick.shape[1]
    assert rows == groups * ice_rows
    slab = ice_rows + 2 * SUB
    wide = cols + LANES

    strip = (2 * slab, cols)
    a, b, c, d = call(
        pack_rows, "pack_rows",
        [strip] * 4,
        [g, base_rhs, depth, ssh_prev, currents, land_blocks, ice_thick, ice_blocks, ice_vel, ice_stress, wind],
        scratch=[
            (2, 2, SUB, cols), (2, SUB, cols),
            (land_blocks.shape, jnp.int32), (ice_blocks.shape, jnp.int32),
        ],
        sems=48,
        hbm=True,
    )
    gf, h = call(
        masks, "masks",
        [(rows, cols), (2, ice_rows, cols)],
        [g, depth, land_blocks, ice_thick, ice_blocks],
        flops=10000000,
    )
    rc = lax.ppermute(c, "grp", [(0, 3), (3, 0), (1, 2), (2, 1)])
    ra = lax.ppermute(a, "grp", [(0, 1), (1, 0), (2, 3), (3, 2)])
    rb = lax.ppermute(b, "grp", [(0, 2), (3, 1)])
    rd = lax.ppermute(d, "grp", [(0, 1), (3, 2)])

    ice_tiles = 2 * NEXT * (slab // SUB)
    ocean_rows = rows + 2 * SUB
    count = ice_tiles + NOC * (ocean_rows // SUB)
    packed = (-(-count // SLOTS) * SUB, LANES)
    ice, ocean, left, right = call(
        pack_cols, "pack_cols",
        [(2, NEXT, slab, cols), (NOC, ocean_rows, cols), packed, packed],
        [g, ra, rb, rc, rd, currents, h, ice_vel, ice_stress, wind, base_rhs, gf, ssh_prev],
    )
    from_left = lax.ppermute(right, "tile", [(i, i + 1) for i in range(tiles - 1)])
    from_right = lax.ppermute(left, "tile", [(i + 1, i) for i in range(tiles - 1)])

    back = (ice_rows + SUB, wide)
    velocity, stress, p1, p2, p3, mine = call(
        ice_steps, "ice_steps",
        [ice_vel.shape, ice_stress.shape, back, back, back, back],
        [g, ice, from_left, from_right],
        scratch=[(2, cols // LANES + 1, slab + 2 * SUB, LANES)] * 16,
        mib=32,
    )
    r1 = lax.ppermute(p1, "grp", [(1, 0), (2, 3), (3, 1), (0, 2)])
    r2 = lax.ppermute(p2, "grp", [(2, 0), (1, 3)])
    r3 = lax.ppermute(p3, "grp", [(3, 0), (0, 3)])

    field = (ocean_rows, wide)
    padded = (ocean_rows + 2 * SUB, wide)
    gw, invd, known = call(
        functools.partial(ocean_before, ice_tiles), "ocean_before",
        [field] * 3,
        [g, ocean, from_left, from_right],
        scratch=[padded, padded, field, field],
        flops=20000000,
    )
    y0, y1, y2, sums = call(
        ocean_basis, "ocean_basis",
        [(rows, cols)] * 3 + [(SUB, LANES)],
        [g, gw, invd, known, r1, r2, r3, mine],
        scratch=[field, padded, padded, padded],
    )
    devices = groups * tiles
    shared = lax.all_to_all(
        jnp.broadcast_to(sums[None], (devices, SUB, LANES)), ("grp", "tile"), 0, 0, tiled=True
    )
    (ssh,) = call(combine, "combine", [(rows, cols)], [g, shared, ssh_prev, y0, y1, y2])
    return ssh, velocity, stress


def solution(mesh):
    return jax.shard_map(
        shards,
        mesh=mesh,
        in_specs=(
            P("grp", "tile"),
            P("grp", "tile"),
            P("grp", "tile"),
            P(None, "grp", "tile"),
            P("grp", "tile"),
            P(None, "grp", "tile"),
            P(None, "grp", "tile"),
            P(None, None, "grp", "tile"),
            P(None, None, "grp", "tile"),
            P(None, None, "grp", "tile"),
        ),
        out_specs=(P("grp", "tile"), P(None, None, "grp", "tile"), P(None, None, "grp", "tile")),
        check_vma=False,
    )
```

```python
import jax
import jax.numpy as jnp
from jax import lax
from jax.experimental import pallas as pl
from jax.experimental.pallas import tpu as pltpu
from jax.sharding import PartitionSpec as P


BS = 8
NSUB = 8
ITERS = 3

DAMP = 0.05
RELAX = 0.2
STRENGTH = 0.5
DRAG = 1.0
STEP = 0.5

F32 = jnp.float32
SUB = 8
LANES = 128
EDGE = 16
SLOTS = LANES // EDGE
WIDE_SLOTS = LANES // (2 * EDGE)
GROUP = 4
SKEW = 1
NICE = 8
NOC = 3


def vmem():
    return pl.BlockSpec(memory_space=pltpu.VMEM)


def smem():
    return pl.BlockSpec(memory_space=pltpu.SMEM)


def call(body, outs, ins, scratch=(), sems=0, hbm=False, mib=24, flops=1000000):
    shapes = tuple(jax.ShapeDtypeStruct(s, F32) for s in outs)
    other = pl.BlockSpec(memory_space=pltpu.HBM) if hbm else vmem()
    specs = [smem() if i == 0 else other for i in range(len(ins))]
    held = [pltpu.VMEM(*s) if isinstance(s[0], tuple) else pltpu.VMEM(s, F32) for s in scratch]
    if sems:
        held.append(pltpu.SemaphoreType.DMA((sems,)))
    return pl.pallas_call(
        body,
        out_shape=shapes,
        in_specs=specs,
        out_specs=tuple(vmem() for _ in outs),
        scratch_shapes=held,
        cost_estimate=pl.CostEstimate(flops=flops, bytes_accessed=4000000, transcendentals=0),
        compiler_params=pltpu.CompilerParams(vmem_limit_bytes=mib * 1024 * 1024),
    )(*([ins[0]] + [pltpu.with_memory_space_constraint(x, pltpu.HBM) for x in ins[1:]] if hbm else ins))


def tile(k):
    return slice(k * SUB, k * SUB + SUB)


def expanded_cols(blocks):
    count = blocks.shape[-1]
    row = lax.broadcasted_iota(jnp.int32, (count, count * BS), 0) * BS
    col = lax.broadcasted_iota(jnp.int32, (count, count * BS), 1)
    spread = ((col >= row) & (col < row + BS)).astype(F32)
    return jnp.dot(blocks.astype(F32), spread, preferred_element_type=F32)


def row_iota(cols):
    return lax.broadcasted_iota(jnp.int32, (SUB, cols), 0)


def lane_iota():
    return lax.broadcasted_iota(jnp.int32, (SUB, LANES), 1)


def from_next_row(here, after, row):
    return pltpu.roll(jnp.where(row == 0, after, here), SUB - 1, 0)


def from_prev_row(here, before, row):
    return pltpu.roll(jnp.where(row == SUB - 1, before, here), 1, 0)


def from_next_col(here):
    return pltpu.roll(here, here.shape[1] - 1, 1)


def from_prev_col(here):
    return pltpu.roll(here, 1, 1)


def own_tile(cur, comp, first, j):
    last = cur.shape[1] // SUB - 1
    t = jnp.clip(first + j, 0, last)
    return cur[comp, pl.ds(pl.multiple_of(t * SUB, SUB), SUB), :]


def pack_rows(g_ref, base, depth, x0, cur, land, thick, iceb, vel, stress, wind,
              c, a, b, token, thick_s, depth_s, land_s, iceb_s, sems):
    g = g_ref[0]
    rows, cols = base.shape
    ice_rows = thick.shape[1]
    slab = ice_rows + 2 * SUB
    token[...] = jnp.zeros((SUB, LANES), F32)

    def run(slabs, halos):
        copies = []

        def copy(src, dst):
            made = pltpu.make_async_copy(src, dst, sems.at[len(copies)])
            made.start()
            copies.append(made)

        for out, dest in slabs:
            start = ice_rows * dest - SUB
            first, last = max(start, 0), min(start + slab, rows)
            for comp in range(2):
                at = comp * slab + first - start
                copy(cur.at[comp, first:last, :], out.at[at : at + last - first, :])
                if first > start:
                    out[comp * slab : at, :] = jnp.zeros((first - start, cols), F32)
                if last < start + slab:
                    out[at + last - first : (comp + 1) * slab, :] = jnp.zeros((start + slab - last, cols), F32)
        if halos:
            copy(land, land_s)
            copy(iceb, iceb_s)
        for i, (out, last) in enumerate(halos):
            r = slice(ice_rows - SUB, ice_rows) if last else slice(0, SUB)
            ro = slice(rows - SUB, rows) if last else slice(0, SUB)
            for cap in range(2):
                copy(thick.at[cap, r, :], thick_s.at[i, cap])
                n = cap * NICE + 1
                pieces = [vel.at[0, cap, r, :], vel.at[1, cap, r, :]]
                pieces += [stress.at[k, cap, r, :] for k in range(3)]
                pieces += [wind.at[k, cap, r, :] for k in range(2)]
                for piece in pieces:
                    copy(piece, out.at[tile(n), :])
                    n += 1
            copy(depth.at[ro, :], depth_s.at[i])
            copy(base.at[ro, :], out.at[tile(2 * NICE), :])
            copy(x0.at[ro, :], out.at[tile(2 * NICE + 2), :])
            out[tile(2 * NICE + 3), :] = jnp.zeros((SUB, cols), F32)
        for made in copies:
            made.wait()
        if halos:
            wet = expanded_cols(land_s[...])
            covers = [expanded_cols(iceb_s[cap]) for cap in range(2)]
        for i, (out, last) in enumerate(halos):
            for cap in range(2):
                k = covers[cap].shape[0] - 1 if last else 0
                out[tile(cap * NICE), :] = thick_s[i, cap] * covers[cap][k : k + 1, :]
            k = wet.shape[0] - 1 if last else 0
            out[tile(2 * NICE + 1), :] = depth_s[i] * wet[k : k + 1, :]

    @pl.when(g == 0)
    def _():
        run([(c, 3), (a, 1), (b, 2)], [])

    @pl.when(g == 3)
    def _():
        run([(c, 0), (a, 2), (b, 1)], [])

    @pl.when(g == 1)
    def _():
        run([], [(a, False), (c, True)])

    @pl.when(g == 2)
    def _():
        run([], [(a, True), (c, False)])


def pack_own(g_ref, token, base, depth, x0, cur, land, thick, iceb, vel, stress, wind, gf, h, left, right):
    cols = base.shape[1]
    lane = lane_iota()
    slot = lane // EDGE
    state = {"n": 0, "l": None, "r": None}

    def emit(first, last):
        n = state["n"]
        s = n % SLOTS
        both = jnp.where(lane < EDGE, first, last)
        both = pltpu.roll(both, EDGE * s, 1) if s else both
        if s == 0:
            state["l"] = state["r"] = both
        else:
            state["l"] = jnp.where(slot == s, both, state["l"])
            state["r"] = jnp.where(slot == s - 1, both, state["r"])
        if s == SLOTS - 1:
            k = n // SLOTS
            left[tile(k), :] = state["l"]
            right[tile(k), :] = state["r"]
        state["n"] = n + 1

    def emit_all(ref):
        for k in range(ref.shape[0] // SUB):
            emit(ref[tile(k), :LANES], ref[tile(k), cols - LANES :])

    wet = expanded_cols(land[...])
    for k in range(depth.shape[0] // SUB):
        gf[tile(k), :] = depth[tile(k), :] * wet[k : k + 1, :]
    for cap in range(2):
        cover = expanded_cols(iceb[cap])
        for k in range(thick.shape[1] // SUB):
            h[cap, tile(k), :] = thick[cap, tile(k), :] * cover[k : k + 1, :]
    for cap in range(2):
        for ref in own_ice(h, vel, stress, wind, cap):
            emit_all(ref)
    for ref in (base, gf, x0):
        emit_all(ref)
    for comp in range(2):
        emit_all(cur.at[comp])
    while state["n"] % SLOTS:
        emit(jnp.zeros((SUB, LANES), F32), jnp.zeros((SUB, LANES), F32))


def own_ice(h, vel, stress, wind, cap):
    fields = [h.at[cap], vel.at[0, cap], vel.at[1, cap]]
    fields += [stress.at[i, cap] for i in range(3)]
    return fields + [wind.at[i, cap] for i in range(2)]


def own_count(rows, ice_rows):
    return 2 * NICE * (ice_rows // SUB), NOC * (rows // SUB), 2 * (rows // SUB)


def halo_tiles(rows, ice_rows, last):
    ice_tiles, ocean_tiles = ice_rows // SUB, rows // SUB
    picked = [n * ice_tiles + (ice_tiles - 1 if last else 0) for n in range(2 * NICE)]
    start = 2 * NICE * ice_tiles
    return picked + [start + i * ocean_tiles + (ocean_tiles - 1 if last else 0) for i in range(NOC)]


def pack_narrow(g_ref, from_left, from_right, h, gf, base, x0, vel, stress, wind, outer, narrow, d):
    g = g_ref[0]
    rows, cols = base.shape
    ice_rows = h.shape[1]
    lane = lane_iota()
    count = sum(own_count(rows, ice_rows))
    batch = 32
    for n in range(0, count, batch):
        made = [outer_columns(from_left, from_right, i, lane) for i in range(n, min(n + batch, count))]
        for i, value in enumerate(made):
            outer[tile(n + i), :] = value
    packed = narrow.shape[1] // SUB

    def pack(put, tiles):
        for k in range(packed):
            value = None
            for i in range(WIDE_SLOTS):
                n = k * WIDE_SLOTS + i
                if n < len(tiles):
                    one = tiles[n]()
                    one = pltpu.roll(one, i * 2 * EDGE, 1) if i else one
                    value = one if value is None else value + one
            put(k, jnp.zeros((SUB, LANES), F32) if value is None else value)

    def picked(n):
        return lambda: outer[tile(n), :]

    def slab(dest):
        start = sum(own_count(rows, ice_rows)[:2])
        per = rows // SUB
        tiles = []
        for comp in range(2):
            for j in range(ice_rows // SUB + 2):
                t = ice_rows // SUB * dest - 1 + j
                inside = 0 <= t < per
                tiles.append(picked(start + comp * per + t) if inside else lambda: jnp.zeros((SUB, LANES), F32))
        return tiles

    def halo(last):
        return [picked(n) for n in halo_tiles(rows, ice_rows, last)]

    def send(dest, tiles):
        def put(k, value):
            narrow[dest, tile(k), :] = value

        pack(put, tiles)

    def strip(last):
        r = slice(ice_rows - SUB, ice_rows) if last else slice(0, SUB)
        ro = slice(rows - SUB, rows) if last else slice(0, SUB)
        n = 0
        for cap in range(2):
            for ref in own_ice(h, vel, stress, wind, cap):
                d[tile(n), :] = ref[r, :]
                n += 1
        for ref in (base, gf, x0):
            d[tile(n), :] = ref[ro, :]
            n += 1
        per = cols // LANES

        def put(k, value):
            c = k % per
            d[tile(n + k // per), c * LANES : (c + 1) * LANES] = value

        pack(put, halo(last))

    @pl.when(g == 0)
    def _():
        send(0, [])
        send(1, slab(1))
        send(2, slab(2))
        send(3, slab(3))
        strip(True)

    @pl.when(g == 1)
    def _():
        send(0, halo(False))
        send(1, [])
        send(2, halo(True))
        send(3, [])

    @pl.when(g == 2)
    def _():
        send(0, [])
        send(1, halo(False))
        send(2, [])
        send(3, halo(True))

    @pl.when(g == 3)
    def _():
        send(0, slab(0))
        send(1, slab(1))
        send(2, slab(2))
        send(3, [])
        strip(False)


def wide_outer(value, i, lane):
    value = pltpu.roll(value, LANES - 2 * EDGE * i, 1) if i else value
    return jnp.where((lane < EDGE) | (lane >= LANES - EDGE), value, 0.0)


def low_high(g, ra, rc, rd, nx, n, lane, low):
    cols = ra.shape[1]
    inner_zero = jnp.zeros((SUB, cols), F32)
    k, i = n // WIDE_SLOTS, n % WIDE_SLOTS
    per = cols // LANES
    first = 2 * NICE + NOC
    tail = rd[tile(first + k // per), (k % per) * LANES : (k % per + 1) * LANES]
    t = tile(n)
    if low:
        inner = jnp.where(g == 1, rd[t, :], jnp.where(g == 2, rc[t, :], jnp.where(g == 3, ra[t, :], inner_zero)))
        packed = jnp.where(g == 1, tail, jnp.where(g == 2, nx[1, tile(k), :], jnp.where(g == 3, nx[2, tile(k), :], 0.0)))
    else:
        inner = jnp.where(g == 2, rd[t, :], jnp.where(g == 1, rc[t, :], jnp.where(g == 0, ra[t, :], inner_zero)))
        packed = jnp.where(g == 2, tail, jnp.where(g == 1, nx[2, tile(k), :], jnp.where(g == 0, nx[1, tile(k), :], 0.0)))
    return split(inner) + [wide_outer(packed, i, lane)]


def outer_columns(from_left, from_right, n, lane):
    s, k = n % SLOTS, n // SLOTS
    both = jnp.where(lane // EDGE == s, from_right[tile(k), :], from_left[tile(k), :])
    both = pltpu.roll(both, LANES - EDGE * s, 1) if s else both
    return jnp.where((lane < EDGE) | (lane >= LANES - EDGE), both, 0.0)


def split(value):
    return [value[:, c * LANES : (c + 1) * LANES] for c in range(value.shape[1] // LANES)]


def turned_next(regs, lane):
    n = len(regs)
    return [pltpu.roll(jnp.where(lane == 0, regs[(c + 1) % n], regs[c]), LANES - 1, 1) for c in range(n)]


def turned_prev(regs, lane):
    n = len(regs)
    return [pltpu.roll(jnp.where(lane == LANES - 1, regs[c - 1], regs[c]), 1, 1) for c in range(n)]


def ice_steps(g_ref, ra, rb, rc, rd, nx, outer, h, vel, stress, wind, cur,
              vel_out, stress_out, p3, p2, p1, mine,
              u_s, v_s, p_s, q_s, s_s, un_s, vn_s, qp_s, sp_s, a_s, m_s, w_s, fx_s, fy_s, f0_s, f1_s):
    g = g_ref[0]
    ice_rows, cols = h.shape[1:]
    rows = cur.shape[1]
    regs = cols // LANES + 1
    per = ice_rows // SUB
    ext = per + 2
    lane = lane_iota()
    zero = jnp.zeros((SUB, LANES), F32)
    keep = 1.0 / (1.0 + RELAX)
    flow_first = sum(own_count(rows, ice_rows)[:2])

    def at(j, shift=0):
        return slice(SUB * (j + 1) + shift, SUB * (j + 2) + shift)

    def flow(cap, comp, j):
        n = comp * ext + j
        t = tile(n)
        k, i = n // WIDE_SLOTS, n % WIDE_SLOTS
        here = jnp.clip(per * g - 1 + j, 0, rows // SUB - 1)
        own = own_tile(cur, comp, per * g - 1, j)
        spot = pl.multiple_of((flow_first + comp * (rows // SUB) + here) * SUB, SUB)
        own_outer = outer[pl.ds(spot, SUB), :]
        if cap == 0:
            inner = jnp.where(g == 0, own, jnp.where(g == 1, ra[t, :], jnp.where(g == 2, rb[t, :], rc[t, :])))
            edge = jnp.where(g == 0, own_outer, wide_outer(nx[0, tile(k), :], i, lane))
        else:
            inner = jnp.where(g == 3, own, jnp.where(g == 2, ra[t, :], jnp.where(g == 1, rb[t, :], rc[t, :])))
            edge = jnp.where(g == 3, own_outer, wide_outer(nx[3, tile(k), :], i, lane))
        return split(inner) + [edge]

    for cap in range(2):
        own = own_ice(h, vel, stress, wind, cap)
        for c in range(regs):
            for ref in (p_s, s_s):
                ref[cap, c, at(-1), :] = zero
            for ref in (u_s, v_s):
                ref[cap, c, at(ext), :] = zero
        flows = []
        for j in range(ext):
            if j % GROUP == 0:
                flows = [[flow(cap, comp, i) for comp in range(2)] for i in range(j, min(j + GROUP, ext))]
            if j == 0 or j == ext - 1:
                fields = [low_high(g, ra, rc, rd, nx, cap * NICE + f, lane, j == 0) for f in range(NICE)]
            else:
                fields = [
                    split(own[f][tile(j - 1), :]) + [outer[tile((cap * NICE + f) * per + j - 1), :]]
                    for f in range(NICE)
                ]
            fields = fields + flows[j % GROUP]
            for c in range(regs):
                hh, u, v, s0, s1, s2, w0, w1, f0, f1 = (f[c] for f in fields)
                u_s[cap, c, at(j), :] = u
                v_s[cap, c, at(j), :] = v
                p_s[cap, c, at(j), :] = 0.5 * (s0 + s1)
                q_s[cap, c, at(j), :] = 0.5 * (s0 - s1)
                s_s[cap, c, at(j), :] = s2
                inv = jnp.where(hh > 0.0, 1.0 / (hh + (1.0 + STEP * DRAG)), 0.0)
                quick = STEP * inv
                a_s[cap, c, at(j), :] = hh * (RELAX * STRENGTH * keep)
                m_s[cap, c, at(j), :] = (hh + 1.0) * inv
                w_s[cap, c, at(j), :] = quick
                fx_s[cap, c, at(j), :] = quick * (w0 + DRAG * f0)
                fy_s[cap, c, at(j), :] = quick * (w1 + DRAG * f1)
                f0_s[cap, c, at(j), :] = f0
                f1_s[cap, c, at(j), :] = f1
    for j in range(ext):
        for cap in range(2):
            for ref, source in ((un_s, u_s), (vn_s, v_s)):
                turned = turned_next([source[cap, c, at(j), :] for c in range(regs)], lane)
                for c in range(regs):
                    ref[cap, c, at(j), :] = turned[c]

    def stress_tile(cap, j):
        qs, ss = [], []
        for c in range(regs):
            u, v = u_s[cap, c, at(j), :], v_s[cap, c, at(j), :]
            ux = u_s[cap, c, at(j, 1), :] - u
            vx = v_s[cap, c, at(j, 1), :] - v
            uy = un_s[cap, c, at(j), :] - u
            vy = vn_s[cap, c, at(j), :] - v
            es = uy + vx
            half = ux * ux + vy * vy
            a = a_s[cap, c, at(j), :]
            ratio = a * lax.rsqrt((half + half) + (es * es + 1.0))
            low = 0.5 * a
            q = q_s[cap, c, at(j), :] * keep + (ratio * vy - low)
            s = s_s[cap, c, at(j), :] * keep + ratio * es
            p_s[cap, c, at(j), :] = p_s[cap, c, at(j), :] * keep + (ratio * ux - low)
            q_s[cap, c, at(j), :] = q
            s_s[cap, c, at(j), :] = s
            qs.append(q)
            ss.append(s)
        for ref, turned in ((qp_s, turned_prev(qs, lane)), (sp_s, turned_prev(ss, lane))):
            for c in range(regs):
                ref[cap, c, at(j), :] = turned[c]

    def velocity_tile(cap, j):
        us, vs = [], []
        for c in range(regs):
            s = s_s[cap, c, at(j), :]
            force_x = (p_s[cap, c, at(j), :] - p_s[cap, c, at(j, -1), :]) + (s - sp_s[cap, c, at(j), :])
            force_y = (q_s[cap, c, at(j), :] - qp_s[cap, c, at(j), :]) + (s - s_s[cap, c, at(j, -1), :])
            m, quick = m_s[cap, c, at(j), :], w_s[cap, c, at(j), :]
            u = m * u_s[cap, c, at(j), :] + (quick * force_x + fx_s[cap, c, at(j), :])
            v = m * v_s[cap, c, at(j), :] + (quick * force_y + fy_s[cap, c, at(j), :])
            u_s[cap, c, at(j), :] = u
            v_s[cap, c, at(j), :] = v
            us.append(u)
            vs.append(v)
        for ref, turned in ((un_s, turned_next(us, lane)), (vn_s, turned_next(vs, lane))):
            for c in range(regs):
                ref[cap, c, at(j), :] = turned[c]

    def subcycle(_, carry):
        for j in range(ext + SKEW):
            for cap in range(2):
                if j < ext:
                    stress_tile(cap, j)
                if j >= SKEW:
                    velocity_tile(cap, j - SKEW)
        return carry

    lax.fori_loop(0, NSUB, subcycle, 0)
    spreads = []
    for cap in range(2):
        for c in range(regs):
            q_s[cap, c, at(0), :] = zero
            q_s[cap, c, at(ext - 1), :] = zero
        parts = []
        across = [[zero] * regs]
        for j in range(1, ext - 1):
            d1s = []
            for c in range(regs):
                u, v = u_s[cap, c, at(j), :], v_s[cap, c, at(j), :]
                p, q = p_s[cap, c, at(j), :], q_s[cap, c, at(j), :]
                if c + 1 < regs:
                    block = (tile(j - 1), slice(c * LANES, (c + 1) * LANES))
                    vel_out[(0, cap) + block] = u
                    vel_out[(1, cap) + block] = v
                    stress_out[(0, cap) + block] = p + q
                    stress_out[(1, cap) + block] = p - q
                    stress_out[(2, cap) + block] = s_s[cap, c, at(j), :]
                iced = m_s[cap, c, at(j), :] > 0.0
                q_s[cap, c, at(j), :] = jnp.where(iced, DRAG * (u - f0_s[cap, c, at(j), :]), 0.0)
                d1s.append(jnp.where(iced, DRAG * (v - f1_s[cap, c, at(j), :]), 0.0))
            turned = turned_prev(d1s, lane)
            across.append([d1s[c] - turned[c] for c in range(regs)])
        across.append([zero] * regs)
        for j in range(1, ext):
            parts.append([
                (q_s[cap, c, at(j), :] - q_s[cap, c, at(j, -1), :]) + across[j][c] for c in range(regs)
            ])
        spreads.append(parts)
    bands = per + 1
    packs = [[None] * -(-bands // WIDE_SLOTS) for _ in range(2)]
    for cap in range(2):
        for k in range(bands):
            i = k % WIDE_SLOTS
            edge = jnp.where((lane < EDGE) | (lane >= LANES - EDGE), spreads[cap][k][regs - 1], 0.0)
            edge = pltpu.roll(edge, 2 * EDGE * i, 1) if i else edge
            held = packs[cap][k // WIDE_SLOTS]
            packs[cap][k // WIDE_SLOTS] = edge if held is None else held + edge

    def put(block, north, south):
        p3[block] = jnp.where(g == 3, north, south)
        p2[block] = jnp.where(g == 2, north, south)
        p1[block] = jnp.where((g == 1) | (g == 3), north, south)
        mine[block] = jnp.where(g == 0, north, south)

    for k in range(bands):
        for c in range(regs - 1):
            put((tile(k), slice(c * LANES, (c + 1) * LANES)), spreads[0][k][c], spreads[1][k][c])
    for c in range(regs - 1):
        pair = [pack[c] if c < len(pack) else zero for pack in packs]
        put((tile(bands), slice(c * LANES, (c + 1) * LANES)), *pair)


def neighbour_sum(ref, k, row):
    here, before, after = ref[tile(k), :], ref[tile(k - 1), :], ref[tile(k + 1), :]
    along = from_prev_row(here, before, row) + from_next_row(here, after, row)
    return along + (from_prev_col(here) + from_next_col(here))


def ocean_before(g_ref, ra, rc, rd, nx, outer, base, gf, x0, gw, invd, ra_out, g_s, gx_s, x_s, b_s):
    g = g_ref[0]
    rows, cols = base.shape
    wide = cols + LANES
    per = rows // SUB
    ext = per + 2
    lane = lane_iota()
    row = row_iota(wide)
    zero = jnp.zeros((SUB, wide), F32)
    ocean_first = (outer.shape[0] // SUB - 2 * per) - NOC * per
    for ref in (g_s, gx_s):
        ref[tile(0), :] = zero
        ref[tile(ext + 1), :] = zero
    for j in range(ext):
        t = tile(j + 1)

        def field(i, ref):
            if j == 0 or j == ext - 1:
                parts = low_high(g, ra, rc, rd, nx, 2 * NICE + i, lane, j == 0)
            else:
                parts = [ref[tile(j - 1), :], outer[tile(ocean_first + i * per + j - 1), :]]
            return jnp.concatenate(parts, axis=1)

        b_s[tile(j), :] = field(0, base)
        depth = field(1, gf)
        x = field(2, x0)
        g_s[t, :] = depth
        gx_s[t, :] = depth * x
        x_s[tile(j), :] = x
        gw[tile(j), :] = depth
    for j in range(ext):
        t = tile(j)
        depth = g_s[tile(j + 1), :]
        diag = DAMP + depth * neighbour_sum(g_s, j + 1, row)
        invd[t, :] = 1.0 / diag
        around = depth * neighbour_sum(gx_s, j + 1, row)
        ra_out[t, :] = jnp.where(depth > 0.0, b_s[t, :], 0.0) - (diag * x_s[t, :] - around)


def ocean_basis(g_ref, gw, invd, ra, r1, r2, r3, mine, y0_out, y1_out, y2_out, sums,
                sp, u0_s, u1_s, u2_s):
    g = g_ref[0]
    wide = gw.shape[1]
    ext = gw.shape[0] // SUB
    cols = y0_out.shape[1]
    slab = r1.shape[0] // SUB - 2
    lane = lane_iota()
    row = row_iota(wide)
    zero = jnp.zeros((SUB, wide), F32)

    def strip(ref, k):
        n, i = k // WIDE_SLOTS, k % WIDE_SLOTS
        edge = wide_outer(ref[tile(slab + 1), n * LANES : (n + 1) * LANES], i, lane)
        return jnp.concatenate([ref[tile(k), :], edge], axis=1)

    for ref in (u0_s, u1_s, u2_s):
        ref[tile(0), :] = zero
        ref[tile(ext + 1), :] = zero

    def clear(which):
        for j in which:
            sp[tile(j), :] = zero

    def whole(slabs):
        clear([0])
        over = None
        for k, ref in enumerate(slabs):
            values = [strip(ref, t) for t in range(slab + 1)]
            for t in range(slab):
                value = values[t] if t or over is None else values[t] + over
                sp[tile(1 + slab * k + t), :] = value
            over = values[slab]
        sp[tile(1 + slab * len(slabs)), :] = over

    @pl.when(g == 0)
    def _():
        whole([mine, r1, r2, r3])

    @pl.when(g == 3)
    def _():
        whole([r3, r2, r1, mine])

    @pl.when(g == 1)
    def _():
        clear(range(2, ext))
        sp[tile(0), :] = strip(r1, slab - 1)
        sp[tile(1), :] = strip(r1, slab)

    @pl.when(g == 2)
    def _():
        clear(range(ext - 1))
        sp[tile(ext - 1), :] = strip(r1, 0)

    acc = [jnp.zeros((SUB, cols), F32) for _ in range(6)]

    def add(k, left, right, j):
        if 0 < j < ext - 1:
            acc[k] = acc[k] + left[:, :cols] * right[:, :cols]

    for j in range(ext):
        t = tile(j)
        depth = gw[t, :]
        r0 = ra[t, :] + jnp.where(depth > 0.0, sp[t, :], 0.0)
        y0 = r0 * invd[t, :]
        u0_s[tile(j + 1), :] = depth * y0
        if 0 < j < ext - 1:
            y0_out[tile(j - 1), :] = y0[:, :cols]
        add(0, r0, y0, j)
    for j in range(ext):
        t = tile(j)
        depth = gw[t, :]
        w = depth * neighbour_sum(u0_s, j + 1, row)
        y1 = w * invd[t, :]
        u1_s[tile(j + 1), :] = depth * y1
        if 0 < j < ext - 1:
            y1_out[tile(j - 1), :] = y1[:, :cols]
            acc[1] = acc[1] + y0_out[tile(j - 1), :] * w[:, :cols]
        add(2, w, y1, j)
    for j in range(ext):
        t = tile(j)
        depth = gw[t, :]
        w = depth * neighbour_sum(u1_s, j + 1, row)
        y2 = w * invd[t, :]
        u2_s[tile(j + 1), :] = depth * y2
        if 0 < j < ext - 1:
            y2_out[tile(j - 1), :] = y2[:, :cols]
            acc[3] = acc[3] + y1_out[tile(j - 1), :] * w[:, :cols]
        add(4, w, y2, j)
    for j in range(1, ext - 1):
        w = neighbour_sum(u2_s, j + 1, row)[:, :cols] * u2_s[tile(j + 1), :][:, :cols]
        acc[5] = acc[5] + w
    for k in range(6):
        total = acc[k][:, :LANES]
        for c in range(1, cols // LANES):
            total = total + acc[k][:, c * LANES : (c + 1) * LANES]
        sums[k : k + 1, :] = jnp.sum(total, axis=0, keepdims=True)
    sums[6:8, :] = jnp.zeros((2, LANES), F32)


def combine(g_ref, parts, x0, y0, y1, y2, out):
    total = jnp.sum(jnp.sum(parts[...], axis=0), axis=1, keepdims=True)
    total = jnp.broadcast_to(total, (SUB, LANES))
    m = [jnp.broadcast_to(total[k : k + 1, :], (SUB, LANES)) for k in range(6)]

    def dot(left, right, image):
        value = None
        for i, a in enumerate(left):
            for j, b in enumerate(right):
                moment = m[i + j] - m[i + j + 1] if image else m[i + j]
                term = a * b * moment
                value = term if value is None else value + term
        return value

    z = [jnp.ones((SUB, LANES), F32)]
    p = z
    rz = m[0]
    coef = [0.0, 0.0, 0.0]
    for step in range(ITERS):
        alpha = rz / dot(p, p, True)
        for i, a in enumerate(p):
            coef[i] = coef[i] + alpha * a
        if step + 1 < ITERS:
            image = [a for a in p] + [jnp.zeros((SUB, LANES), F32)]
            for i, a in enumerate(p):
                image[i + 1] = image[i + 1] - a
            z = [(z[i] if i < len(z) else 0.0) - alpha * image[i] for i in range(len(image))]
            fresh = dot(z, z, False)
            beta = fresh / rz
            p = [z[i] + beta * p[i] if i < len(p) else z[i] for i in range(len(z))]
            rz = fresh
    reps = x0.shape[1] // LANES
    wide = [jnp.concatenate([c] * reps, axis=1) for c in coef]
    for k in range(x0.shape[0] // SUB):
        t = tile(k)
        out[t, :] = x0[t, :] + (wide[0] * y0[t, :] + wide[1] * y1[t, :] + wide[2] * y2[t, :])


def shards(
    base_rhs,
    depth,
    ssh_prev,
    currents,
    land_blocks,
    ice_thick,
    ice_blocks,
    ice_vel,
    ice_stress,
    wind,
):
    groups = lax.axis_size("grp")
    tiles = lax.axis_size("tile")
    assert groups == 4
    g = lax.axis_index("grp").astype(jnp.int32).reshape(1)
    rows, cols = base_rhs.shape
    ice_rows = ice_thick.shape[1]
    assert rows == groups * ice_rows
    slab = ice_rows + 2 * SUB
    wide = cols + LANES

    strip = (2 * slab, cols)
    c, a, b, token = call(
        pack_rows,
        [strip] * 3 + [(SUB, LANES)],
        [g, base_rhs, depth, ssh_prev, currents, land_blocks, ice_thick, ice_blocks, ice_vel, ice_stress, wind],
        scratch=[
            (2, 2, SUB, cols), (2, SUB, cols),
            (land_blocks.shape, jnp.int32), (ice_blocks.shape, jnp.int32),
        ],
        sems=48,
        hbm=True,
    )
    rc = lax.ppermute(c, "grp", [(0, 3), (3, 0), (1, 2), (2, 1)])
    ra = lax.ppermute(a, "grp", [(0, 1), (1, 0), (2, 3), (3, 2)])
    rb = lax.ppermute(b, "grp", [(0, 2), (3, 1)])

    own = sum(own_count(rows, ice_rows))
    packed = (-(-own // SLOTS) * SUB, LANES)
    gf, h, left, right = call(
        pack_own,
        [(rows, cols), (2, ice_rows, cols), packed, packed],
        [g, token, base_rhs, depth, ssh_prev, currents, land_blocks, ice_thick, ice_blocks, ice_vel, ice_stress,
         wind],
    )
    from_left = lax.ppermute(right, "tile", [(i, i + 1) for i in range(tiles - 1)])
    from_right = lax.ppermute(left, "tile", [(i + 1, i) for i in range(tiles - 1)])
    strip_tiles = 2 * (slab // SUB)
    narrow_rows = -(-strip_tiles // WIDE_SLOTS) * SUB
    tail = -(-narrow_rows * LANES // (SUB * cols)) * SUB
    outer, narrow, d = call(
        pack_narrow,
        [(own * SUB, LANES), (groups, narrow_rows, LANES), ((2 * NICE + NOC) * SUB + tail, cols)],
        [g, from_left, from_right, h, gf, base_rhs, ssh_prev, ice_vel, ice_stress, wind],
    )
    rd = lax.ppermute(d, "grp", [(0, 1), (3, 2)])
    nx = lax.all_to_all(narrow, "grp", 0, 0, tiled=True)

    back = (ice_rows + 2 * SUB, cols)
    velocity, stress, p3, p2, p1, mine = call(
        ice_steps,
        [ice_vel.shape, ice_stress.shape, back, back, back, back],
        [g, ra, rb, rc, rd, nx, outer, h, ice_vel, ice_stress, wind, currents],
        scratch=[(2, cols // LANES + 1, slab + 2 * SUB, LANES)] * 16,
        mib=32,
    )
    r3 = lax.ppermute(p3, "grp", [(3, 0), (0, 3)])
    r2 = lax.ppermute(p2, "grp", [(2, 0), (1, 3)])
    r1 = lax.ppermute(p1, "grp", [(1, 0), (2, 3), (3, 1), (0, 2)])

    ocean_rows = rows + 2 * SUB
    field = (ocean_rows, wide)
    padded = (ocean_rows + 2 * SUB, wide)
    gw, invd, known = call(
        ocean_before,
        [field] * 3,
        [g, ra, rc, rd, nx, outer, base_rhs, gf, ssh_prev],
        scratch=[padded, padded, field, field],
        flops=20000000,
    )
    y0, y1, y2, sums = call(
        ocean_basis,
        [(rows, cols)] * 3 + [(SUB, LANES)],
        [g, gw, invd, known, r1, r2, r3, mine],
        scratch=[field, padded, padded, padded],
    )
    devices = groups * tiles
    shared = lax.all_to_all(
        jnp.broadcast_to(sums[None], (devices, SUB, LANES)), ("grp", "tile"), 0, 0, tiled=True
    )
    (ssh,) = call(combine, [(rows, cols)], [g, shared, ssh_prev, y0, y1, y2])
    return ssh, velocity, stress


def solution(mesh):
    return jax.shard_map(
        shards,
        mesh=mesh,
        in_specs=(
            P("grp", "tile"),
            P("grp", "tile"),
            P("grp", "tile"),
            P(None, "grp", "tile"),
            P("grp", "tile"),
            P(None, "grp", "tile"),
            P(None, "grp", "tile"),
            P(None, None, "grp", "tile"),
            P(None, None, "grp", "tile"),
            P(None, None, "grp", "tile"),
        ),
        out_specs=(P("grp", "tile"), P(None, None, "grp", "tile"), P(None, None, "grp", "tile")),
        check_vma=False,
    )
```

```python
import jax
import jax.numpy as jnp
from jax import lax
from jax.experimental import pallas as pl
from jax.experimental.pallas import tpu as pltpu
from jax.sharding import PartitionSpec as P


BS = 8
NSUB = 8
ITERS = 3

DAMP = 0.05
RELAX = 0.2
STRENGTH = 0.5
DRAG = 1.0
STEP = 0.5

F32 = jnp.float32
SUB = 8
LANES = 128
EDGE = 16
SLOTS = LANES // EDGE
WIDE_SLOTS = LANES // (2 * EDGE)
GROUP = 4
SKEW = 1
NICE = 8
NOC = 3


def vmem():
    return pl.BlockSpec(memory_space=pltpu.VMEM)


def smem():
    return pl.BlockSpec(memory_space=pltpu.SMEM)


def call(body, outs, ins, scratch=(), sems=0, hbm=False, mib=24, flops=1000000):
    shapes = tuple(jax.ShapeDtypeStruct(s, F32) for s in outs)
    other = pl.BlockSpec(memory_space=pltpu.HBM) if hbm else vmem()
    specs = [smem() if i == 0 else other for i in range(len(ins))]
    held = [pltpu.VMEM(*s) if isinstance(s[0], tuple) else pltpu.VMEM(s, F32) for s in scratch]
    if sems:
        held.append(pltpu.SemaphoreType.DMA((sems,)))
    return pl.pallas_call(
        body,
        out_shape=shapes,
        in_specs=specs,
        out_specs=tuple(vmem() for _ in outs),
        scratch_shapes=held,
        cost_estimate=pl.CostEstimate(flops=flops, bytes_accessed=4000000, transcendentals=0),
        compiler_params=pltpu.CompilerParams(vmem_limit_bytes=mib * 1024 * 1024),
    )(*([ins[0]] + [pltpu.with_memory_space_constraint(x, pltpu.HBM) for x in ins[1:]] if hbm else ins))


def tile(k):
    return slice(k * SUB, k * SUB + SUB)


def expanded_cols(blocks):
    count = blocks.shape[-1]
    row = lax.broadcasted_iota(jnp.int32, (count, count * BS), 0) * BS
    col = lax.broadcasted_iota(jnp.int32, (count, count * BS), 1)
    spread = ((col >= row) & (col < row + BS)).astype(F32)
    return jnp.dot(blocks.astype(F32), spread, preferred_element_type=F32)


def row_iota(cols):
    return lax.broadcasted_iota(jnp.int32, (SUB, cols), 0)


def lane_iota():
    return lax.broadcasted_iota(jnp.int32, (SUB, LANES), 1)


def from_next_row(here, after, row):
    return pltpu.roll(jnp.where(row == 0, after, here), SUB - 1, 0)


def from_prev_row(here, before, row):
    return pltpu.roll(jnp.where(row == SUB - 1, before, here), 1, 0)


def from_next_col(here):
    return pltpu.roll(here, here.shape[1] - 1, 1)


def from_prev_col(here):
    return pltpu.roll(here, 1, 1)


def own_tile(cur, comp, first, j):
    last = cur.shape[1] // SUB - 1
    t = jnp.clip(first + j, 0, last)
    return cur[comp, pl.ds(pl.multiple_of(t * SUB, SUB), SUB), :]


def pack_rows(g_ref, base, depth, x0, cur, land, thick, iceb, vel, stress, wind,
              c, a, b, token, thick_s, depth_s, land_s, iceb_s, sems):
    g = g_ref[0]
    rows, cols = base.shape
    ice_rows = thick.shape[1]
    slab = ice_rows + 2 * SUB
    token[...] = jnp.zeros((SUB, LANES), F32)

    def run(slabs, halos):
        copies = []

        def copy(src, dst):
            made = pltpu.make_async_copy(src, dst, sems.at[len(copies)])
            made.start()
            copies.append(made)

        for out, dest in slabs:
            start = ice_rows * dest - SUB
            first, last = max(start, 0), min(start + slab, rows)
            for comp in range(2):
                at = comp * slab + first - start
                copy(cur.at[comp, first:last, :], out.at[at : at + last - first, :])
                if first > start:
                    out[comp * slab : at, :] = jnp.zeros((first - start, cols), F32)
                if last < start + slab:
                    out[at + last - first : (comp + 1) * slab, :] = jnp.zeros((start + slab - last, cols), F32)
        if halos:
            copy(land, land_s)
            copy(iceb, iceb_s)
        for i, (out, last) in enumerate(halos):
            r = slice(ice_rows - SUB, ice_rows) if last else slice(0, SUB)
            ro = slice(rows - SUB, rows) if last else slice(0, SUB)
            for cap in range(2):
                copy(thick.at[cap, r, :], thick_s.at[i, cap])
                n = cap * NICE + 1
                pieces = [vel.at[0, cap, r, :], vel.at[1, cap, r, :]]
                pieces += [stress.at[k, cap, r, :] for k in range(3)]
                pieces += [wind.at[k, cap, r, :] for k in range(2)]
                for piece in pieces:
                    copy(piece, out.at[tile(n), :])
                    n += 1
            copy(depth.at[ro, :], depth_s.at[i])
            copy(base.at[ro, :], out.at[tile(2 * NICE), :])
            copy(x0.at[ro, :], out.at[tile(2 * NICE + 2), :])
            out[tile(2 * NICE + 3), :] = jnp.zeros((SUB, cols), F32)
        for made in copies:
            made.wait()
        if halos:
            wet = expanded_cols(land_s[...])
            covers = [expanded_cols(iceb_s[cap]) for cap in range(2)]
        for i, (out, last) in enumerate(halos):
            for cap in range(2):
                k = covers[cap].shape[0] - 1 if last else 0
                out[tile(cap * NICE), :] = thick_s[i, cap] * covers[cap][k : k + 1, :]
            k = wet.shape[0] - 1 if last else 0
            out[tile(2 * NICE + 1), :] = depth_s[i] * wet[k : k + 1, :]

    @pl.when(g == 0)
    def _():
        run([(c, 3), (a, 1), (b, 2)], [])

    @pl.when(g == 3)
    def _():
        run([(c, 0), (a, 2), (b, 1)], [])

    @pl.when(g == 1)
    def _():
        run([], [(a, False), (c, True)])

    @pl.when(g == 2)
    def _():
        run([], [(a, True), (c, False)])


def pack_own(g_ref, token, base, depth, x0, cur, land, thick, iceb, vel, stress, wind, gf, h, left, right):
    cols = base.shape[1]
    lane = lane_iota()
    slot = lane // EDGE
    state = {"n": 0, "l": None, "r": None}

    def emit(first, last):
        n = state["n"]
        s = n % SLOTS
        both = jnp.where(lane < EDGE, first, last)
        both = pltpu.roll(both, EDGE * s, 1) if s else both
        if s == 0:
            state["l"] = state["r"] = both
        else:
            state["l"] = jnp.where(slot == s, both, state["l"])
            state["r"] = jnp.where(slot == s - 1, both, state["r"])
        if s == SLOTS - 1:
            k = n // SLOTS
            left[tile(k), :] = state["l"]
            right[tile(k), :] = state["r"]
        state["n"] = n + 1

    def emit_all(ref):
        for k in range(ref.shape[0] // SUB):
            emit(ref[tile(k), :LANES], ref[tile(k), cols - LANES :])

    wet = expanded_cols(land[...])
    for k in range(depth.shape[0] // SUB):
        gf[tile(k), :] = depth[tile(k), :] * wet[k : k + 1, :]
    for cap in range(2):
        cover = expanded_cols(iceb[cap])
        for k in range(thick.shape[1] // SUB):
            h[cap, tile(k), :] = thick[cap, tile(k), :] * cover[k : k + 1, :]
    for cap in range(2):
        for ref in own_ice(h, vel, stress, wind, cap):
            emit_all(ref)
    for ref in (base, gf, x0):
        emit_all(ref)
    for comp in range(2):
        emit_all(cur.at[comp])
    while state["n"] % SLOTS:
        emit(jnp.zeros((SUB, LANES), F32), jnp.zeros((SUB, LANES), F32))


def own_ice(h, vel, stress, wind, cap):
    fields = [h.at[cap], vel.at[0, cap], vel.at[1, cap]]
    fields += [stress.at[i, cap] for i in range(3)]
    return fields + [wind.at[i, cap] for i in range(2)]


def own_count(rows, ice_rows):
    return 2 * NICE * (ice_rows // SUB), NOC * (rows // SUB), 2 * (rows // SUB)


def halo_tiles(rows, ice_rows, last):
    ice_tiles, ocean_tiles = ice_rows // SUB, rows // SUB
    picked = [n * ice_tiles + (ice_tiles - 1 if last else 0) for n in range(2 * NICE)]
    start = 2 * NICE * ice_tiles
    return picked + [start + i * ocean_tiles + (ocean_tiles - 1 if last else 0) for i in range(NOC)]


def pack_narrow(g_ref, from_left, from_right, h, gf, base, x0, vel, stress, wind, outer, narrow, d):
    g = g_ref[0]
    rows, cols = base.shape
    ice_rows = h.shape[1]
    lane = lane_iota()
    count = sum(own_count(rows, ice_rows))
    batch = 32
    for n in range(0, count, batch):
        made = [outer_columns(from_left, from_right, i, lane) for i in range(n, min(n + batch, count))]
        for i, value in enumerate(made):
            outer[tile(n + i), :] = value
    packed = narrow.shape[1] // SUB

    def pack(put, tiles):
        for k in range(packed):
            value = None
            for i in range(WIDE_SLOTS):
                n = k * WIDE_SLOTS + i
                if n < len(tiles):
                    one = tiles[n]()
                    one = pltpu.roll(one, i * 2 * EDGE, 1) if i else one
                    value = one if value is None else value + one
            put(k, jnp.zeros((SUB, LANES), F32) if value is None else value)

    def picked(n):
        return lambda: outer[tile(n), :]

    def slab(dest):
        start = sum(own_count(rows, ice_rows)[:2])
        per = rows // SUB
        tiles = []
        for comp in range(2):
            for j in range(ice_rows // SUB + 2):
                t = ice_rows // SUB * dest - 1 + j
                inside = 0 <= t < per
                tiles.append(picked(start + comp * per + t) if inside else lambda: jnp.zeros((SUB, LANES), F32))
        return tiles

    def halo(last):
        return [picked(n) for n in halo_tiles(rows, ice_rows, last)]

    def send(dest, tiles):
        def put(k, value):
            narrow[dest, tile(k), :] = value

        pack(put, tiles)

    def strip(last):
        r = slice(ice_rows - SUB, ice_rows) if last else slice(0, SUB)
        ro = slice(rows - SUB, rows) if last else slice(0, SUB)
        n = 0
        for cap in range(2):
            for ref in own_ice(h, vel, stress, wind, cap):
                d[tile(n), :] = ref[r, :]
                n += 1
        for ref in (base, gf, x0):
            d[tile(n), :] = ref[ro, :]
            n += 1
        per = cols // LANES

        def put(k, value):
            c = k % per
            d[tile(n + k // per), c * LANES : (c + 1) * LANES] = value

        pack(put, halo(last))

    @pl.when(g == 0)
    def _():
        send(0, [])
        send(1, slab(1))
        send(2, slab(2))
        send(3, slab(3))
        strip(True)

    @pl.when(g == 1)
    def _():
        send(0, halo(False))
        send(1, [])
        send(2, halo(True))
        send(3, [])

    @pl.when(g == 2)
    def _():
        send(0, [])
        send(1, halo(False))
        send(2, [])
        send(3, halo(True))

    @pl.when(g == 3)
    def _():
        send(0, slab(0))
        send(1, slab(1))
        send(2, slab(2))
        send(3, [])
        strip(False)


def wide_outer(value, i, lane):
    value = pltpu.roll(value, LANES - 2 * EDGE * i, 1) if i else value
    return jnp.where((lane < EDGE) | (lane >= LANES - EDGE), value, 0.0)


def low_high(g, ra, rc, rd, nx, n, lane, low):
    cols = ra.shape[1]
    inner_zero = jnp.zeros((SUB, cols), F32)
    k, i = n // WIDE_SLOTS, n % WIDE_SLOTS
    per = cols // LANES
    first = 2 * NICE + NOC
    tail = rd[tile(first + k // per), (k % per) * LANES : (k % per + 1) * LANES]
    t = tile(n)
    if low:
        inner = jnp.where(g == 1, rd[t, :], jnp.where(g == 2, rc[t, :], jnp.where(g == 3, ra[t, :], inner_zero)))
        packed = jnp.where(g == 1, tail, jnp.where(g == 2, nx[1, tile(k), :], jnp.where(g == 3, nx[2, tile(k), :], 0.0)))
    else:
        inner = jnp.where(g == 2, rd[t, :], jnp.where(g == 1, rc[t, :], jnp.where(g == 0, ra[t, :], inner_zero)))
        packed = jnp.where(g == 2, tail, jnp.where(g == 1, nx[2, tile(k), :], jnp.where(g == 0, nx[1, tile(k), :], 0.0)))
    return split(inner) + [wide_outer(packed, i, lane)]


def outer_columns(from_left, from_right, n, lane):
    s, k = n % SLOTS, n // SLOTS
    both = jnp.where(lane // EDGE == s, from_right[tile(k), :], from_left[tile(k), :])
    both = pltpu.roll(both, LANES - EDGE * s, 1) if s else both
    return jnp.where((lane < EDGE) | (lane >= LANES - EDGE), both, 0.0)


def split(value):
    return [value[:, c * LANES : (c + 1) * LANES] for c in range(value.shape[1] // LANES)]


def turned_next(regs, lane):
    n = len(regs)
    return [pltpu.roll(jnp.where(lane == 0, regs[(c + 1) % n], regs[c]), LANES - 1, 1) for c in range(n)]


def turned_prev(regs, lane):
    n = len(regs)
    return [pltpu.roll(jnp.where(lane == LANES - 1, regs[c - 1], regs[c]), 1, 1) for c in range(n)]


def ice_steps(g_ref, ra, rb, rc, rd, nx, outer, h, vel, stress, wind, cur,
              vel_out, stress_out, p3, p2, p1, mine,
              u_s, v_s, p_s, q_s, s_s, un_s, vn_s, qp_s, sp_s, a_s, m_s, w_s, fx_s, fy_s, f0_s, f1_s):
    g = g_ref[0]
    ice_rows, cols = h.shape[1:]
    rows = cur.shape[1]
    regs = cols // LANES + 1
    per = ice_rows // SUB
    ext = per + 2
    lane = lane_iota()
    zero = jnp.zeros((SUB, LANES), F32)
    keep = 1.0 / (1.0 + RELAX)
    flow_first = sum(own_count(rows, ice_rows)[:2])

    def at(j, shift=0):
        return slice(SUB * (j + 1) + shift, SUB * (j + 2) + shift)

    def flow(cap, comp, j):
        n = comp * ext + j
        t = tile(n)
        k, i = n // WIDE_SLOTS, n % WIDE_SLOTS
        here = jnp.clip(per * g - 1 + j, 0, rows // SUB - 1)
        own = own_tile(cur, comp, per * g - 1, j)
        spot = pl.multiple_of((flow_first + comp * (rows // SUB) + here) * SUB, SUB)
        own_outer = outer[pl.ds(spot, SUB), :]
        if cap == 0:
            inner = jnp.where(g == 0, own, jnp.where(g == 1, ra[t, :], jnp.where(g == 2, rb[t, :], rc[t, :])))
            edge = jnp.where(g == 0, own_outer, wide_outer(nx[0, tile(k), :], i, lane))
        else:
            inner = jnp.where(g == 3, own, jnp.where(g == 2, ra[t, :], jnp.where(g == 1, rb[t, :], rc[t, :])))
            edge = jnp.where(g == 3, own_outer, wide_outer(nx[3, tile(k), :], i, lane))
        return split(inner) + [edge]

    for cap in range(2):
        own = own_ice(h, vel, stress, wind, cap)
        for c in range(regs):
            for ref in (p_s, s_s):
                ref[cap, c, at(-1), :] = zero
            for ref in (u_s, v_s):
                ref[cap, c, at(ext), :] = zero
        flows = []
        for j in range(ext):
            if j % GROUP == 0:
                flows = [[flow(cap, comp, i) for comp in range(2)] for i in range(j, min(j + GROUP, ext))]
            if j == 0 or j == ext - 1:
                fields = [low_high(g, ra, rc, rd, nx, cap * NICE + f, lane, j == 0) for f in range(NICE)]
            else:
                fields = [
                    split(own[f][tile(j - 1), :]) + [outer[tile((cap * NICE + f) * per + j - 1), :]]
                    for f in range(NICE)
                ]
            fields = fields + flows[j % GROUP]
            for c in range(regs):
                hh, u, v, s0, s1, s2, w0, w1, f0, f1 = (f[c] for f in fields)
                u_s[cap, c, at(j), :] = u
                v_s[cap, c, at(j), :] = v
                p_s[cap, c, at(j), :] = 0.5 * (s0 + s1)
                q_s[cap, c, at(j), :] = 0.5 * (s0 - s1)
                s_s[cap, c, at(j), :] = s2
                inv = jnp.where(hh > 0.0, 1.0 / (hh + (1.0 + STEP * DRAG)), 0.0)
                quick = STEP * inv
                a_s[cap, c, at(j), :] = hh * (RELAX * STRENGTH * keep)
                m_s[cap, c, at(j), :] = (hh + 1.0) * inv
                w_s[cap, c, at(j), :] = quick
                fx_s[cap, c, at(j), :] = quick * (w0 + DRAG * f0)
                fy_s[cap, c, at(j), :] = quick * (w1 + DRAG * f1)
                f0_s[cap, c, at(j), :] = f0
                f1_s[cap, c, at(j), :] = f1
    for j in range(ext):
        for cap in range(2):
            for ref, source in ((un_s, u_s), (vn_s, v_s)):
                turned = turned_next([source[cap, c, at(j), :] for c in range(regs)], lane)
                for c in range(regs):
                    ref[cap, c, at(j), :] = turned[c]

    def stress_tile(cap, j):
        qs, ss = [], []
        for c in range(regs):
            u, v = u_s[cap, c, at(j), :], v_s[cap, c, at(j), :]
            ux = u_s[cap, c, at(j, 1), :] - u
            vx = v_s[cap, c, at(j, 1), :] - v
            uy = un_s[cap, c, at(j), :] - u
            vy = vn_s[cap, c, at(j), :] - v
            es = uy + vx
            half = ux * ux + vy * vy
            a = a_s[cap, c, at(j), :]
            ratio = a * lax.rsqrt((half + half) + (es * es + 1.0))
            low = 0.5 * a
            q = q_s[cap, c, at(j), :] * keep + (ratio * vy - low)
            s = s_s[cap, c, at(j), :] * keep + ratio * es
            p_s[cap, c, at(j), :] = p_s[cap, c, at(j), :] * keep + (ratio * ux - low)
            q_s[cap, c, at(j), :] = q
            s_s[cap, c, at(j), :] = s
            qs.append(q)
            ss.append(s)
        for ref, turned in ((qp_s, turned_prev(qs, lane)), (sp_s, turned_prev(ss, lane))):
            for c in range(regs):
                ref[cap, c, at(j), :] = turned[c]

    def velocity_tile(cap, j):
        us, vs = [], []
        for c in range(regs):
            s = s_s[cap, c, at(j), :]
            force_x = (p_s[cap, c, at(j), :] - p_s[cap, c, at(j, -1), :]) + (s - sp_s[cap, c, at(j), :])
            force_y = (q_s[cap, c, at(j), :] - qp_s[cap, c, at(j), :]) + (s - s_s[cap, c, at(j, -1), :])
            m, quick = m_s[cap, c, at(j), :], w_s[cap, c, at(j), :]
            u = m * u_s[cap, c, at(j), :] + (quick * force_x + fx_s[cap, c, at(j), :])
            v = m * v_s[cap, c, at(j), :] + (quick * force_y + fy_s[cap, c, at(j), :])
            u_s[cap, c, at(j), :] = u
            v_s[cap, c, at(j), :] = v
            us.append(u)
            vs.append(v)
        for ref, turned in ((un_s, turned_next(us, lane)), (vn_s, turned_next(vs, lane))):
            for c in range(regs):
                ref[cap, c, at(j), :] = turned[c]

    def subcycle(_, carry):
        for j in range(ext + SKEW):
            for cap in range(2):
                if j < ext:
                    stress_tile(cap, j)
                if j >= SKEW:
                    velocity_tile(cap, j - SKEW)
        return carry

    lax.fori_loop(0, NSUB, subcycle, 0)
    spreads = []
    for cap in range(2):
        for c in range(regs):
            q_s[cap, c, at(0), :] = zero
            q_s[cap, c, at(ext - 1), :] = zero
        parts = []
        across = [[zero] * regs]
        for j in range(1, ext - 1):
            d1s = []
            for c in range(regs):
                u, v = u_s[cap, c, at(j), :], v_s[cap, c, at(j), :]
                p, q = p_s[cap, c, at(j), :], q_s[cap, c, at(j), :]
                if c + 1 < regs:
                    block = (tile(j - 1), slice(c * LANES, (c + 1) * LANES))
                    vel_out[(0, cap) + block] = u
                    vel_out[(1, cap) + block] = v
                    stress_out[(0, cap) + block] = p + q
                    stress_out[(1, cap) + block] = p - q
                    stress_out[(2, cap) + block] = s_s[cap, c, at(j), :]
                iced = m_s[cap, c, at(j), :] > 0.0
                q_s[cap, c, at(j), :] = jnp.where(iced, DRAG * (u - f0_s[cap, c, at(j), :]), 0.0)
                d1s.append(jnp.where(iced, DRAG * (v - f1_s[cap, c, at(j), :]), 0.0))
            turned = turned_prev(d1s, lane)
            across.append([d1s[c] - turned[c] for c in range(regs)])
        across.append([zero] * regs)
        for j in range(1, ext):
            parts.append([
                (q_s[cap, c, at(j), :] - q_s[cap, c, at(j, -1), :]) + across[j][c] for c in range(regs)
            ])
        spreads.append(parts)
    bands = per + 1
    packs = [[None] * -(-bands // WIDE_SLOTS) for _ in range(2)]
    for cap in range(2):
        for k in range(bands):
            i = k % WIDE_SLOTS
            edge = jnp.where((lane < EDGE) | (lane >= LANES - EDGE), spreads[cap][k][regs - 1], 0.0)
            edge = pltpu.roll(edge, 2 * EDGE * i, 1) if i else edge
            held = packs[cap][k // WIDE_SLOTS]
            packs[cap][k // WIDE_SLOTS] = edge if held is None else held + edge

    def put(block, north, south):
        p3[block] = jnp.where(g == 3, north, south)
        p2[block] = jnp.where(g == 2, north, south)
        p1[block] = jnp.where((g == 1) | (g == 3), north, south)
        mine[block] = jnp.where(g == 0, north, south)

    for k in range(bands):
        for c in range(regs - 1):
            put((tile(k), slice(c * LANES, (c + 1) * LANES)), spreads[0][k][c], spreads[1][k][c])
    for c in range(regs - 1):
        pair = [pack[c] if c < len(pack) else zero for pack in packs]
        put((tile(bands), slice(c * LANES, (c + 1) * LANES)), *pair)


def neighbour_sum(ref, k, row):
    here, before, after = ref[tile(k), :], ref[tile(k - 1), :], ref[tile(k + 1), :]
    along = from_prev_row(here, before, row) + from_next_row(here, after, row)
    return along + (from_prev_col(here) + from_next_col(here))


def ocean_before(g_ref, ra, rc, rd, nx, outer, base, gf, x0, gw, invd, ra_out, g_s, gx_s, x_s, b_s):
    g = g_ref[0]
    rows, cols = base.shape
    wide = cols + LANES
    per = rows // SUB
    ext = per + 2
    lane = lane_iota()
    row = row_iota(wide)
    zero = jnp.zeros((SUB, wide), F32)
    ocean_first = (outer.shape[0] // SUB - 2 * per) - NOC * per
    for ref in (g_s, gx_s):
        ref[tile(0), :] = zero
        ref[tile(ext + 1), :] = zero
    for j in range(ext):
        t = tile(j + 1)

        def field(i, ref):
            if j == 0 or j == ext - 1:
                parts = low_high(g, ra, rc, rd, nx, 2 * NICE + i, lane, j == 0)
            else:
                parts = [ref[tile(j - 1), :], outer[tile(ocean_first + i * per + j - 1), :]]
            return jnp.concatenate(parts, axis=1)

        b_s[tile(j), :] = field(0, base)
        depth = field(1, gf)
        x = field(2, x0)
        g_s[t, :] = depth
        gx_s[t, :] = depth * x
        x_s[tile(j), :] = x
        gw[tile(j), :] = depth
    for j in range(ext):
        t = tile(j)
        depth = g_s[tile(j + 1), :]
        diag = DAMP + depth * neighbour_sum(g_s, j + 1, row)
        invd[t, :] = 1.0 / diag
        around = depth * neighbour_sum(gx_s, j + 1, row)
        ra_out[t, :] = jnp.where(depth > 0.0, b_s[t, :], 0.0) - (diag * x_s[t, :] - around)


def ocean_basis(g_ref, gw, invd, ra, r1, r2, r3, mine, y0_out, y1_out, y2_out, sums,
                sp, u0_s, u1_s, u2_s):
    g = g_ref[0]
    wide = gw.shape[1]
    ext = gw.shape[0] // SUB
    cols = y0_out.shape[1]
    slab = r1.shape[0] // SUB - 2
    lane = lane_iota()
    row = row_iota(wide)
    zero = jnp.zeros((SUB, wide), F32)

    def strip(ref, k):
        n, i = k // WIDE_SLOTS, k % WIDE_SLOTS
        edge = wide_outer(ref[tile(slab + 1), n * LANES : (n + 1) * LANES], i, lane)
        return jnp.concatenate([ref[tile(k), :], edge], axis=1)

    for ref in (u0_s, u1_s, u2_s):
        ref[tile(0), :] = zero
        ref[tile(ext + 1), :] = zero

    def clear(which):
        for j in which:
            sp[tile(j), :] = zero

    def whole(slabs):
        clear([0])
        over = None
        for k, ref in enumerate(slabs):
            values = [strip(ref, t) for t in range(slab + 1)]
            for t in range(slab):
                value = values[t] if t or over is None else values[t] + over
                sp[tile(1 + slab * k + t), :] = value
            over = values[slab]
        sp[tile(1 + slab * len(slabs)), :] = over

    @pl.when(g == 0)
    def _():
        whole([mine, r1, r2, r3])

    @pl.when(g == 3)
    def _():
        whole([r3, r2, r1, mine])

    @pl.when(g == 1)
    def _():
        clear(range(2, ext))
        sp[tile(0), :] = strip(r1, slab - 1)
        sp[tile(1), :] = strip(r1, slab)

    @pl.when(g == 2)
    def _():
        clear(range(ext - 1))
        sp[tile(ext - 1), :] = strip(r1, 0)

    acc = [jnp.zeros((SUB, cols), F32) for _ in range(6)]

    def add(k, left, right, j):
        if 0 < j < ext - 1:
            acc[k] = acc[k] + left[:, :cols] * right[:, :cols]

    for j in range(ext):
        t = tile(j)
        depth = gw[t, :]
        r0 = ra[t, :] + jnp.where(depth > 0.0, sp[t, :], 0.0)
        y0 = r0 * invd[t, :]
        u0_s[tile(j + 1), :] = depth * y0
        if 0 < j < ext - 1:
            y0_out[tile(j - 1), :] = y0[:, :cols]
        add(0, r0, y0, j)
    for j in range(ext):
        t = tile(j)
        depth = gw[t, :]
        w = depth * neighbour_sum(u0_s, j + 1, row)
        y1 = w * invd[t, :]
        u1_s[tile(j + 1), :] = depth * y1
        if 0 < j < ext - 1:
            y1_out[tile(j - 1), :] = y1[:, :cols]
            acc[1] = acc[1] + y0_out[tile(j - 1), :] * w[:, :cols]
        add(2, w, y1, j)
    for j in range(ext):
        t = tile(j)
        depth = gw[t, :]
        w = depth * neighbour_sum(u1_s, j + 1, row)
        y2 = w * invd[t, :]
        u2_s[tile(j + 1), :] = depth * y2
        if 0 < j < ext - 1:
            y2_out[tile(j - 1), :] = y2[:, :cols]
            acc[3] = acc[3] + y1_out[tile(j - 1), :] * w[:, :cols]
        add(4, w, y2, j)
    for j in range(1, ext - 1):
        w = neighbour_sum(u2_s, j + 1, row)[:, :cols] * u2_s[tile(j + 1), :][:, :cols]
        acc[5] = acc[5] + w
    lane_sums = []
    for k in range(6):
        total = acc[k][:, :LANES]
        for c in range(1, cols // LANES):
            total = total + acc[k][:, c * LANES : (c + 1) * LANES]
        lane_sums.append(jnp.sum(total, axis=0, keepdims=True))
    stacked = jnp.concatenate(lane_sums + [jnp.zeros((2, LANES), F32)], axis=0)
    each = jnp.broadcast_to(jnp.sum(stacked, axis=1, keepdims=True), (SUB, LANES))
    sums[...] = jnp.sum(jnp.where(lane == row_iota(LANES), each, 0.0), axis=0, keepdims=True)


def combine(g_ref, parts, x0, y0, y1, y2, out):
    total = jnp.broadcast_to(jnp.sum(parts[...], axis=0), (SUB, LANES))
    lane = lane_iota()
    m = [
        jnp.broadcast_to(jnp.sum(jnp.where(lane == k, total, 0.0), axis=1, keepdims=True), (SUB, LANES))
        for k in range(6)
    ]

    def dot(left, right, image):
        value = None
        for i, a in enumerate(left):
            for j, b in enumerate(right):
                moment = m[i + j] - m[i + j + 1] if image else m[i + j]
                term = a * b * moment
                value = term if value is None else value + term
        return value

    z = [jnp.ones((SUB, LANES), F32)]
    p = z
    rz = m[0]
    coef = [0.0, 0.0, 0.0]
    for step in range(ITERS):
        alpha = rz / dot(p, p, True)
        for i, a in enumerate(p):
            coef[i] = coef[i] + alpha * a
        if step + 1 < ITERS:
            image = [a for a in p] + [jnp.zeros((SUB, LANES), F32)]
            for i, a in enumerate(p):
                image[i + 1] = image[i + 1] - a
            z = [(z[i] if i < len(z) else 0.0) - alpha * image[i] for i in range(len(image))]
            fresh = dot(z, z, False)
            beta = fresh / rz
            p = [z[i] + beta * p[i] if i < len(p) else z[i] for i in range(len(z))]
            rz = fresh
    reps = x0.shape[1] // LANES
    wide = [jnp.concatenate([c] * reps, axis=1) for c in coef]
    for k in range(x0.shape[0] // SUB):
        t = tile(k)
        out[t, :] = x0[t, :] + (wide[0] * y0[t, :] + wide[1] * y1[t, :] + wide[2] * y2[t, :])


def shards(
    base_rhs,
    depth,
    ssh_prev,
    currents,
    land_blocks,
    ice_thick,
    ice_blocks,
    ice_vel,
    ice_stress,
    wind,
):
    groups = lax.axis_size("grp")
    tiles = lax.axis_size("tile")
    assert groups == 4
    g = lax.axis_index("grp").astype(jnp.int32).reshape(1)
    rows, cols = base_rhs.shape
    ice_rows = ice_thick.shape[1]
    assert rows == groups * ice_rows
    slab = ice_rows + 2 * SUB
    wide = cols + LANES

    strip = (2 * slab, cols)
    c, a, b, token = call(
        pack_rows,
        [strip] * 3 + [(SUB, LANES)],
        [g, base_rhs, depth, ssh_prev, currents, land_blocks, ice_thick, ice_blocks, ice_vel, ice_stress, wind],
        scratch=[
            (2, 2, SUB, cols), (2, SUB, cols),
            (land_blocks.shape, jnp.int32), (ice_blocks.shape, jnp.int32),
        ],
        sems=48,
        hbm=True,
    )
    rc = lax.ppermute(c, "grp", [(0, 3), (3, 0), (1, 2), (2, 1)])
    ra = lax.ppermute(a, "grp", [(0, 1), (1, 0), (2, 3), (3, 2)])
    rb = lax.ppermute(b, "grp", [(0, 2), (3, 1)])

    own = sum(own_count(rows, ice_rows))
    packed = (-(-own // SLOTS) * SUB, LANES)
    gf, h, left, right = call(
        pack_own,
        [(rows, cols), (2, ice_rows, cols), packed, packed],
        [g, token, base_rhs, depth, ssh_prev, currents, land_blocks, ice_thick, ice_blocks, ice_vel, ice_stress,
         wind],
    )
    from_left = lax.ppermute(right, "tile", [(i, i + 1) for i in range(tiles - 1)])
    from_right = lax.ppermute(left, "tile", [(i + 1, i) for i in range(tiles - 1)])
    strip_tiles = 2 * (slab // SUB)
    narrow_rows = -(-strip_tiles // WIDE_SLOTS) * SUB
    tail = -(-narrow_rows * LANES // (SUB * cols)) * SUB
    outer, narrow, d = call(
        pack_narrow,
        [(own * SUB, LANES), (groups, narrow_rows, LANES), ((2 * NICE + NOC) * SUB + tail, cols)],
        [g, from_left, from_right, h, gf, base_rhs, ssh_prev, ice_vel, ice_stress, wind],
    )
    rd = lax.ppermute(d, "grp", [(0, 1), (3, 2)])
    nx = lax.all_to_all(narrow, "grp", 0, 0, tiled=True)

    back = (ice_rows + 2 * SUB, cols)
    velocity, stress, p3, p2, p1, mine = call(
        ice_steps,
        [ice_vel.shape, ice_stress.shape, back, back, back, back],
        [g, ra, rb, rc, rd, nx, outer, h, ice_vel, ice_stress, wind, currents],
        scratch=[(2, cols // LANES + 1, slab + 2 * SUB, LANES)] * 16,
        mib=32,
    )
    r3 = lax.ppermute(p3, "grp", [(3, 0), (0, 3)])
    r2 = lax.ppermute(p2, "grp", [(2, 0), (1, 3)])
    r1 = lax.ppermute(p1, "grp", [(1, 0), (2, 3), (3, 1), (0, 2)])

    ocean_rows = rows + 2 * SUB
    field = (ocean_rows, wide)
    padded = (ocean_rows + 2 * SUB, wide)
    gw, invd, known = call(
        ocean_before,
        [field] * 3,
        [g, ra, rc, rd, nx, outer, base_rhs, gf, ssh_prev],
        scratch=[padded, padded, field, field],
        flops=20000000,
    )
    y0, y1, y2, sums = call(
        ocean_basis,
        [(rows, cols)] * 3 + [(1, LANES)],
        [g, gw, invd, known, r1, r2, r3, mine],
        scratch=[field, padded, padded, padded],
    )
    devices = groups * tiles
    shared = lax.all_to_all(
        jnp.broadcast_to(sums[None], (devices, 1, LANES)), ("grp", "tile"), 0, 0, tiled=True
    )
    (ssh,) = call(combine, [(rows, cols)], [g, shared, ssh_prev, y0, y1, y2])
    return ssh, velocity, stress


def solution(mesh):
    return jax.shard_map(
        shards,
        mesh=mesh,
        in_specs=(
            P("grp", "tile"),
            P("grp", "tile"),
            P("grp", "tile"),
            P(None, "grp", "tile"),
            P("grp", "tile"),
            P(None, "grp", "tile"),
            P(None, "grp", "tile"),
            P(None, None, "grp", "tile"),
            P(None, None, "grp", "tile"),
            P(None, None, "grp", "tile"),
        ),
        out_specs=(P("grp", "tile"), P(None, None, "grp", "tile"), P(None, None, "grp", "tile")),
        check_vma=False,
    )
```

```python
import jax
import jax.numpy as jnp
from jax import lax
from jax.experimental import pallas as pl
from jax.experimental.pallas import tpu as pltpu
from jax.sharding import PartitionSpec as P


BS = 8
NSUB = 8
ITERS = 3

DAMP = 0.05
RELAX = 0.2
STRENGTH = 0.5
DRAG = 1.0
STEP = 0.5

F32 = jnp.float32
SUB = 8
LANES = 128
EDGE = 16
SLOTS = LANES // EDGE
WIDE_SLOTS = LANES // (2 * EDGE)
GROUP = 4
SKEW = 1
NICE = 8
NOC = 3


def vmem():
    return pl.BlockSpec(memory_space=pltpu.VMEM)


def smem():
    return pl.BlockSpec(memory_space=pltpu.SMEM)


def call(body, outs, ins, scratch=(), sems=0, hbm=False, mib=24, flops=1000000):
    shapes = tuple(jax.ShapeDtypeStruct(s, F32) for s in outs)
    other = pl.BlockSpec(memory_space=pltpu.HBM) if hbm else vmem()
    specs = [smem() if i == 0 else other for i in range(len(ins))]
    held = [pltpu.VMEM(*s) if isinstance(s[0], tuple) else pltpu.VMEM(s, F32) for s in scratch]
    if sems:
        held.append(pltpu.SemaphoreType.DMA((sems,)))
    return pl.pallas_call(
        body,
        out_shape=shapes,
        in_specs=specs,
        out_specs=tuple(vmem() for _ in outs),
        scratch_shapes=held,
        cost_estimate=pl.CostEstimate(flops=flops, bytes_accessed=4000000, transcendentals=0),
        compiler_params=pltpu.CompilerParams(vmem_limit_bytes=mib * 1024 * 1024),
    )(*([ins[0]] + [pltpu.with_memory_space_constraint(x, pltpu.HBM) for x in ins[1:]] if hbm else ins))


def tile(k):
    return slice(k * SUB, k * SUB + SUB)


def expanded_cols(blocks):
    count = blocks.shape[-1]
    row = lax.broadcasted_iota(jnp.int32, (count, count * BS), 0) * BS
    col = lax.broadcasted_iota(jnp.int32, (count, count * BS), 1)
    spread = ((col >= row) & (col < row + BS)).astype(F32)
    return jnp.dot(blocks.astype(F32), spread, preferred_element_type=F32)


def row_iota(cols):
    return lax.broadcasted_iota(jnp.int32, (SUB, cols), 0)


def lane_iota():
    return lax.broadcasted_iota(jnp.int32, (SUB, LANES), 1)


def from_next_row(here, after, row):
    return pltpu.roll(jnp.where(row == 0, after, here), SUB - 1, 0)


def from_prev_row(here, before, row):
    return pltpu.roll(jnp.where(row == SUB - 1, before, here), 1, 0)


def from_next_col(here):
    return pltpu.roll(here, here.shape[1] - 1, 1)


def from_prev_col(here):
    return pltpu.roll(here, 1, 1)


def own_tile(cur, comp, first, j):
    last = cur.shape[1] // SUB - 1
    t = jnp.clip(first + j, 0, last)
    return cur[comp, pl.ds(pl.multiple_of(t * SUB, SUB), SUB), :]


def pack_rows(g_ref, base, depth, x0, cur, land, thick, iceb, vel, stress, wind,
              c, a, b, token, thick_s, depth_s, land_s, iceb_s, sems):
    g = g_ref[0]
    rows, cols = base.shape
    ice_rows = thick.shape[1]
    slab = ice_rows + 2 * SUB
    token[...] = jnp.zeros((SUB, LANES), F32)

    def run(slabs, halos):
        copies = []

        def copy(src, dst):
            made = pltpu.make_async_copy(src, dst, sems.at[len(copies)])
            made.start()
            copies.append(made)

        for out, dest in slabs:
            start = ice_rows * dest - SUB
            first, last = max(start, 0), min(start + slab, rows)
            for comp in range(2):
                at = comp * slab + first - start
                copy(cur.at[comp, first:last, :], out.at[at : at + last - first, :])
                if first > start:
                    out[comp * slab : at, :] = jnp.zeros((first - start, cols), F32)
                if last < start + slab:
                    out[at + last - first : (comp + 1) * slab, :] = jnp.zeros((start + slab - last, cols), F32)
        if halos:
            copy(land, land_s)
            copy(iceb, iceb_s)
        for i, (out, last) in enumerate(halos):
            r = slice(ice_rows - SUB, ice_rows) if last else slice(0, SUB)
            ro = slice(rows - SUB, rows) if last else slice(0, SUB)
            for cap in range(2):
                copy(thick.at[cap, r, :], thick_s.at[i, cap])
                n = cap * NICE + 1
                pieces = [vel.at[0, cap, r, :], vel.at[1, cap, r, :]]
                pieces += [stress.at[k, cap, r, :] for k in range(3)]
                pieces += [wind.at[k, cap, r, :] for k in range(2)]
                for piece in pieces:
                    copy(piece, out.at[tile(n), :])
                    n += 1
            copy(depth.at[ro, :], depth_s.at[i])
            copy(base.at[ro, :], out.at[tile(2 * NICE), :])
            copy(x0.at[ro, :], out.at[tile(2 * NICE + 2), :])
            out[tile(2 * NICE + 3), :] = jnp.zeros((SUB, cols), F32)
        for made in copies:
            made.wait()
        if halos:
            wet = expanded_cols(land_s[...])
            covers = [expanded_cols(iceb_s[cap]) for cap in range(2)]
        for i, (out, last) in enumerate(halos):
            for cap in range(2):
                k = covers[cap].shape[0] - 1 if last else 0
                out[tile(cap * NICE), :] = thick_s[i, cap] * covers[cap][k : k + 1, :]
            k = wet.shape[0] - 1 if last else 0
            out[tile(2 * NICE + 1), :] = depth_s[i] * wet[k : k + 1, :]

    @pl.when(g == 0)
    def _():
        run([(c, 3), (a, 1), (b, 2)], [])

    @pl.when(g == 3)
    def _():
        run([(c, 0), (a, 2), (b, 1)], [])

    @pl.when(g == 1)
    def _():
        run([], [(a, False), (c, True)])

    @pl.when(g == 2)
    def _():
        run([], [(a, True), (c, False)])


def pack_own(g_ref, token, base, depth, x0, cur, land, thick, iceb, vel, stress, wind, gf, h, left, right):
    cols = base.shape[1]
    lane = lane_iota()
    slot = lane // EDGE
    state = {"n": 0, "l": None, "r": None}

    def emit(first, last):
        n = state["n"]
        s = n % SLOTS
        both = jnp.where(lane < EDGE, first, last)
        both = pltpu.roll(both, EDGE * s, 1) if s else both
        if s == 0:
            state["l"] = state["r"] = both
        else:
            state["l"] = jnp.where(slot == s, both, state["l"])
            state["r"] = jnp.where(slot == s - 1, both, state["r"])
        if s == SLOTS - 1:
            k = n // SLOTS
            left[tile(k), :] = state["l"]
            right[tile(k), :] = state["r"]
        state["n"] = n + 1

    def emit_all(ref):
        for k in range(ref.shape[0] // SUB):
            emit(ref[tile(k), :LANES], ref[tile(k), cols - LANES :])

    wet = expanded_cols(land[...])
    for k in range(depth.shape[0] // SUB):
        gf[tile(k), :] = depth[tile(k), :] * wet[k : k + 1, :]
    for cap in range(2):
        cover = expanded_cols(iceb[cap])
        for k in range(thick.shape[1] // SUB):
            h[cap, tile(k), :] = thick[cap, tile(k), :] * cover[k : k + 1, :]
    for cap in range(2):
        for ref in own_ice(h, vel, stress, wind, cap):
            emit_all(ref)
    for ref in (base, gf, x0):
        emit_all(ref)
    for comp in range(2):
        emit_all(cur.at[comp])
    while state["n"] % SLOTS:
        emit(jnp.zeros((SUB, LANES), F32), jnp.zeros((SUB, LANES), F32))


def own_ice(h, vel, stress, wind, cap):
    fields = [h.at[cap], vel.at[0, cap], vel.at[1, cap]]
    fields += [stress.at[i, cap] for i in range(3)]
    return fields + [wind.at[i, cap] for i in range(2)]


def own_count(rows, ice_rows):
    return 2 * NICE * (ice_rows // SUB), NOC * (rows // SUB), 2 * (rows // SUB)


def halo_tiles(rows, ice_rows, last):
    ice_tiles, ocean_tiles = ice_rows // SUB, rows // SUB
    picked = [n * ice_tiles + (ice_tiles - 1 if last else 0) for n in range(2 * NICE)]
    start = 2 * NICE * ice_tiles
    return picked + [start + i * ocean_tiles + (ocean_tiles - 1 if last else 0) for i in range(NOC)]


def pack_narrow(g_ref, from_left, from_right, h, gf, base, x0, vel, stress, wind, outer, narrow, d):
    g = g_ref[0]
    rows, cols = base.shape
    ice_rows = h.shape[1]
    lane = lane_iota()
    count = sum(own_count(rows, ice_rows))
    batch = 32
    for n in range(0, count, batch):
        made = [outer_columns(from_left, from_right, i, lane) for i in range(n, min(n + batch, count))]
        for i, value in enumerate(made):
            outer[tile(n + i), :] = value
    packed = narrow.shape[1] // SUB

    def pack(put, tiles):
        for k in range(packed):
            value = None
            for i in range(WIDE_SLOTS):
                n = k * WIDE_SLOTS + i
                if n < len(tiles):
                    one = tiles[n]()
                    one = pltpu.roll(one, i * 2 * EDGE, 1) if i else one
                    value = one if value is None else value + one
            put(k, jnp.zeros((SUB, LANES), F32) if value is None else value)

    def picked(n):
        return lambda: outer[tile(n), :]

    def slab(dest):
        start = sum(own_count(rows, ice_rows)[:2])
        per = rows // SUB
        tiles = []
        for comp in range(2):
            for j in range(ice_rows // SUB + 2):
                t = ice_rows // SUB * dest - 1 + j
                inside = 0 <= t < per
                tiles.append(picked(start + comp * per + t) if inside else lambda: jnp.zeros((SUB, LANES), F32))
        return tiles

    def halo(last):
        return [picked(n) for n in halo_tiles(rows, ice_rows, last)]

    def send(dest, tiles):
        def put(k, value):
            narrow[dest, tile(k), :] = value

        pack(put, tiles)

    def strip(last):
        r = slice(ice_rows - SUB, ice_rows) if last else slice(0, SUB)
        ro = slice(rows - SUB, rows) if last else slice(0, SUB)
        n = 0
        for cap in range(2):
            for ref in own_ice(h, vel, stress, wind, cap):
                d[tile(n), :] = ref[r, :]
                n += 1
        for ref in (base, gf, x0):
            d[tile(n), :] = ref[ro, :]
            n += 1
        per = cols // LANES

        def put(k, value):
            c = k % per
            d[tile(n + k // per), c * LANES : (c + 1) * LANES] = value

        pack(put, halo(last))

    @pl.when(g == 0)
    def _():
        send(0, [])
        send(1, slab(1))
        send(2, slab(2))
        send(3, slab(3))
        strip(True)

    @pl.when(g == 1)
    def _():
        send(0, halo(False))
        send(1, [])
        send(2, halo(True))
        send(3, [])

    @pl.when(g == 2)
    def _():
        send(0, [])
        send(1, halo(False))
        send(2, [])
        send(3, halo(True))

    @pl.when(g == 3)
    def _():
        send(0, slab(0))
        send(1, slab(1))
        send(2, slab(2))
        send(3, [])
        strip(False)


def wide_outer(value, i, lane):
    value = pltpu.roll(value, LANES - 2 * EDGE * i, 1) if i else value
    return jnp.where((lane < EDGE) | (lane >= LANES - EDGE), value, 0.0)


def late_tile(rd, n, lane):
    per = rd.shape[1] // LANES
    k, i = n // WIDE_SLOTS, n % WIDE_SLOTS
    tail = rd[tile(2 * NICE + NOC + k // per), (k % per) * LANES : (k % per + 1) * LANES]
    return split(rd[tile(n), :]) + [wide_outer(tail, i, lane)]


def low_high(g, ra, rc, nx, n, lane, low):
    k, i = n // WIDE_SLOTS, n % WIDE_SLOTS
    t = tile(n)
    pieces = [(2, rc, 1), (3, ra, 2)] if low else [(0, ra, 1), (1, rc, 2)]
    inner = jnp.zeros((SUB, ra.shape[1]), F32)
    packed = jnp.zeros((SUB, LANES), F32)
    for group, ref, source in pieces:
        inner = jnp.where(g == group, ref[t, :], inner)
        packed = jnp.where(g == group, nx[source, tile(k), :], packed)
    return split(inner) + [wide_outer(packed, i, lane)]


def outer_columns(from_left, from_right, n, lane):
    s, k = n % SLOTS, n // SLOTS
    both = jnp.where(lane // EDGE == s, from_right[tile(k), :], from_left[tile(k), :])
    both = pltpu.roll(both, LANES - EDGE * s, 1) if s else both
    return jnp.where((lane < EDGE) | (lane >= LANES - EDGE), both, 0.0)


def split(value):
    return [value[:, c * LANES : (c + 1) * LANES] for c in range(value.shape[1] // LANES)]


def turned_next(regs, lane):
    n = len(regs)
    return [pltpu.roll(jnp.where(lane == 0, regs[(c + 1) % n], regs[c]), LANES - 1, 1) for c in range(n)]


def turned_prev(regs, lane):
    n = len(regs)
    return [pltpu.roll(jnp.where(lane == LANES - 1, regs[c - 1], regs[c]), 1, 1) for c in range(n)]


KEEP = 1.0 / (1.0 + RELAX)


def at(j, shift=0):
    return slice(SUB * (j + 1) + shift, SUB * (j + 2) + shift)


def ice_core(count, load, state, rest, lane):
    u_s, v_s, p_s, q_s, s_s = state
    un_s, vn_s, qp_s, sp_s, a_s, m_s, w_s, fx_s, fy_s, f0_s, f1_s = rest
    regs = u_s.shape[1]
    zero = jnp.zeros((SUB, LANES), F32)
    for cap in range(2):
        for c in range(regs):
            for ref in (p_s, s_s):
                ref[cap, c, at(-1), :] = zero
            for ref in (u_s, v_s):
                ref[cap, c, at(count), :] = zero
        for j in range(count):
            fields = load(cap, j)
            for c in range(regs):
                hh, u, v, s0, s1, s2, w0, w1, f0, f1 = (f[c] for f in fields)
                u_s[cap, c, at(j), :] = u
                v_s[cap, c, at(j), :] = v
                p_s[cap, c, at(j), :] = 0.5 * (s0 + s1)
                q_s[cap, c, at(j), :] = 0.5 * (s0 - s1)
                s_s[cap, c, at(j), :] = s2
                inv = jnp.where(hh > 0.0, 1.0 / (hh + (1.0 + STEP * DRAG)), 0.0)
                quick = STEP * inv
                a_s[cap, c, at(j), :] = hh * (RELAX * STRENGTH * KEEP)
                m_s[cap, c, at(j), :] = (hh + 1.0) * inv
                w_s[cap, c, at(j), :] = quick
                fx_s[cap, c, at(j), :] = quick * (w0 + DRAG * f0)
                fy_s[cap, c, at(j), :] = quick * (w1 + DRAG * f1)
                f0_s[cap, c, at(j), :] = f0
                f1_s[cap, c, at(j), :] = f1
    for j in range(count):
        for cap in range(2):
            for ref, source in ((un_s, u_s), (vn_s, v_s)):
                turned = turned_next([source[cap, c, at(j), :] for c in range(regs)], lane)
                for c in range(regs):
                    ref[cap, c, at(j), :] = turned[c]

    def stress_tile(cap, j):
        qs, ss = [], []
        for c in range(regs):
            u, v = u_s[cap, c, at(j), :], v_s[cap, c, at(j), :]
            ux = u_s[cap, c, at(j, 1), :] - u
            vx = v_s[cap, c, at(j, 1), :] - v
            uy = un_s[cap, c, at(j), :] - u
            vy = vn_s[cap, c, at(j), :] - v
            es = uy + vx
            half = ux * ux + vy * vy
            a = a_s[cap, c, at(j), :]
            ratio = a * lax.rsqrt((half + half) + (es * es + 1.0))
            low = 0.5 * a
            q = q_s[cap, c, at(j), :] * KEEP + (ratio * vy - low)
            s = s_s[cap, c, at(j), :] * KEEP + ratio * es
            p_s[cap, c, at(j), :] = p_s[cap, c, at(j), :] * KEEP + (ratio * ux - low)
            q_s[cap, c, at(j), :] = q
            s_s[cap, c, at(j), :] = s
            qs.append(q)
            ss.append(s)
        for ref, turned in ((qp_s, turned_prev(qs, lane)), (sp_s, turned_prev(ss, lane))):
            for c in range(regs):
                ref[cap, c, at(j), :] = turned[c]

    def velocity_tile(cap, j):
        us, vs = [], []
        for c in range(regs):
            s = s_s[cap, c, at(j), :]
            force_x = (p_s[cap, c, at(j), :] - p_s[cap, c, at(j, -1), :]) + (s - sp_s[cap, c, at(j), :])
            force_y = (q_s[cap, c, at(j), :] - qp_s[cap, c, at(j), :]) + (s - s_s[cap, c, at(j, -1), :])
            m, quick = m_s[cap, c, at(j), :], w_s[cap, c, at(j), :]
            u = m * u_s[cap, c, at(j), :] + (quick * force_x + fx_s[cap, c, at(j), :])
            v = m * v_s[cap, c, at(j), :] + (quick * force_y + fy_s[cap, c, at(j), :])
            u_s[cap, c, at(j), :] = u
            v_s[cap, c, at(j), :] = v
            us.append(u)
            vs.append(v)
        for ref, turned in ((un_s, turned_next(us, lane)), (vn_s, turned_next(vs, lane))):
            for c in range(regs):
                ref[cap, c, at(j), :] = turned[c]

    def subcycle(_, carry):
        for j in range(count + SKEW):
            for cap in range(2):
                if j < count:
                    stress_tile(cap, j)
                if j >= SKEW:
                    velocity_tile(cap, j - SKEW)
        return carry

    lax.fori_loop(0, NSUB, subcycle, 0)


def drag_tile(state, rest, cap, j):
    u_s, v_s = state[:2]
    m_s, f0_s, f1_s = rest[5], rest[9], rest[10]
    d0, d1 = [], []
    for c in range(u_s.shape[1]):
        iced = m_s[cap, c, at(j), :] > 0.0
        d0.append(jnp.where(iced, DRAG * (u_s[cap, c, at(j), :] - f0_s[cap, c, at(j), :]), 0.0))
        d1.append(jnp.where(iced, DRAG * (v_s[cap, c, at(j), :] - f1_s[cap, c, at(j), :]), 0.0))
    return d0, d1


def packed_edge(edge, k, lane):
    edge = jnp.where((lane < EDGE) | (lane >= LANES - EDGE), edge, 0.0)
    i = k % WIDE_SLOTS
    return pltpu.roll(edge, 2 * EDGE * i, 1) if i else edge


def ice_steps(g_ref, ra, rb, rc, nx, outer, h, vel, stress, wind, cur,
              u_s, v_s, p_s, q_s, s_s, p3, p2, p1, mine, kept, *rest):
    g = g_ref[0]
    state = (u_s, v_s, p_s, q_s, s_s)
    ice_rows, cols = h.shape[1:]
    rows = cur.shape[1]
    regs = cols // LANES + 1
    per = ice_rows // SUB
    ext = per + 2
    lane = lane_iota()
    zero = jnp.zeros((SUB, LANES), F32)
    flow_first = sum(own_count(rows, ice_rows)[:2])

    def flow(cap, comp, j):
        n = comp * ext + j
        t = tile(n)
        k, i = n // WIDE_SLOTS, n % WIDE_SLOTS
        here = jnp.clip(per * g - 1 + j, 0, rows // SUB - 1)
        own = own_tile(cur, comp, per * g - 1, j)
        spot = pl.multiple_of((flow_first + comp * (rows // SUB) + here) * SUB, SUB)
        own_outer = outer[pl.ds(spot, SUB), :]
        if cap == 0:
            inner = jnp.where(g == 0, own, jnp.where(g == 1, ra[t, :], jnp.where(g == 2, rb[t, :], rc[t, :])))
            edge = jnp.where(g == 0, own_outer, wide_outer(nx[0, tile(k), :], i, lane))
        else:
            inner = jnp.where(g == 3, own, jnp.where(g == 2, ra[t, :], jnp.where(g == 1, rb[t, :], rc[t, :])))
            edge = jnp.where(g == 3, own_outer, wide_outer(nx[3, tile(k), :], i, lane))
        return split(inner) + [edge]

    flows = {}

    def load(cap, j):
        own = own_ice(h, vel, stress, wind, cap)
        if j % GROUP == 0:
            flows.clear()
            for i in range(j, min(j + GROUP, ext)):
                flows[i] = [flow(cap, comp, i) for comp in range(2)]
        if j == 0 or j == ext - 1:
            fields = [low_high(g, ra, rc, nx, cap * NICE + f, lane, j == 0) for f in range(NICE)]
        else:
            fields = [
                split(own[f][tile(j - 1), :]) + [outer[tile((cap * NICE + f) * per + j - 1), :]]
                for f in range(NICE)
            ]
        return fields + flows[j]

    ice_core(ext, load, state, rest, lane)
    drag_s = rest[0]
    bands = per + 1
    packs = [[None] * -(-bands // WIDE_SLOTS) for _ in range(2)]
    spreads = []
    for cap in range(2):
        across = [[zero] * regs]
        for c in range(regs):
            drag_s[cap, c, at(0), :] = zero
            drag_s[cap, c, at(ext - 1), :] = zero
        for j in range(1, ext - 1):
            d0, d1 = drag_tile(state, rest, cap, j)
            turned = turned_prev(d1, lane)
            across.append([d1[c] - turned[c] for c in range(regs)])
            for c in range(regs):
                drag_s[cap, c, at(j), :] = d0[c]
                if j == 1:
                    kept[0, cap, c] = d0[c]
                if j == ext - 3:
                    kept[1, cap, c] = d0[c]
        across.append([zero] * regs)
        parts = []
        for j in range(1, ext):
            parts.append([
                (drag_s[cap, c, at(j), :] - drag_s[cap, c, at(j, -1), :]) + across[j][c] for c in range(regs)
            ])
        for k in range(bands):
            edge = packed_edge(parts[k][regs - 1], k, lane)
            held = packs[cap][k // WIDE_SLOTS]
            packs[cap][k // WIDE_SLOTS] = edge if held is None else held + edge
        spreads.append(parts)

    def put(block, north, south):
        p3[block] = jnp.where(g == 3, north, south)
        p2[block] = jnp.where(g == 2, north, south)
        p1[block] = jnp.where((g == 1) | (g == 3), north, south)
        mine[block] = jnp.where(g == 0, north, south)

    for k in range(bands):
        for c in range(regs - 1):
            put((tile(k), slice(c * LANES, (c + 1) * LANES)), spreads[0][k][c], spreads[1][k][c])
    for c in range(regs - 1):
        pair = [pack[c] if c < len(pack) else zero for pack in packs]
        put((tile(bands), slice(c * LANES, (c + 1) * LANES)), *pair)


def ice_late(g_ref, rd, ra, rb, nx, outer, h, vel, stress, wind, kept, p2_in, p1_in, p2, p1, fixed, *scratch):
    g = g_ref[0]
    state, rest = scratch[:5], scratch[5:]
    ice_rows, cols = h.shape[1:]
    regs = cols // LANES + 1
    per = ice_rows // SUB
    ext = per + 2
    bands = per + 1
    lane = lane_iota()
    row = row_iota(LANES)
    zero = jnp.zeros((SUB, LANES), F32)
    count = 3
    for k in range(p2.shape[0] // SUB):
        p2[tile(k), :] = p2_in[tile(k), :]
        p1[tile(k), :] = p1_in[tile(k), :]

    def run(group):
        first = 0 if group == 1 else ext - count
        edge_tile = 0 if group == 1 else ext - 1
        flow_of = (ra, rb) if group == 1 else (rb, ra)
        outs = (p1, p2) if group == 1 else (p2, p1)

        def load(cap, jj):
            j = first + jj
            own = own_ice(h, vel, stress, wind, cap)
            if j == edge_tile:
                fields = [late_tile(rd, cap * NICE + f, lane) for f in range(NICE)]
            else:
                fields = [
                    split(own[f][tile(j - 1), :]) + [outer[tile((cap * NICE + f) * per + j - 1), :]]
                    for f in range(NICE)
                ]
            for comp in range(2):
                n = comp * ext + j
                edge = wide_outer(nx[3 * cap, tile(n // WIDE_SLOTS), :], n % WIDE_SLOTS, lane)
                fields.append(split(flow_of[cap][tile(n), :]) + [edge])
            return fields

        ice_core(count, load, state, rest, lane)
        for cap in range(2):
            d0, d1 = drag_tile(state, rest, cap, 1)
            turned = turned_prev(d1, lane)
            bits = []
            for c in range(regs):
                across = d1[c] - turned[c]
                if group == 1:
                    here = (d0[c] - from_prev_row(d0[c], zero, row)) + across
                    change = jnp.where(row == 0, pltpu.roll(kept[0, cap, c] - d0[c], 1, 0), 0.0)
                    bits.append((here, change))
                else:
                    here = (d0[c] - from_prev_row(d0[c], kept[1, cap, c], row)) + across
                    bits.append((here, jnp.where(row == 0, -pltpu.roll(d0[c], 1, 0), 0.0)))
                if c + 1 < regs:
                    cut = slice(c * LANES, (c + 1) * LANES)
                    p, q = state[2][cap, c, at(1), :], state[3][cap, c, at(1), :]
                    fixed[cap, 0, :, cut] = state[0][cap, c, at(1), :]
                    fixed[cap, 1, :, cut] = state[1][cap, c, at(1), :]
                    fixed[cap, 2, :, cut] = p + q
                    fixed[cap, 3, :, cut] = p - q
                    fixed[cap, 4, :, cut] = state[4][cap, c, at(1), :]
            out = outs[cap]
            k = 0 if group == 1 else per - 1
            for c in range(regs - 1):
                cut = slice(c * LANES, (c + 1) * LANES)
                out[tile(k), cut] = bits[c][0]
                out[tile(k + 1), cut] = out[tile(k + 1), cut] + bits[c][1] if group == 1 else bits[c][1]
            for n, add in ((k, False), (k + 1, group == 1)):
                c = n // WIDE_SLOTS
                cut = slice(c * LANES, (c + 1) * LANES)
                edge = packed_edge(bits[regs - 1][n - k], n, lane)
                start = (2 * EDGE * (n % WIDE_SLOTS) - EDGE) % LANES
                inside = (lane - start) % LANES < 2 * EDGE if start else lane < 2 * EDGE
                old = out[tile(bands), cut]
                out[tile(bands), cut] = old + edge if add else jnp.where(inside, edge, old)

    @pl.when(g == 1)
    def _():
        run(1)

    @pl.when(g == 2)
    def _():
        run(2)


def ice_results(g_ref, u_s, v_s, p_s, q_s, s_s, fixed, vel_out, stress_out):
    g = g_ref[0]
    per = vel_out.shape[2] // SUB
    regs = u_s.shape[1]
    for cap in range(2):
        for j in range(per):
            for c in range(regs - 1):
                cut = slice(c * LANES, (c + 1) * LANES)
                p, q = p_s[cap, c, at(j + 1), :], q_s[cap, c, at(j + 1), :]
                values = [u_s[cap, c, at(j + 1), :], v_s[cap, c, at(j + 1), :], p + q, p - q, s_s[cap, c, at(j + 1), :]]
                if j == 0 or j == per - 1:
                    late = g == (1 if j == 0 else 2)
                    values = [jnp.where(late, fixed[cap, f, :, cut], value) for f, value in enumerate(values)]
                for f, value in enumerate(values):
                    if f < 2:
                        vel_out[f, cap, tile(j), cut] = value
                    else:
                        stress_out[f - 2, cap, tile(j), cut] = value


def neighbour_sum(ref, k, row):
    here, before, after = ref[tile(k), :], ref[tile(k - 1), :], ref[tile(k + 1), :]
    along = from_prev_row(here, before, row) + from_next_row(here, after, row)
    return along + (from_prev_col(here) + from_next_col(here))


def ocean_before(g_ref, ra, rc, rd, nx, outer, base, gf, x0, gw, invd, ra_out, g_s, gx_s, x_s, b_s):
    g = g_ref[0]
    rows, cols = base.shape
    wide = cols + LANES
    per = rows // SUB
    ext = per + 2
    lane = lane_iota()
    row = row_iota(wide)
    zero = jnp.zeros((SUB, wide), F32)
    ocean_first = (outer.shape[0] // SUB - 2 * per) - NOC * per
    for ref in (g_s, gx_s):
        ref[tile(0), :] = zero
        ref[tile(ext + 1), :] = zero
    for j in range(ext):
        t = tile(j + 1)

        def field(i, ref):
            if j == 0 or j == ext - 1:
                n = 2 * NICE + i
                late = g == (1 if j == 0 else 2)
                pairs = zip(late_tile(rd, n, lane), low_high(g, ra, rc, nx, n, lane, j == 0))
                parts = [jnp.where(late, x, y) for x, y in pairs]
            else:
                parts = [ref[tile(j - 1), :], outer[tile(ocean_first + i * per + j - 1), :]]
            return jnp.concatenate(parts, axis=1)

        b_s[tile(j), :] = field(0, base)
        depth = field(1, gf)
        x = field(2, x0)
        g_s[t, :] = depth
        gx_s[t, :] = depth * x
        x_s[tile(j), :] = x
        gw[tile(j), :] = depth
    for j in range(ext):
        t = tile(j)
        depth = g_s[tile(j + 1), :]
        diag = DAMP + depth * neighbour_sum(g_s, j + 1, row)
        invd[t, :] = 1.0 / diag
        around = depth * neighbour_sum(gx_s, j + 1, row)
        ra_out[t, :] = jnp.where(depth > 0.0, b_s[t, :], 0.0) - (diag * x_s[t, :] - around)


def ocean_basis(g_ref, gw, invd, ra, r1, r2, r3, mine, y0_out, y1_out, y2_out, sums,
                sp, u0_s, u1_s, u2_s):
    g = g_ref[0]
    wide = gw.shape[1]
    ext = gw.shape[0] // SUB
    cols = y0_out.shape[1]
    slab = r1.shape[0] // SUB - 2
    lane = lane_iota()
    row = row_iota(wide)
    zero = jnp.zeros((SUB, wide), F32)

    def strip(ref, k):
        n, i = k // WIDE_SLOTS, k % WIDE_SLOTS
        edge = wide_outer(ref[tile(slab + 1), n * LANES : (n + 1) * LANES], i, lane)
        return jnp.concatenate([ref[tile(k), :], edge], axis=1)

    for ref in (u0_s, u1_s, u2_s):
        ref[tile(0), :] = zero
        ref[tile(ext + 1), :] = zero

    def clear(which):
        for j in which:
            sp[tile(j), :] = zero

    def whole(slabs):
        clear([0])
        over = None
        for k, ref in enumerate(slabs):
            values = [strip(ref, t) for t in range(slab + 1)]
            for t in range(slab):
                value = values[t] if t or over is None else values[t] + over
                sp[tile(1 + slab * k + t), :] = value
            over = values[slab]
        sp[tile(1 + slab * len(slabs)), :] = over

    @pl.when(g == 0)
    def _():
        whole([mine, r1, r2, r3])

    @pl.when(g == 3)
    def _():
        whole([r3, r2, r1, mine])

    @pl.when(g == 1)
    def _():
        clear(range(2, ext))
        sp[tile(0), :] = strip(r1, slab - 1)
        sp[tile(1), :] = strip(r1, slab)

    @pl.when(g == 2)
    def _():
        clear(range(ext - 1))
        sp[tile(ext - 1), :] = strip(r1, 0)

    acc = [jnp.zeros((SUB, cols), F32) for _ in range(6)]

    def add(k, left, right, j):
        if 0 < j < ext - 1:
            acc[k] = acc[k] + left[:, :cols] * right[:, :cols]

    for j in range(ext):
        t = tile(j)
        depth = gw[t, :]
        r0 = ra[t, :] + jnp.where(depth > 0.0, sp[t, :], 0.0)
        y0 = r0 * invd[t, :]
        u0_s[tile(j + 1), :] = depth * y0
        if 0 < j < ext - 1:
            y0_out[tile(j - 1), :] = y0[:, :cols]
        add(0, r0, y0, j)
    for j in range(ext):
        t = tile(j)
        depth = gw[t, :]
        w = depth * neighbour_sum(u0_s, j + 1, row)
        y1 = w * invd[t, :]
        u1_s[tile(j + 1), :] = depth * y1
        if 0 < j < ext - 1:
            y1_out[tile(j - 1), :] = y1[:, :cols]
            acc[1] = acc[1] + y0_out[tile(j - 1), :] * w[:, :cols]
        add(2, w, y1, j)
    for j in range(ext):
        t = tile(j)
        depth = gw[t, :]
        w = depth * neighbour_sum(u1_s, j + 1, row)
        y2 = w * invd[t, :]
        u2_s[tile(j + 1), :] = depth * y2
        if 0 < j < ext - 1:
            y2_out[tile(j - 1), :] = y2[:, :cols]
            acc[3] = acc[3] + y1_out[tile(j - 1), :] * w[:, :cols]
        add(4, w, y2, j)
    for j in range(1, ext - 1):
        w = neighbour_sum(u2_s, j + 1, row)[:, :cols] * u2_s[tile(j + 1), :][:, :cols]
        acc[5] = acc[5] + w
    lane_sums = []
    for k in range(6):
        total = acc[k][:, :LANES]
        for c in range(1, cols // LANES):
            total = total + acc[k][:, c * LANES : (c + 1) * LANES]
        lane_sums.append(jnp.sum(total, axis=0, keepdims=True))
    stacked = jnp.concatenate(lane_sums + [jnp.zeros((2, LANES), F32)], axis=0)
    each = jnp.broadcast_to(jnp.sum(stacked, axis=1, keepdims=True), (SUB, LANES))
    sums[...] = jnp.sum(jnp.where(lane == row_iota(LANES), each, 0.0), axis=0, keepdims=True)


def combine(g_ref, parts, x0, y0, y1, y2, out):
    total = jnp.broadcast_to(jnp.sum(parts[...], axis=0), (SUB, LANES))
    lane = lane_iota()
    m = [
        jnp.broadcast_to(jnp.sum(jnp.where(lane == k, total, 0.0), axis=1, keepdims=True), (SUB, LANES))
        for k in range(6)
    ]

    def dot(left, right, image):
        value = None
        for i, a in enumerate(left):
            for j, b in enumerate(right):
                moment = m[i + j] - m[i + j + 1] if image else m[i + j]
                term = a * b * moment
                value = term if value is None else value + term
        return value

    z = [jnp.ones((SUB, LANES), F32)]
    p = z
    rz = m[0]
    coef = [0.0, 0.0, 0.0]
    for step in range(ITERS):
        alpha = rz / dot(p, p, True)
        for i, a in enumerate(p):
            coef[i] = coef[i] + alpha * a
        if step + 1 < ITERS:
            image = [a for a in p] + [jnp.zeros((SUB, LANES), F32)]
            for i, a in enumerate(p):
                image[i + 1] = image[i + 1] - a
            z = [(z[i] if i < len(z) else 0.0) - alpha * image[i] for i in range(len(image))]
            fresh = dot(z, z, False)
            beta = fresh / rz
            p = [z[i] + beta * p[i] if i < len(p) else z[i] for i in range(len(z))]
            rz = fresh
    reps = x0.shape[1] // LANES
    wide = [jnp.concatenate([c] * reps, axis=1) for c in coef]
    for k in range(x0.shape[0] // SUB):
        t = tile(k)
        out[t, :] = x0[t, :] + (wide[0] * y0[t, :] + wide[1] * y1[t, :] + wide[2] * y2[t, :])


def shards(
    base_rhs,
    depth,
    ssh_prev,
    currents,
    land_blocks,
    ice_thick,
    ice_blocks,
    ice_vel,
    ice_stress,
    wind,
):
    groups = lax.axis_size("grp")
    tiles = lax.axis_size("tile")
    assert groups == 4
    g = lax.axis_index("grp").astype(jnp.int32).reshape(1)
    rows, cols = base_rhs.shape
    ice_rows = ice_thick.shape[1]
    assert rows == groups * ice_rows
    slab = ice_rows + 2 * SUB
    wide = cols + LANES

    strip = (2 * slab, cols)
    c, a, b, token = call(
        pack_rows,
        [strip] * 3 + [(SUB, LANES)],
        [g, base_rhs, depth, ssh_prev, currents, land_blocks, ice_thick, ice_blocks, ice_vel, ice_stress, wind],
        scratch=[
            (2, 2, SUB, cols), (2, SUB, cols),
            (land_blocks.shape, jnp.int32), (ice_blocks.shape, jnp.int32),
        ],
        sems=48,
        hbm=True,
    )
    rc = lax.ppermute(c, "grp", [(0, 3), (3, 0), (1, 2), (2, 1)])
    ra = lax.ppermute(a, "grp", [(0, 1), (1, 0), (2, 3), (3, 2)])
    rb = lax.ppermute(b, "grp", [(0, 2), (3, 1)])

    own = sum(own_count(rows, ice_rows))
    packed = (-(-own // SLOTS) * SUB, LANES)
    gf, h, left, right = call(
        pack_own,
        [(rows, cols), (2, ice_rows, cols), packed, packed],
        [g, token, base_rhs, depth, ssh_prev, currents, land_blocks, ice_thick, ice_blocks, ice_vel, ice_stress,
         wind],
    )
    from_left = lax.ppermute(right, "tile", [(i, i + 1) for i in range(tiles - 1)])
    from_right = lax.ppermute(left, "tile", [(i + 1, i) for i in range(tiles - 1)])
    strip_tiles = 2 * (slab // SUB)
    narrow_rows = -(-strip_tiles // WIDE_SLOTS) * SUB
    tail = -(-narrow_rows * LANES // (SUB * cols)) * SUB
    outer, narrow, d = call(
        pack_narrow,
        [(own * SUB, LANES), (groups, narrow_rows, LANES), ((2 * NICE + NOC) * SUB + tail, cols)],
        [g, from_left, from_right, h, gf, base_rhs, ssh_prev, ice_vel, ice_stress, wind],
    )
    nx = lax.all_to_all(narrow, "grp", 0, 0, tiled=True)
    d, nx = lax.optimization_barrier((d, nx))
    rd = lax.ppermute(d, "grp", [(0, 1), (3, 2)])

    back = (ice_rows + 2 * SUB, cols)
    regs = cols // LANES + 1
    held = (2, regs, slab + 2 * SUB, LANES)
    *state, p3, p2, p1, mine, kept = call(
        ice_steps,
        [held] * 5 + [back] * 4 + [(2, 2, regs, SUB, LANES)],
        [g, ra, rb, rc, nx, outer, h, ice_vel, ice_stress, wind, currents],
        scratch=[held] * 11,
        mib=32,
        flops=20000000,
    )
    p2, p1, fixed = call(
        ice_late,
        [back, back, (2, 5, SUB, cols)],
        [g, rd, ra, rb, nx, outer, h, ice_vel, ice_stress, wind, kept, p2, p1],
        scratch=[(2, regs, 5 * SUB, LANES)] * 16,
        flops=20000000,
    )
    r3 = lax.ppermute(p3, "grp", [(3, 0), (0, 3)])
    r2 = lax.ppermute(p2, "grp", [(2, 0), (1, 3)])
    r1 = lax.ppermute(p1, "grp", [(1, 0), (2, 3), (3, 1), (0, 2)])
    velocity, stress = call(ice_results, [ice_vel.shape, ice_stress.shape], [g, *state, fixed], flops=10000000)

    ocean_rows = rows + 2 * SUB
    field = (ocean_rows, wide)
    padded = (ocean_rows + 2 * SUB, wide)
    gw, invd, known = call(
        ocean_before,
        [field] * 3,
        [g, ra, rc, rd, nx, outer, base_rhs, gf, ssh_prev],
        scratch=[padded, padded, field, field],
        flops=20000000,
    )
    y0, y1, y2, sums = call(
        ocean_basis,
        [(rows, cols)] * 3 + [(1, LANES)],
        [g, gw, invd, known, r1, r2, r3, mine],
        scratch=[field, padded, padded, padded],
    )
    devices = groups * tiles
    shared = lax.all_to_all(
        jnp.broadcast_to(sums[None], (devices, 1, LANES)), ("grp", "tile"), 0, 0, tiled=True
    )
    (ssh,) = call(combine, [(rows, cols)], [g, shared, ssh_prev, y0, y1, y2])
    return ssh, velocity, stress


def solution(mesh):
    return jax.shard_map(
        shards,
        mesh=mesh,
        in_specs=(
            P("grp", "tile"),
            P("grp", "tile"),
            P("grp", "tile"),
            P(None, "grp", "tile"),
            P("grp", "tile"),
            P(None, "grp", "tile"),
            P(None, "grp", "tile"),
            P(None, None, "grp", "tile"),
            P(None, None, "grp", "tile"),
            P(None, None, "grp", "tile"),
        ),
        out_specs=(P("grp", "tile"), P(None, None, "grp", "tile"), P(None, None, "grp", "tile")),
        check_vma=False,
    )
```

```python
import jax
import jax.numpy as jnp
from jax import lax
from jax.experimental import pallas as pl
from jax.experimental.pallas import tpu as pltpu
from jax.sharding import PartitionSpec as P


BS = 8
NSUB = 8
ITERS = 3

DAMP = 0.05
RELAX = 0.2
STRENGTH = 0.5
DRAG = 1.0
STEP = 0.5

F32 = jnp.float32
SUB = 8
LANES = 128
EDGE = 16
SLOTS = LANES // EDGE
WIDE_SLOTS = LANES // (2 * EDGE)
GROUP = 4
SKEW = 1
NICE = 8
NOC = 3


def vmem():
    return pl.BlockSpec(memory_space=pltpu.VMEM)


def smem():
    return pl.BlockSpec(memory_space=pltpu.SMEM)


def call(body, outs, ins, scratch=(), sems=0, hbm=False, mib=24, flops=1000000):
    shapes = tuple(jax.ShapeDtypeStruct(s, F32) for s in outs)
    other = pl.BlockSpec(memory_space=pltpu.HBM) if hbm else vmem()
    specs = [smem() if i == 0 else other for i in range(len(ins))]
    held = [pltpu.VMEM(*s) if isinstance(s[0], tuple) else pltpu.VMEM(s, F32) for s in scratch]
    if sems:
        held.append(pltpu.SemaphoreType.DMA((sems,)))
    return pl.pallas_call(
        body,
        out_shape=shapes,
        in_specs=specs,
        out_specs=tuple(vmem() for _ in outs),
        scratch_shapes=held,
        cost_estimate=pl.CostEstimate(flops=flops, bytes_accessed=4000000, transcendentals=0),
        compiler_params=pltpu.CompilerParams(vmem_limit_bytes=mib * 1024 * 1024),
    )(*([ins[0]] + [pltpu.with_memory_space_constraint(x, pltpu.HBM) for x in ins[1:]] if hbm else ins))


def tile(k):
    return slice(k * SUB, k * SUB + SUB)


def expanded_cols(blocks):
    count = blocks.shape[-1]
    row = lax.broadcasted_iota(jnp.int32, (count, count * BS), 0) * BS
    col = lax.broadcasted_iota(jnp.int32, (count, count * BS), 1)
    spread = ((col >= row) & (col < row + BS)).astype(F32)
    return jnp.dot(blocks.astype(F32), spread, preferred_element_type=F32)


def row_iota(cols):
    return lax.broadcasted_iota(jnp.int32, (SUB, cols), 0)


def lane_iota():
    return lax.broadcasted_iota(jnp.int32, (SUB, LANES), 1)


def from_prev_row(here, before, row):
    return pltpu.roll(jnp.where(row == SUB - 1, before, here), 1, 0)


def own_tile(cur, comp, first, j):
    last = cur.shape[1] // SUB - 1
    t = jnp.clip(first + j, 0, last)
    return cur[comp, pl.ds(pl.multiple_of(t * SUB, SUB), SUB), :]


def half_and_half(base, depth, last):
    row = row_iota(base.shape[1])
    return jnp.where(row >= SUB // 2 if last else row < SUB // 2, base, pltpu.roll(depth, SUB // 2, 0))


def halved(value, which, last):
    row = row_iota(value.shape[1])
    value = pltpu.roll(value, SUB // 2, 0) if which else value
    return jnp.where(row >= SUB // 2 if last else row < SUB // 2, value, 0.0)


def strip_tile(ref, n, low):
    if n < 2 * NICE:
        return ref[tile(n), :]
    if n == 2 * NICE + 2:
        return ref[tile(2 * NICE + 1), :]
    return halved(ref[tile(2 * NICE), :], n - 2 * NICE, low)


def pack_rows(g_ref, base, depth, x0, cur, land, thick, iceb, vel, stress, wind,
              c, a, b, token, thick_s, depth_s, land_s, iceb_s, sems):
    g = g_ref[0]
    rows, cols = base.shape
    ice_rows = thick.shape[1]
    slab = ice_rows + 2 * SUB
    token[...] = jnp.zeros((SUB, LANES), F32)

    def run(slabs, halos):
        copies = []

        def copy(src, dst):
            made = pltpu.make_async_copy(src, dst, sems.at[len(copies)])
            made.start()
            copies.append(made)

        for out, dest in slabs:
            start = ice_rows * dest - SUB
            first, last = max(start, 0), min(start + slab, rows)
            for comp in range(2):
                begin = comp * (last - first)
                copy(cur.at[comp, first:last, :], out.at[begin : begin + last - first, :])
        if halos:
            copy(land, land_s)
            copy(iceb, iceb_s)
        for i, (out, last) in enumerate(halos):
            r = slice(ice_rows - SUB, ice_rows) if last else slice(0, SUB)
            ro = slice(rows - SUB, rows) if last else slice(0, SUB)
            for cap in range(2):
                copy(thick.at[cap, r, :], thick_s.at[i, cap])
                n = cap * NICE + 1
                pieces = [vel.at[0, cap, r, :], vel.at[1, cap, r, :]]
                pieces += [stress.at[k, cap, r, :] for k in range(3)]
                pieces += [wind.at[k, cap, r, :] for k in range(2)]
                for piece in pieces:
                    copy(piece, out.at[tile(n), :])
                    n += 1
            copy(depth.at[ro, :], depth_s.at[i, 0])
            copy(base.at[ro, :], depth_s.at[i, 1])
            copy(x0.at[ro, :], out.at[tile(2 * NICE + 1), :])
            for k in range(2 * NICE + 2, out.shape[0] // SUB):
                out[tile(k), :] = jnp.zeros((SUB, cols), F32)
        for made in copies:
            made.wait()
        if halos:
            wet = expanded_cols(land_s[...])
            covers = [expanded_cols(iceb_s[cap]) for cap in range(2)]
        for i, (out, last) in enumerate(halos):
            for cap in range(2):
                k = covers[cap].shape[0] - 1 if last else 0
                out[tile(cap * NICE), :] = thick_s[i, cap] * covers[cap][k : k + 1, :]
            k = wet.shape[0] - 1 if last else 0
            out[tile(2 * NICE), :] = half_and_half(depth_s[i, 1], depth_s[i, 0] * wet[k : k + 1, :], last)

    @pl.when(g == 0)
    def _():
        run([(c, 3), (a, 1), (b, 2)], [])

    @pl.when(g == 3)
    def _():
        run([(c, 0), (a, 2), (b, 1)], [])

    @pl.when(g == 1)
    def _():
        run([], [(a, False), (c, True)])

    @pl.when(g == 2)
    def _():
        run([], [(a, True), (c, False)])


def pack_own(g_ref, token, base, depth, x0, cur, land, thick, iceb, vel, stress, wind, gf, h, left, right):
    cols = base.shape[1]
    lane = lane_iota()
    slot = lane // EDGE
    state = {"n": 0, "l": None, "r": None}

    def emit(first, last):
        n = state["n"]
        s = n % SLOTS
        both = jnp.where(lane < EDGE, first, last)
        both = pltpu.roll(both, EDGE * s, 1) if s else both
        if s == 0:
            state["l"] = state["r"] = both
        else:
            state["l"] = jnp.where(slot == s, both, state["l"])
            state["r"] = jnp.where(slot == s - 1, both, state["r"])
        if s == SLOTS - 1:
            k = n // SLOTS
            left[tile(k), :] = state["l"]
            right[tile(k), :] = state["r"]
        state["n"] = n + 1

    def emit_all(ref):
        for k in range(ref.shape[0] // SUB):
            emit(ref[tile(k), :LANES], ref[tile(k), cols - LANES :])

    wet = expanded_cols(land[...])
    for k in range(depth.shape[0] // SUB):
        gf[tile(k), :] = depth[tile(k), :] * wet[k : k + 1, :]
    for cap in range(2):
        cover = expanded_cols(iceb[cap])
        for k in range(thick.shape[1] // SUB):
            h[cap, tile(k), :] = thick[cap, tile(k), :] * cover[k : k + 1, :]
    for cap in range(2):
        for ref in own_ice(h, vel, stress, wind, cap):
            emit_all(ref)
    for ref in (base, gf, x0):
        emit_all(ref)
    for comp in range(2):
        emit_all(cur.at[comp])
    while state["n"] % SLOTS:
        emit(jnp.zeros((SUB, LANES), F32), jnp.zeros((SUB, LANES), F32))


def own_ice(h, vel, stress, wind, cap):
    fields = [h.at[cap], vel.at[0, cap], vel.at[1, cap]]
    fields += [stress.at[i, cap] for i in range(3)]
    return fields + [wind.at[i, cap] for i in range(2)]


def own_count(rows, ice_rows):
    return 2 * NICE * (ice_rows // SUB), NOC * (rows // SUB), 2 * (rows // SUB)


def halo_tiles(rows, ice_rows, last):
    ice_tiles, ocean_tiles = ice_rows // SUB, rows // SUB
    picked = [n * ice_tiles + (ice_tiles - 1 if last else 0) for n in range(2 * NICE)]
    start = 2 * NICE * ice_tiles
    return picked + [start + i * ocean_tiles + (ocean_tiles - 1 if last else 0) for i in range(NOC)]


def pack_narrow(g_ref, from_left, from_right, h, gf, base, x0, vel, stress, wind, outer, narrow, d):
    g = g_ref[0]
    rows, cols = base.shape
    ice_rows = h.shape[1]
    lane = lane_iota()
    count = sum(own_count(rows, ice_rows))
    batch = 32
    for n in range(0, count, batch):
        made = [outer_columns(from_left, from_right, i, lane) for i in range(n, min(n + batch, count))]
        for i, value in enumerate(made):
            outer[tile(n + i), :] = value
    packed = narrow.shape[1] // SUB

    def pack(put, tiles):
        for k in range(packed):
            value = None
            for i in range(WIDE_SLOTS):
                n = k * WIDE_SLOTS + i
                if n < len(tiles):
                    one = tiles[n]()
                    one = pltpu.roll(one, i * 2 * EDGE, 1) if i else one
                    value = one if value is None else value + one
            put(k, jnp.zeros((SUB, LANES), F32) if value is None else value)

    def picked(n):
        return lambda: outer[tile(n), :]

    def slab(dest):
        start = sum(own_count(rows, ice_rows)[:2])
        per = rows // SUB
        tiles = []
        for comp in range(2):
            for j in range(ice_rows // SUB + 2):
                t = ice_rows // SUB * dest - 1 + j
                inside = 0 <= t < per
                tiles.append(picked(start + comp * per + t) if inside else lambda: jnp.zeros((SUB, LANES), F32))
        return tiles

    def halo(last):
        return [picked(n) for n in halo_tiles(rows, ice_rows, last)]

    def send(dest, tiles):
        def put(k, value):
            narrow[dest, tile(k), :] = value

        pack(put, tiles)

    def strip(last):
        r = slice(ice_rows - SUB, ice_rows) if last else slice(0, SUB)
        ro = slice(rows - SUB, rows) if last else slice(0, SUB)
        n = 0
        for cap in range(2):
            for ref in own_ice(h, vel, stress, wind, cap):
                d[tile(n), :] = ref[r, :]
                n += 1
        d[tile(n), :] = half_and_half(base[ro, :], gf[ro, :], last)
        d[tile(n + 1), :] = x0[ro, :]
        n += 2
        per = cols // LANES

        def put(k, value):
            c = k % per
            d[tile(n + k // per), c * LANES : (c + 1) * LANES] = value

        pack(put, halo(last))

    @pl.when(g == 0)
    def _():
        send(0, [])
        send(1, slab(1))
        send(2, slab(2))
        send(3, slab(3))
        strip(True)

    @pl.when(g == 1)
    def _():
        send(0, halo(False))
        send(1, [])
        send(2, halo(True))
        send(3, [])

    @pl.when(g == 2)
    def _():
        send(0, [])
        send(1, halo(False))
        send(2, [])
        send(3, halo(True))

    @pl.when(g == 3)
    def _():
        send(0, slab(0))
        send(1, slab(1))
        send(2, slab(2))
        send(3, [])
        strip(False)


def wide_outer(value, i, lane):
    value = pltpu.roll(value, LANES - 2 * EDGE * i, 1) if i else value
    return jnp.where((lane < EDGE) | (lane >= LANES - EDGE), value, 0.0)


def late_tile(rd, n, lane, low):
    per = rd.shape[1] // LANES
    k, i = n // WIDE_SLOTS, n % WIDE_SLOTS
    tail = rd[tile(2 * NICE + 2 + k // per), (k % per) * LANES : (k % per + 1) * LANES]
    return split(strip_tile(rd, n, low)) + [wide_outer(tail, i, lane)]


def low_high(g, ra, rc, nx, n, lane, low):
    k, i = n // WIDE_SLOTS, n % WIDE_SLOTS
    pieces = [(2, rc, 1), (3, ra, 2)] if low else [(0, ra, 1), (1, rc, 2)]
    inner = jnp.zeros((SUB, ra.shape[1]), F32)
    packed = jnp.zeros((SUB, LANES), F32)
    for group, ref, source in pieces:
        inner = jnp.where(g == group, strip_tile(ref, n, low), inner)
        packed = jnp.where(g == group, nx[source, tile(k), :], packed)
    return split(inner) + [wide_outer(packed, i, lane)]


def outer_columns(from_left, from_right, n, lane):
    s, k = n % SLOTS, n // SLOTS
    both = jnp.where(lane // EDGE == s, from_right[tile(k), :], from_left[tile(k), :])
    both = pltpu.roll(both, LANES - EDGE * s, 1) if s else both
    return jnp.where((lane < EDGE) | (lane >= LANES - EDGE), both, 0.0)


def split(value):
    return [value[:, c * LANES : (c + 1) * LANES] for c in range(value.shape[1] // LANES)]


def turned_next(regs, lane):
    n = len(regs)
    return [pltpu.roll(jnp.where(lane == 0, regs[(c + 1) % n], regs[c]), LANES - 1, 1) for c in range(n)]


def turned_prev(regs, lane):
    n = len(regs)
    return [pltpu.roll(jnp.where(lane == LANES - 1, regs[c - 1], regs[c]), 1, 1) for c in range(n)]


KEEP = 1.0 / (1.0 + RELAX)


def at(j, shift=0):
    return slice(SUB * (j + 1) + shift, SUB * (j + 2) + shift)


def ice_core(count, load, state, rest, lane):
    u_s, v_s, p_s, q_s, s_s = state
    un_s, vn_s, qp_s, sp_s, a_s, m_s, w_s, fx_s, fy_s, f0_s, f1_s = rest
    regs = u_s.shape[1]
    zero = jnp.zeros((SUB, LANES), F32)
    for cap in range(2):
        for c in range(regs):
            for ref in (p_s, s_s):
                ref[cap, c, at(-1), :] = zero
            for ref in (u_s, v_s):
                ref[cap, c, at(count), :] = zero
        for j in range(count):
            fields = load(cap, j)
            for c in range(regs):
                hh, u, v, s0, s1, s2, w0, w1, f0, f1 = (f[c] for f in fields)
                u_s[cap, c, at(j), :] = u
                v_s[cap, c, at(j), :] = v
                p_s[cap, c, at(j), :] = 0.5 * (s0 + s1)
                q_s[cap, c, at(j), :] = 0.5 * (s0 - s1)
                s_s[cap, c, at(j), :] = s2
                inv = jnp.where(hh > 0.0, 1.0 / (hh + (1.0 + STEP * DRAG)), 0.0)
                quick = STEP * inv
                a_s[cap, c, at(j), :] = hh * (RELAX * STRENGTH * KEEP)
                m_s[cap, c, at(j), :] = (hh + 1.0) * inv
                w_s[cap, c, at(j), :] = quick
                fx_s[cap, c, at(j), :] = quick * (w0 + DRAG * f0)
                fy_s[cap, c, at(j), :] = quick * (w1 + DRAG * f1)
                f0_s[cap, c, at(j), :] = f0
                f1_s[cap, c, at(j), :] = f1
    for j in range(count):
        for cap in range(2):
            for ref, source in ((un_s, u_s), (vn_s, v_s)):
                turned = turned_next([source[cap, c, at(j), :] for c in range(regs)], lane)
                for c in range(regs):
                    ref[cap, c, at(j), :] = turned[c]

    def stress_tile(cap, j):
        qs, ss = [], []
        for c in range(regs):
            u, v = u_s[cap, c, at(j), :], v_s[cap, c, at(j), :]
            ux = u_s[cap, c, at(j, 1), :] - u
            vx = v_s[cap, c, at(j, 1), :] - v
            uy = un_s[cap, c, at(j), :] - u
            vy = vn_s[cap, c, at(j), :] - v
            es = uy + vx
            half = ux * ux + vy * vy
            a = a_s[cap, c, at(j), :]
            ratio = a * lax.rsqrt((half + half) + (es * es + 1.0))
            low = 0.5 * a
            q = q_s[cap, c, at(j), :] * KEEP + (ratio * vy - low)
            s = s_s[cap, c, at(j), :] * KEEP + ratio * es
            p_s[cap, c, at(j), :] = p_s[cap, c, at(j), :] * KEEP + (ratio * ux - low)
            q_s[cap, c, at(j), :] = q
            s_s[cap, c, at(j), :] = s
            qs.append(q)
            ss.append(s)
        for ref, turned in ((qp_s, turned_prev(qs, lane)), (sp_s, turned_prev(ss, lane))):
            for c in range(regs):
                ref[cap, c, at(j), :] = turned[c]

    def velocity_tile(cap, j):
        us, vs = [], []
        for c in range(regs):
            s = s_s[cap, c, at(j), :]
            force_x = (p_s[cap, c, at(j), :] - p_s[cap, c, at(j, -1), :]) + (s - sp_s[cap, c, at(j), :])
            force_y = (q_s[cap, c, at(j), :] - qp_s[cap, c, at(j), :]) + (s - s_s[cap, c, at(j, -1), :])
            m, quick = m_s[cap, c, at(j), :], w_s[cap, c, at(j), :]
            u = m * u_s[cap, c, at(j), :] + (quick * force_x + fx_s[cap, c, at(j), :])
            v = m * v_s[cap, c, at(j), :] + (quick * force_y + fy_s[cap, c, at(j), :])
            u_s[cap, c, at(j), :] = u
            v_s[cap, c, at(j), :] = v
            us.append(u)
            vs.append(v)
        for ref, turned in ((un_s, turned_next(us, lane)), (vn_s, turned_next(vs, lane))):
            for c in range(regs):
                ref[cap, c, at(j), :] = turned[c]

    def subcycle(_, carry):
        for j in range(count + SKEW):
            for cap in range(2):
                if j < count:
                    stress_tile(cap, j)
                if j >= SKEW:
                    velocity_tile(cap, j - SKEW)
        return carry

    lax.fori_loop(0, NSUB, subcycle, 0)


def drag_tile(state, rest, cap, j):
    u_s, v_s = state[:2]
    m_s, f0_s, f1_s = rest[5], rest[9], rest[10]
    d0, d1 = [], []
    for c in range(u_s.shape[1]):
        iced = m_s[cap, c, at(j), :] > 0.0
        d0.append(jnp.where(iced, DRAG * (u_s[cap, c, at(j), :] - f0_s[cap, c, at(j), :]), 0.0))
        d1.append(jnp.where(iced, DRAG * (v_s[cap, c, at(j), :] - f1_s[cap, c, at(j), :]), 0.0))
    return d0, d1


def packed_edge(edge, k, lane):
    edge = jnp.where((lane < EDGE) | (lane >= LANES - EDGE), edge, 0.0)
    i = k % WIDE_SLOTS
    return pltpu.roll(edge, 2 * EDGE * i, 1) if i else edge


def ice_steps(g_ref, ra, rb, rc, nx, outer, h, vel, stress, wind, cur,
              u_s, v_s, p_s, q_s, s_s, p3, p2, p1, mine, kept, *rest):
    g = g_ref[0]
    state = (u_s, v_s, p_s, q_s, s_s)
    ice_rows, cols = h.shape[1:]
    rows = cur.shape[1]
    regs = cols // LANES + 1
    per = ice_rows // SUB
    ext = per + 2
    lane = lane_iota()
    zero = jnp.zeros((SUB, LANES), F32)
    flow_first = sum(own_count(rows, ice_rows)[:2])

    def flow(cap, comp, j):
        n = comp * ext + j
        t = tile(n)
        k, i = n // WIDE_SLOTS, n % WIDE_SLOTS
        far = j - cap
        diag = rc[tile(comp * (per + 1) + far), :] if 0 <= far <= per else jnp.zeros((SUB, cols), F32)
        here = jnp.clip(per * g - 1 + j, 0, rows // SUB - 1)
        own = own_tile(cur, comp, per * g - 1, j)
        spot = pl.multiple_of((flow_first + comp * (rows // SUB) + here) * SUB, SUB)
        own_outer = outer[pl.ds(spot, SUB), :]
        if cap == 0:
            inner = jnp.where(g == 0, own, jnp.where(g == 1, ra[t, :], jnp.where(g == 2, rb[t, :], diag)))
            edge = jnp.where(g == 0, own_outer, wide_outer(nx[0, tile(k), :], i, lane))
        else:
            inner = jnp.where(g == 3, own, jnp.where(g == 2, ra[t, :], jnp.where(g == 1, rb[t, :], diag)))
            edge = jnp.where(g == 3, own_outer, wide_outer(nx[3, tile(k), :], i, lane))
        return split(inner) + [edge]

    flows = {}

    def load(cap, j):
        own = own_ice(h, vel, stress, wind, cap)
        if j % GROUP == 0:
            flows.clear()
            for i in range(j, min(j + GROUP, ext)):
                flows[i] = [flow(cap, comp, i) for comp in range(2)]
        if j == 0 or j == ext - 1:
            fields = [low_high(g, ra, rc, nx, cap * NICE + f, lane, j == 0) for f in range(NICE)]
        else:
            fields = [
                split(own[f][tile(j - 1), :]) + [outer[tile((cap * NICE + f) * per + j - 1), :]]
                for f in range(NICE)
            ]
        return fields + flows[j]

    ice_core(ext, load, state, rest, lane)
    drag_s = rest[0]
    bands = per + 1
    packs = [[None] * -(-bands // WIDE_SLOTS) for _ in range(2)]
    spreads = []
    for cap in range(2):
        across = [[zero] * regs]
        for c in range(regs):
            drag_s[cap, c, at(0), :] = zero
            drag_s[cap, c, at(ext - 1), :] = zero
        for j in range(1, ext - 1):
            d0, d1 = drag_tile(state, rest, cap, j)
            turned = turned_prev(d1, lane)
            across.append([d1[c] - turned[c] for c in range(regs)])
            for c in range(regs):
                drag_s[cap, c, at(j), :] = d0[c]
                if j == 1:
                    kept[0, cap, c] = d0[c]
                if j == ext - 3:
                    kept[1, cap, c] = d0[c]
        across.append([zero] * regs)
        parts = []
        for j in range(1, ext):
            parts.append([
                (drag_s[cap, c, at(j), :] - drag_s[cap, c, at(j, -1), :]) + across[j][c] for c in range(regs)
            ])
        for k in range(bands):
            edge = packed_edge(parts[k][regs - 1], k, lane)
            held = packs[cap][k // WIDE_SLOTS]
            packs[cap][k // WIDE_SLOTS] = edge if held is None else held + edge
        spreads.append(parts)

    def put(block, north, south):
        p3[block] = jnp.where(g == 3, north, south)
        p2[block] = jnp.where(g == 2, north, south)
        p1[block] = jnp.where((g == 1) | (g == 3), north, south)
        mine[block] = jnp.where(g == 0, north, south)

    for k in range(bands):
        for c in range(regs - 1):
            put((tile(k), slice(c * LANES, (c + 1) * LANES)), spreads[0][k][c], spreads[1][k][c])
    for c in range(regs - 1):
        pair = [pack[c] if c < len(pack) else zero for pack in packs]
        put((tile(bands), slice(c * LANES, (c + 1) * LANES)), *pair)


def ice_late(g_ref, rd, ra, rb, nx, outer, h, vel, stress, wind, kept, p2_in, p1_in, p2, p1, fixed, *scratch):
    g = g_ref[0]
    state, rest = scratch[:5], scratch[5:]
    ice_rows, cols = h.shape[1:]
    regs = cols // LANES + 1
    per = ice_rows // SUB
    ext = per + 2
    bands = per + 1
    lane = lane_iota()
    row = row_iota(LANES)
    zero = jnp.zeros((SUB, LANES), F32)
    count = 3
    for k in range(p2.shape[0] // SUB):
        p2[tile(k), :] = p2_in[tile(k), :]
        p1[tile(k), :] = p1_in[tile(k), :]

    def run(group):
        first = 0 if group == 1 else ext - count
        edge_tile = 0 if group == 1 else ext - 1
        flow_of = (ra, rb) if group == 1 else (rb, ra)
        outs = (p1, p2) if group == 1 else (p2, p1)

        def load(cap, jj):
            j = first + jj
            own = own_ice(h, vel, stress, wind, cap)
            if j == edge_tile:
                fields = [late_tile(rd, cap * NICE + f, lane, group == 1) for f in range(NICE)]
            else:
                fields = [
                    split(own[f][tile(j - 1), :]) + [outer[tile((cap * NICE + f) * per + j - 1), :]]
                    for f in range(NICE)
                ]
            for comp in range(2):
                n = comp * ext + j
                edge = wide_outer(nx[3 * cap, tile(n // WIDE_SLOTS), :], n % WIDE_SLOTS, lane)
                fields.append(split(flow_of[cap][tile(n), :]) + [edge])
            return fields

        ice_core(count, load, state, rest, lane)
        for cap in range(2):
            d0, d1 = drag_tile(state, rest, cap, 1)
            turned = turned_prev(d1, lane)
            bits = []
            for c in range(regs):
                across = d1[c] - turned[c]
                if group == 1:
                    here = (d0[c] - from_prev_row(d0[c], zero, row)) + across
                    change = jnp.where(row == 0, pltpu.roll(kept[0, cap, c] - d0[c], 1, 0), 0.0)
                    bits.append((here, change))
                else:
                    here = (d0[c] - from_prev_row(d0[c], kept[1, cap, c], row)) + across
                    bits.append((here, jnp.where(row == 0, -pltpu.roll(d0[c], 1, 0), 0.0)))
                if c + 1 < regs:
                    cut = slice(c * LANES, (c + 1) * LANES)
                    p, q = state[2][cap, c, at(1), :], state[3][cap, c, at(1), :]
                    fixed[cap, 0, :, cut] = state[0][cap, c, at(1), :]
                    fixed[cap, 1, :, cut] = state[1][cap, c, at(1), :]
                    fixed[cap, 2, :, cut] = p + q
                    fixed[cap, 3, :, cut] = p - q
                    fixed[cap, 4, :, cut] = state[4][cap, c, at(1), :]
            out = outs[cap]
            k = 0 if group == 1 else per - 1
            for c in range(regs - 1):
                cut = slice(c * LANES, (c + 1) * LANES)
                out[tile(k), cut] = bits[c][0]
                out[tile(k + 1), cut] = out[tile(k + 1), cut] + bits[c][1] if group == 1 else bits[c][1]
            for n, add in ((k, False), (k + 1, group == 1)):
                c = n // WIDE_SLOTS
                cut = slice(c * LANES, (c + 1) * LANES)
                edge = packed_edge(bits[regs - 1][n - k], n, lane)
                start = (2 * EDGE * (n % WIDE_SLOTS) - EDGE) % LANES
                inside = (lane - start) % LANES < 2 * EDGE if start else lane < 2 * EDGE
                old = out[tile(bands), cut]
                out[tile(bands), cut] = old + edge if add else jnp.where(inside, edge, old)

    @pl.when(g == 1)
    def _():
        run(1)

    @pl.when(g == 2)
    def _():
        run(2)


def ice_results(g_ref, u_s, v_s, p_s, q_s, s_s, fixed, vel_out, stress_out):
    g = g_ref[0]
    per = vel_out.shape[2] // SUB
    regs = u_s.shape[1]
    for cap in range(2):
        for j in range(per):
            for c in range(regs - 1):
                cut = slice(c * LANES, (c + 1) * LANES)
                p, q = p_s[cap, c, at(j + 1), :], q_s[cap, c, at(j + 1), :]
                values = [u_s[cap, c, at(j + 1), :], v_s[cap, c, at(j + 1), :], p + q, p - q, s_s[cap, c, at(j + 1), :]]
                if j == 0 or j == per - 1:
                    late = g == (1 if j == 0 else 2)
                    values = [jnp.where(late, fixed[cap, f, :, cut], value) for f, value in enumerate(values)]
                for f, value in enumerate(values):
                    if f < 2:
                        vel_out[f, cap, tile(j), cut] = value
                    else:
                        stress_out[f - 2, cap, tile(j), cut] = value


def neighbour_sums(ref, j, lane):
    regs = ref.shape[0]
    here = [ref[c, at(j), :] for c in range(regs)]
    after, before = turned_next(here, lane), turned_prev(here, lane)
    return [
        (ref[c, at(j, -1), :] + ref[c, at(j, 1), :]) + (before[c] + after[c]) for c in range(regs)
    ]


def clear_ends(refs, count):
    zero = jnp.zeros((SUB, LANES), F32)
    for ref in refs:
        for c in range(ref.shape[0]):
            ref[c, at(-1), :] = zero
            ref[c, at(count), :] = zero


def ocean_before(g_ref, ra, rc, rd, nx, outer, base, gf, x0, g_s, invd, ra_out, gx_s, x_s, b_s):
    g = g_ref[0]
    rows, cols = base.shape
    regs = cols // LANES + 1
    per = rows // SUB
    ext = per + 2
    lane = lane_iota()
    ocean_first = (outer.shape[0] // SUB - 2 * per) - NOC * per
    clear_ends((g_s, gx_s), ext)
    for j in range(ext):

        def field(i, ref):
            if j == 0 or j == ext - 1:
                n = 2 * NICE + i
                late = g == (1 if j == 0 else 2)
                pairs = zip(late_tile(rd, n, lane, j == 0), low_high(g, ra, rc, nx, n, lane, j == 0))
                return [jnp.where(late, x, y) for x, y in pairs]
            return split(ref[tile(j - 1), :]) + [outer[tile(ocean_first + i * per + j - 1), :]]

        for c, (b, depth, x) in enumerate(zip(field(0, base), field(1, gf), field(2, x0))):
            b_s[c, at(j), :] = b
            g_s[c, at(j), :] = depth
            gx_s[c, at(j), :] = depth * x
            x_s[c, at(j), :] = x
    for j in range(ext):
        around, products = neighbour_sums(g_s, j, lane), neighbour_sums(gx_s, j, lane)
        for c in range(regs):
            depth = g_s[c, at(j), :]
            diag = DAMP + depth * around[c]
            invd[c, at(j), :] = 1.0 / diag
            known = jnp.where(depth > 0.0, b_s[c, at(j), :], 0.0)
            ra_out[c, at(j), :] = known - (diag * x_s[c, at(j), :] - depth * products[c])


def ocean_basis(g_ref, gw, invd, ra, r1, r2, r3, mine, y0_out, y1_out, y2_out, sums,
                sp, u0_s, u1_s, u2_s):
    g = g_ref[0]
    regs = gw.shape[0]
    ext = gw.shape[1] // SUB - 2
    slab = r1.shape[0] // SUB - 2
    lane = lane_iota()
    zero = jnp.zeros((SUB, LANES), F32)
    clear_ends((u0_s, u1_s, u2_s), ext)

    def strip(ref, k):
        n, i = k // WIDE_SLOTS, k % WIDE_SLOTS
        return split(ref[tile(k), :]) + [wide_outer(ref[tile(slab + 1), n * LANES : (n + 1) * LANES], i, lane)]

    def put(j, values):
        for c in range(regs):
            sp[c, at(j), :] = values[c]

    def clear(which):
        for j in which:
            put(j, [zero] * regs)

    def whole(slabs):
        clear([0])
        over = None
        for k, ref in enumerate(slabs):
            values = [strip(ref, t) for t in range(slab + 1)]
            for t in range(slab):
                value = values[t]
                if t == 0 and over is not None:
                    value = [x + y for x, y in zip(value, over)]
                put(1 + slab * k + t, value)
            over = values[slab]
        put(1 + slab * len(slabs), over)

    @pl.when(g == 0)
    def _():
        whole([mine, r1, r2, r3])

    @pl.when(g == 3)
    def _():
        whole([r3, r2, r1, mine])

    @pl.when(g == 1)
    def _():
        clear(range(2, ext))
        put(0, strip(r1, slab - 1))
        put(1, strip(r1, slab))

    @pl.when(g == 2)
    def _():
        clear(range(ext - 1))
        put(ext - 1, strip(r1, 0))

    acc = [[zero] * (regs - 1) for _ in range(6)]

    def add(k, c, left, right):
        acc[k][c] = acc[k][c] + left * right

    for j in range(ext):
        inside = 0 < j < ext - 1
        for c in range(regs):
            depth = gw[c, at(j), :]
            r0 = ra[c, at(j), :] + jnp.where(depth > 0.0, sp[c, at(j), :], 0.0)
            y0 = r0 * invd[c, at(j), :]
            u0_s[c, at(j), :] = depth * y0
            if inside and c + 1 < regs:
                y0_out[c, tile(j - 1), :] = y0
                add(0, c, r0, y0)
    for level, (source, target, before, here) in enumerate(
        ((u0_s, u1_s, y0_out, y1_out), (u1_s, u2_s, y1_out, y2_out))
    ):
        for j in range(ext):
            inside = 0 < j < ext - 1
            around = neighbour_sums(source, j, lane)
            for c in range(regs):
                depth = gw[c, at(j), :]
                w = depth * around[c]
                y = w * invd[c, at(j), :]
                target[c, at(j), :] = depth * y
                if inside and c + 1 < regs:
                    here[c, tile(j - 1), :] = y
                    add(2 * level + 1, c, before[c, tile(j - 1), :], w)
                    add(2 * level + 2, c, w, y)
    for j in range(1, ext - 1):
        around = neighbour_sums(u2_s, j, lane)
        for c in range(regs - 1):
            add(5, c, u2_s[c, at(j), :], around[c])
    lane_sums = []
    for k in range(6):
        total = acc[k][0]
        for c in range(1, regs - 1):
            total = total + acc[k][c]
        lane_sums.append(jnp.sum(total, axis=0, keepdims=True))
    stacked = jnp.concatenate(lane_sums + [jnp.zeros((2, LANES), F32)], axis=0)
    each = jnp.broadcast_to(jnp.sum(stacked, axis=1, keepdims=True), (SUB, LANES))
    sums[...] = jnp.sum(jnp.where(lane == row_iota(LANES), each, 0.0), axis=0, keepdims=True)


def combine(g_ref, parts, x0, y0, y1, y2, out):
    total = jnp.broadcast_to(jnp.sum(parts[...], axis=0), (SUB, LANES))
    lane = lane_iota()
    m = [
        jnp.broadcast_to(jnp.sum(jnp.where(lane == k, total, 0.0), axis=1, keepdims=True), (SUB, LANES))
        for k in range(6)
    ]

    def dot(left, right, image):
        value = None
        for i, a in enumerate(left):
            for j, b in enumerate(right):
                moment = m[i + j] - m[i + j + 1] if image else m[i + j]
                term = a * b * moment
                value = term if value is None else value + term
        return value

    z = [jnp.ones((SUB, LANES), F32)]
    p = z
    rz = m[0]
    coef = [0.0, 0.0, 0.0]
    for step in range(ITERS):
        alpha = rz / dot(p, p, True)
        for i, a in enumerate(p):
            coef[i] = coef[i] + alpha * a
        if step + 1 < ITERS:
            image = [a for a in p] + [jnp.zeros((SUB, LANES), F32)]
            for i, a in enumerate(p):
                image[i + 1] = image[i + 1] - a
            z = [(z[i] if i < len(z) else 0.0) - alpha * image[i] for i in range(len(image))]
            fresh = dot(z, z, False)
            beta = fresh / rz
            p = [z[i] + beta * p[i] if i < len(p) else z[i] for i in range(len(z))]
            rz = fresh
    for k in range(x0.shape[0] // SUB):
        t = tile(k)
        for c in range(y0.shape[0]):
            cut = slice(c * LANES, (c + 1) * LANES)
            move = coef[0] * y0[c, t, :] + coef[1] * y1[c, t, :] + coef[2] * y2[c, t, :]
            out[t, cut] = x0[t, cut] + move


def shards(
    base_rhs,
    depth,
    ssh_prev,
    currents,
    land_blocks,
    ice_thick,
    ice_blocks,
    ice_vel,
    ice_stress,
    wind,
):
    groups = lax.axis_size("grp")
    tiles = lax.axis_size("tile")
    assert groups == 4
    g = lax.axis_index("grp").astype(jnp.int32).reshape(1)
    rows, cols = base_rhs.shape
    ice_rows = ice_thick.shape[1]
    assert rows == groups * ice_rows
    slab = ice_rows + 2 * SUB
    strip = (2 * slab, cols)
    c, a, b, token = call(
        pack_rows,
        [(2 * (ice_rows + SUB), cols), strip, strip, (SUB, LANES)],
        [g, base_rhs, depth, ssh_prev, currents, land_blocks, ice_thick, ice_blocks, ice_vel, ice_stress, wind],
        scratch=[
            (2, 2, SUB, cols), (2, 2, SUB, cols),
            (land_blocks.shape, jnp.int32), (ice_blocks.shape, jnp.int32),
        ],
        sems=48,
        hbm=True,
    )
    rc = lax.ppermute(c, "grp", [(0, 3), (3, 0), (1, 2), (2, 1)])
    ra = lax.ppermute(a, "grp", [(0, 1), (1, 0), (2, 3), (3, 2)])
    rb = lax.ppermute(b, "grp", [(0, 2), (3, 1)])

    own = sum(own_count(rows, ice_rows))
    packed = (-(-own // SLOTS) * SUB, LANES)
    gf, h, left, right = call(
        pack_own,
        [(rows, cols), (2, ice_rows, cols), packed, packed],
        [g, token, base_rhs, depth, ssh_prev, currents, land_blocks, ice_thick, ice_blocks, ice_vel, ice_stress,
         wind],
    )
    from_left = lax.ppermute(right, "tile", [(i, i + 1) for i in range(tiles - 1)])
    from_right = lax.ppermute(left, "tile", [(i + 1, i) for i in range(tiles - 1)])
    strip_tiles = 2 * (slab // SUB)
    narrow_rows = -(-strip_tiles // WIDE_SLOTS) * SUB
    tail = -(-narrow_rows * LANES // (SUB * cols)) * SUB
    outer, narrow, d = call(
        pack_narrow,
        [(own * SUB, LANES), (groups, narrow_rows, LANES), ((2 * NICE + 2) * SUB + tail, cols)],
        [g, from_left, from_right, h, gf, base_rhs, ssh_prev, ice_vel, ice_stress, wind],
    )
    nx = lax.all_to_all(narrow, "grp", 0, 0, tiled=True)
    d, nx = lax.optimization_barrier((d, nx))
    rd = lax.ppermute(d, "grp", [(0, 1), (3, 2)])

    back = (ice_rows + 2 * SUB, cols)
    regs = cols // LANES + 1
    held = (2, regs, slab + 2 * SUB, LANES)
    *state, p3, p2, p1, mine, kept = call(
        ice_steps,
        [held] * 5 + [back] * 4 + [(2, 2, regs, SUB, LANES)],
        [g, ra, rb, rc, nx, outer, h, ice_vel, ice_stress, wind, currents],
        scratch=[held] * 11,
        mib=32,
        flops=20000000,
    )
    p2, p1, fixed = call(
        ice_late,
        [back, back, (2, 5, SUB, cols)],
        [g, rd, ra, rb, nx, outer, h, ice_vel, ice_stress, wind, kept, p2, p1],
        scratch=[(2, regs, 5 * SUB, LANES)] * 16,
        flops=20000000,
    )
    r3 = lax.ppermute(p3, "grp", [(3, 0), (0, 3)])
    r2 = lax.ppermute(p2, "grp", [(2, 0), (1, 3)])
    r1 = lax.ppermute(p1, "grp", [(1, 0), (2, 3), (3, 1), (0, 2)])
    velocity, stress = call(ice_results, [ice_vel.shape, ice_stress.shape], [g, *state, fixed], flops=10000000)

    field = (regs, rows + 4 * SUB, LANES)
    gw, invd, known = call(
        ocean_before,
        [field] * 3,
        [g, ra, rc, rd, nx, outer, base_rhs, gf, ssh_prev],
        scratch=[field] * 3,
        flops=20000000,
    )
    y0, y1, y2, sums = call(
        ocean_basis,
        [(regs - 1, rows, LANES)] * 3 + [(1, LANES)],
        [g, gw, invd, known, r1, r2, r3, mine],
        scratch=[field] * 4,
    )
    devices = groups * tiles
    shared = lax.all_to_all(
        jnp.broadcast_to(sums[None], (devices, 1, LANES)), ("grp", "tile"), 0, 0, tiled=True
    )
    (ssh,) = call(combine, [(rows, cols)], [g, shared, ssh_prev, y0, y1, y2])
    return ssh, velocity, stress


def solution(mesh):
    return jax.shard_map(
        shards,
        mesh=mesh,
        in_specs=(
            P("grp", "tile"),
            P("grp", "tile"),
            P("grp", "tile"),
            P(None, "grp", "tile"),
            P("grp", "tile"),
            P(None, "grp", "tile"),
            P(None, "grp", "tile"),
            P(None, None, "grp", "tile"),
            P(None, None, "grp", "tile"),
            P(None, None, "grp", "tile"),
        ),
        out_specs=(P("grp", "tile"), P(None, None, "grp", "tile"), P(None, None, "grp", "tile")),
        check_vma=False,
    )
```

```python
import jax
import jax.numpy as jnp
from jax import lax
from jax.experimental import pallas as pl
from jax.experimental.pallas import tpu as pltpu
from jax.sharding import PartitionSpec as P


BS = 8
NSUB = 8
ITERS = 3

DAMP = 0.05
RELAX = 0.2
STRENGTH = 0.5
DRAG = 1.0
STEP = 0.5

F32 = jnp.float32
SUB = 8
LANES = 128
EDGE = 16
SLOTS = LANES // EDGE
WIDE_SLOTS = LANES // (2 * EDGE)
GROUP = 4
SKEW = 1
NICE = 8
FIRST = [(0, 1), (1, 0), (2, 3), (3, 2)]
SECOND = [(0, 2), (2, 0), (1, 3), (3, 1)]
DIAGONAL = [(0, 3), (3, 0), (1, 2), (2, 1)]
NOC = 3


def vmem():
    return pl.BlockSpec(memory_space=pltpu.VMEM)


def smem():
    return pl.BlockSpec(memory_space=pltpu.SMEM)


def call(body, outs, ins, scratch=(), sems=0, hbm=False, mib=24, flops=1000000):
    shapes = tuple(jax.ShapeDtypeStruct(s, F32) for s in outs)
    other = pl.BlockSpec(memory_space=pltpu.HBM) if hbm else vmem()
    specs = [smem() if i == 0 else other for i in range(len(ins))]
    held = [pltpu.VMEM(*s) if isinstance(s[0], tuple) else pltpu.VMEM(s, F32) for s in scratch]
    if sems:
        held.append(pltpu.SemaphoreType.DMA((sems,)))
    return pl.pallas_call(
        body,
        out_shape=shapes,
        in_specs=specs,
        out_specs=tuple(vmem() for _ in outs),
        scratch_shapes=held,
        cost_estimate=pl.CostEstimate(flops=flops, bytes_accessed=4000000, transcendentals=0),
        compiler_params=pltpu.CompilerParams(vmem_limit_bytes=mib * 1024 * 1024),
    )(*([ins[0]] + [pltpu.with_memory_space_constraint(x, pltpu.HBM) for x in ins[1:]] if hbm else ins))


def tile(k):
    return slice(k * SUB, k * SUB + SUB)


def expanded_cols(blocks):
    count = blocks.shape[-1]
    row = lax.broadcasted_iota(jnp.int32, (count, count * BS), 0) * BS
    col = lax.broadcasted_iota(jnp.int32, (count, count * BS), 1)
    spread = ((col >= row) & (col < row + BS)).astype(F32)
    return jnp.dot(blocks.astype(F32), spread, preferred_element_type=F32)


def row_iota(cols):
    return lax.broadcasted_iota(jnp.int32, (SUB, cols), 0)


def lane_iota():
    return lax.broadcasted_iota(jnp.int32, (SUB, LANES), 1)


def from_prev_row(here, before, row):
    return pltpu.roll(jnp.where(row == SUB - 1, before, here), 1, 0)


def own_tile(cur, comp, first, j):
    last = cur.shape[1] // SUB - 1
    t = jnp.clip(first + j, 0, last)
    return cur[comp, pl.ds(pl.multiple_of(t * SUB, SUB), SUB), :]


def half_and_half(base, depth, last):
    row = row_iota(base.shape[1])
    return jnp.where(row >= SUB // 2 if last else row < SUB // 2, base, pltpu.roll(depth, SUB // 2, 0))


def halved(value, which, last):
    row = row_iota(value.shape[1])
    value = pltpu.roll(value, SUB // 2, 0) if which else value
    return jnp.where(row >= SUB // 2 if last else row < SUB // 2, value, 0.0)


def strip_tile(ref, n, low):
    if n < 2 * NICE:
        return ref[tile(n), :]
    if n == 2 * NICE + 2:
        return ref[tile(2 * NICE + 1), :]
    return halved(ref[tile(2 * NICE), :], n - 2 * NICE, low)


def pack_rows(g_ref, base, depth, x0, cur, land, thick, iceb, vel, stress, wind,
              c, a, b, token, thick_s, depth_s, land_s, iceb_s, sems):
    g = g_ref[0] & 3
    rows, cols = base.shape
    ice_rows = thick.shape[1]
    slab = ice_rows + 2 * SUB
    token[...] = jnp.zeros((SUB, LANES), F32)

    def run(slabs, halos):
        copies = []

        def copy(src, dst):
            made = pltpu.make_async_copy(src, dst, sems.at[len(copies)])
            made.start()
            copies.append(made)

        for out, dest in slabs:
            start = ice_rows * dest - SUB
            first, last = max(start, 0), min(start + slab, rows)
            for comp in range(2):
                begin = comp * (last - first)
                copy(cur.at[comp, first:last, :], out.at[begin : begin + last - first, :])
        if halos:
            copy(land, land_s)
            copy(iceb, iceb_s)
        for i, (out, last) in enumerate(halos):
            r = slice(ice_rows - SUB, ice_rows) if last else slice(0, SUB)
            ro = slice(rows - SUB, rows) if last else slice(0, SUB)
            for cap in range(2):
                copy(thick.at[cap, r, :], thick_s.at[i, cap])
                n = cap * NICE + 1
                pieces = [vel.at[0, cap, r, :], vel.at[1, cap, r, :]]
                pieces += [stress.at[k, cap, r, :] for k in range(3)]
                pieces += [wind.at[k, cap, r, :] for k in range(2)]
                for piece in pieces:
                    copy(piece, out.at[tile(n), :])
                    n += 1
            copy(depth.at[ro, :], depth_s.at[i, 0])
            copy(base.at[ro, :], depth_s.at[i, 1])
            copy(x0.at[ro, :], out.at[tile(2 * NICE + 1), :])
            for k in range(2 * NICE + 2, out.shape[0] // SUB):
                out[tile(k), :] = jnp.zeros((SUB, cols), F32)
        for made in copies:
            made.wait()
        if halos:
            wet = expanded_cols(land_s[...])
            covers = [expanded_cols(iceb_s[cap]) for cap in range(2)]
        for i, (out, last) in enumerate(halos):
            for cap in range(2):
                k = covers[cap].shape[0] - 1 if last else 0
                out[tile(cap * NICE), :] = thick_s[i, cap] * covers[cap][k : k + 1, :]
            k = wet.shape[0] - 1 if last else 0
            out[tile(2 * NICE), :] = half_and_half(depth_s[i, 1], depth_s[i, 0] * wet[k : k + 1, :], last)

    @pl.when(g == 0)
    def _():
        run([(c, 3), (a, 1), (b, 2)], [])

    @pl.when(g == 3)
    def _():
        run([(c, 0), (a, 2), (b, 1)], [])

    @pl.when(g == 1)
    def _():
        run([], [(a, False), (c, True)])

    @pl.when(g == 2)
    def _():
        run([], [(a, True), (c, False)])


def pack_own(g_ref, token, base, depth, x0, cur, land, thick, iceb, vel, stress, wind, gf, h, inner, cross):
    cols = base.shape[1]
    even = g_ref[0] < 4
    lane = lane_iota()
    slot = lane // EDGE
    state = {"n": 0, "l": None, "r": None}

    def emit(first, last):
        n = state["n"]
        s = n % SLOTS
        both = jnp.where(lane < EDGE, first, last)
        both = pltpu.roll(both, EDGE * s, 1) if s else both
        if s == 0:
            state["l"] = state["r"] = both
        else:
            state["l"] = jnp.where(slot == s, both, state["l"])
            state["r"] = jnp.where(slot == s - 1, both, state["r"])
        if s == SLOTS - 1:
            k = n // SLOTS
            inner[tile(k), :] = jnp.where(even, state["r"], state["l"])
            cross[tile(k), :] = jnp.where(even, state["l"], state["r"])
        state["n"] = n + 1

    def emit_all(ref):
        for k in range(ref.shape[0] // SUB):
            emit(ref[tile(k), :LANES], ref[tile(k), cols - LANES :])

    wet = expanded_cols(land[...])
    for k in range(depth.shape[0] // SUB):
        gf[tile(k), :] = depth[tile(k), :] * wet[k : k + 1, :]
    for cap in range(2):
        cover = expanded_cols(iceb[cap])
        for k in range(thick.shape[1] // SUB):
            h[cap, tile(k), :] = thick[cap, tile(k), :] * cover[k : k + 1, :]
    for cap in range(2):
        for ref in own_ice(h, vel, stress, wind, cap):
            emit_all(ref)
    for ref in (base, gf, x0):
        emit_all(ref)
    for comp in range(2):
        emit_all(cur.at[comp])
    while state["n"] % SLOTS:
        emit(jnp.zeros((SUB, LANES), F32), jnp.zeros((SUB, LANES), F32))


def own_ice(h, vel, stress, wind, cap):
    fields = [h.at[cap], vel.at[0, cap], vel.at[1, cap]]
    fields += [stress.at[i, cap] for i in range(3)]
    return fields + [wind.at[i, cap] for i in range(2)]


def own_count(rows, ice_rows):
    return 2 * NICE * (ice_rows // SUB), NOC * (rows // SUB), 2 * (rows // SUB)


def halo_tiles(rows, ice_rows, last):
    ice_tiles, ocean_tiles = ice_rows // SUB, rows // SUB
    picked = [n * ice_tiles + (ice_tiles - 1 if last else 0) for n in range(2 * NICE)]
    start = 2 * NICE * ice_tiles
    return picked + [start + i * ocean_tiles + (ocean_tiles - 1 if last else 0) for i in range(NOC)]


def pack_narrow(g_ref, inner, cross, h, gf, base, x0, vel, stress, wind, outer, narrow, d):
    g = g_ref[0] & 3
    rows, cols = base.shape
    ice_rows = h.shape[1]
    lane = lane_iota()
    count = sum(own_count(rows, ice_rows))
    batch = 32
    for n in range(0, count, batch):
        made = [outer_columns(g_ref[0] < 4, inner, cross, i, lane) for i in range(n, min(n + batch, count))]
        for i, value in enumerate(made):
            outer[tile(n + i), :] = value
    packed = narrow.shape[1] // SUB

    def pack(put, tiles):
        for k in range(packed):
            value = None
            for i in range(WIDE_SLOTS):
                n = k * WIDE_SLOTS + i
                if n < len(tiles):
                    one = tiles[n]()
                    one = pltpu.roll(one, i * 2 * EDGE, 1) if i else one
                    value = one if value is None else value + one
            put(k, jnp.zeros((SUB, LANES), F32) if value is None else value)

    def picked(n):
        return lambda: outer[tile(n), :]

    def slab(dest):
        start = sum(own_count(rows, ice_rows)[:2])
        per = rows // SUB
        tiles = []
        for comp in range(2):
            for j in range(ice_rows // SUB + 2):
                t = ice_rows // SUB * dest - 1 + j
                inside = 0 <= t < per
                tiles.append(picked(start + comp * per + t) if inside else lambda: jnp.zeros((SUB, LANES), F32))
        return tiles

    def halo(last):
        return [picked(n) for n in halo_tiles(rows, ice_rows, last)]

    def send(dest, tiles):
        def put(k, value):
            narrow[dest, tile(k), :] = value

        pack(put, tiles)

    def strip(last):
        r = slice(ice_rows - SUB, ice_rows) if last else slice(0, SUB)
        ro = slice(rows - SUB, rows) if last else slice(0, SUB)
        n = 0
        for cap in range(2):
            for ref in own_ice(h, vel, stress, wind, cap):
                d[tile(n), :] = ref[r, :]
                n += 1
        d[tile(n), :] = half_and_half(base[ro, :], gf[ro, :], last)
        d[tile(n + 1), :] = x0[ro, :]
        n += 2
        per = cols // LANES

        def put(k, value):
            c = k % per
            d[tile(n + k // per), c * LANES : (c + 1) * LANES] = value

        pack(put, halo(last))

    @pl.when(g == 0)
    def _():
        send(0, [])
        send(1, slab(1))
        send(2, slab(2))
        send(3, slab(3))
        strip(True)

    @pl.when(g == 1)
    def _():
        send(0, halo(False))
        send(1, [])
        send(2, halo(True))
        send(3, [])

    @pl.when(g == 2)
    def _():
        send(0, [])
        send(1, halo(False))
        send(2, [])
        send(3, halo(True))

    @pl.when(g == 3)
    def _():
        send(0, slab(0))
        send(1, slab(1))
        send(2, slab(2))
        send(3, [])
        strip(False)


def wide_outer(value, i, lane):
    value = pltpu.roll(value, LANES - 2 * EDGE * i, 1) if i else value
    return jnp.where((lane < EDGE) | (lane >= LANES - EDGE), value, 0.0)


def late_tile(rd, n, lane, low):
    per = rd.shape[1] // LANES
    k, i = n // WIDE_SLOTS, n % WIDE_SLOTS
    tail = rd[tile(2 * NICE + 2 + k // per), (k % per) * LANES : (k % per + 1) * LANES]
    return split(strip_tile(rd, n, low)) + [wide_outer(tail, i, lane)]


def low_high(g, ra, rc, nx, n, lane, low):
    k, i = n // WIDE_SLOTS, n % WIDE_SLOTS
    pieces = [(2, rc, 1), (3, ra, 2)] if low else [(0, ra, 1), (1, rc, 2)]
    inner = jnp.zeros((SUB, ra.shape[1]), F32)
    packed = jnp.zeros((SUB, LANES), F32)
    for group, ref, source in pieces:
        inner = jnp.where(g == group, strip_tile(ref, n, low), inner)
        packed = jnp.where(g == group, nx[source, tile(k), :], packed)
    return split(inner) + [wide_outer(packed, i, lane)]


def outer_columns(even, inner, cross, n, lane):
    s, k = n % SLOTS, n // SLOTS
    from_right = jnp.where(even, inner[tile(k), :], cross[tile(k), :])
    from_left = jnp.where(even, cross[tile(k), :], inner[tile(k), :])
    both = jnp.where(lane // EDGE == s, from_right, from_left)
    both = pltpu.roll(both, LANES - EDGE * s, 1) if s else both
    return jnp.where((lane < EDGE) | (lane >= LANES - EDGE), both, 0.0)


def split(value):
    return [value[:, c * LANES : (c + 1) * LANES] for c in range(value.shape[1] // LANES)]


def turned_next(regs, lane):
    n = len(regs)
    return [pltpu.roll(jnp.where(lane == 0, regs[(c + 1) % n], regs[c]), LANES - 1, 1) for c in range(n)]


def turned_prev(regs, lane):
    n = len(regs)
    return [pltpu.roll(jnp.where(lane == LANES - 1, regs[c - 1], regs[c]), 1, 1) for c in range(n)]


KEEP = 1.0 / (1.0 + RELAX)


def at(j, shift=0):
    return slice(SUB * (j + 1) + shift, SUB * (j + 2) + shift)


def ice_core(count, load, state, rest, lane):
    u_s, v_s, p_s, q_s, s_s = state
    un_s, vn_s, qp_s, sp_s, a_s, m_s, w_s, fx_s, fy_s, f0_s, f1_s = rest
    regs = u_s.shape[1]
    zero = jnp.zeros((SUB, LANES), F32)
    for cap in range(2):
        for c in range(regs):
            for ref in (p_s, s_s):
                ref[cap, c, at(-1), :] = zero
            for ref in (u_s, v_s):
                ref[cap, c, at(count), :] = zero
        for j in range(count):
            fields = load(cap, j)
            for c in range(regs):
                hh, u, v, s0, s1, s2, w0, w1, f0, f1 = (f[c] for f in fields)
                u_s[cap, c, at(j), :] = u
                v_s[cap, c, at(j), :] = v
                p_s[cap, c, at(j), :] = 0.5 * (s0 + s1)
                q_s[cap, c, at(j), :] = 0.5 * (s0 - s1)
                s_s[cap, c, at(j), :] = s2
                inv = jnp.where(hh > 0.0, 1.0 / (hh + (1.0 + STEP * DRAG)), 0.0)
                quick = STEP * inv
                a_s[cap, c, at(j), :] = hh * (RELAX * STRENGTH * KEEP)
                m_s[cap, c, at(j), :] = (hh + 1.0) * inv
                w_s[cap, c, at(j), :] = quick
                fx_s[cap, c, at(j), :] = quick * (w0 + DRAG * f0)
                fy_s[cap, c, at(j), :] = quick * (w1 + DRAG * f1)
                f0_s[cap, c, at(j), :] = f0
                f1_s[cap, c, at(j), :] = f1
    for j in range(count):
        for cap in range(2):
            for ref, source in ((un_s, u_s), (vn_s, v_s)):
                turned = turned_next([source[cap, c, at(j), :] for c in range(regs)], lane)
                for c in range(regs):
                    ref[cap, c, at(j), :] = turned[c]

    def stress_tile(cap, j):
        qs, ss = [], []
        for c in range(regs):
            u, v = u_s[cap, c, at(j), :], v_s[cap, c, at(j), :]
            ux = u_s[cap, c, at(j, 1), :] - u
            vx = v_s[cap, c, at(j, 1), :] - v
            uy = un_s[cap, c, at(j), :] - u
            vy = vn_s[cap, c, at(j), :] - v
            es = uy + vx
            half = ux * ux + vy * vy
            a = a_s[cap, c, at(j), :]
            ratio = a * lax.rsqrt((half + half) + (es * es + 1.0))
            low = 0.5 * a
            q = q_s[cap, c, at(j), :] * KEEP + (ratio * vy - low)
            s = s_s[cap, c, at(j), :] * KEEP + ratio * es
            p_s[cap, c, at(j), :] = p_s[cap, c, at(j), :] * KEEP + (ratio * ux - low)
            q_s[cap, c, at(j), :] = q
            s_s[cap, c, at(j), :] = s
            qs.append(q)
            ss.append(s)
        for ref, turned in ((qp_s, turned_prev(qs, lane)), (sp_s, turned_prev(ss, lane))):
            for c in range(regs):
                ref[cap, c, at(j), :] = turned[c]

    def velocity_tile(cap, j):
        us, vs = [], []
        for c in range(regs):
            s = s_s[cap, c, at(j), :]
            force_x = (p_s[cap, c, at(j), :] - p_s[cap, c, at(j, -1), :]) + (s - sp_s[cap, c, at(j), :])
            force_y = (q_s[cap, c, at(j), :] - qp_s[cap, c, at(j), :]) + (s - s_s[cap, c, at(j, -1), :])
            m, quick = m_s[cap, c, at(j), :], w_s[cap, c, at(j), :]
            u = m * u_s[cap, c, at(j), :] + (quick * force_x + fx_s[cap, c, at(j), :])
            v = m * v_s[cap, c, at(j), :] + (quick * force_y + fy_s[cap, c, at(j), :])
            u_s[cap, c, at(j), :] = u
            v_s[cap, c, at(j), :] = v
            us.append(u)
            vs.append(v)
        for ref, turned in ((un_s, turned_next(us, lane)), (vn_s, turned_next(vs, lane))):
            for c in range(regs):
                ref[cap, c, at(j), :] = turned[c]

    def subcycle(_, carry):
        for j in range(count + SKEW):
            for cap in range(2):
                if j < count:
                    stress_tile(cap, j)
                if j >= SKEW:
                    velocity_tile(cap, j - SKEW)
        return carry

    lax.fori_loop(0, NSUB, subcycle, 0)


def drag_tile(state, rest, cap, j):
    u_s, v_s = state[:2]
    m_s, f0_s, f1_s = rest[5], rest[9], rest[10]
    d0, d1 = [], []
    for c in range(u_s.shape[1]):
        iced = m_s[cap, c, at(j), :] > 0.0
        d0.append(jnp.where(iced, DRAG * (u_s[cap, c, at(j), :] - f0_s[cap, c, at(j), :]), 0.0))
        d1.append(jnp.where(iced, DRAG * (v_s[cap, c, at(j), :] - f1_s[cap, c, at(j), :]), 0.0))
    return d0, d1


def packed_edge(edge, k, lane):
    edge = jnp.where((lane < EDGE) | (lane >= LANES - EDGE), edge, 0.0)
    i = k % WIDE_SLOTS
    return pltpu.roll(edge, 2 * EDGE * i, 1) if i else edge


def ice_steps(g_ref, ra, rb, rc, nx, outer, h, vel, stress, wind, cur,
              u_s, v_s, p_s, q_s, s_s, p3, p2, p1, mine, kept, *rest):
    g = g_ref[0] & 3
    state = (u_s, v_s, p_s, q_s, s_s)
    ice_rows, cols = h.shape[1:]
    rows = cur.shape[1]
    regs = cols // LANES + 1
    per = ice_rows // SUB
    ext = per + 2
    lane = lane_iota()
    zero = jnp.zeros((SUB, LANES), F32)
    flow_first = sum(own_count(rows, ice_rows)[:2])

    def flow(cap, comp, j):
        n = comp * ext + j
        t = tile(n)
        k, i = n // WIDE_SLOTS, n % WIDE_SLOTS
        far = j - cap
        diag = rc[tile(comp * (per + 1) + far), :] if 0 <= far <= per else jnp.zeros((SUB, cols), F32)
        here = jnp.clip(per * g - 1 + j, 0, rows // SUB - 1)
        own = own_tile(cur, comp, per * g - 1, j)
        spot = pl.multiple_of((flow_first + comp * (rows // SUB) + here) * SUB, SUB)
        own_outer = outer[pl.ds(spot, SUB), :]
        if cap == 0:
            inner = jnp.where(g == 0, own, jnp.where(g == 1, ra[t, :], jnp.where(g == 2, rb[t, :], diag)))
            edge = jnp.where(g == 0, own_outer, wide_outer(nx[0, tile(k), :], i, lane))
        else:
            inner = jnp.where(g == 3, own, jnp.where(g == 2, ra[t, :], jnp.where(g == 1, rb[t, :], diag)))
            edge = jnp.where(g == 3, own_outer, wide_outer(nx[3, tile(k), :], i, lane))
        return split(inner) + [edge]

    flows = {}

    def load(cap, j):
        own = own_ice(h, vel, stress, wind, cap)
        if j % GROUP == 0:
            flows.clear()
            for i in range(j, min(j + GROUP, ext)):
                flows[i] = [flow(cap, comp, i) for comp in range(2)]
        if j == 0 or j == ext - 1:
            fields = [low_high(g, ra, rc, nx, cap * NICE + f, lane, j == 0) for f in range(NICE)]
        else:
            fields = [
                split(own[f][tile(j - 1), :]) + [outer[tile((cap * NICE + f) * per + j - 1), :]]
                for f in range(NICE)
            ]
        return fields + flows[j]

    ice_core(ext, load, state, rest, lane)
    drag_s = rest[0]
    bands = per + 1
    packs = [[None] * -(-bands // WIDE_SLOTS) for _ in range(2)]
    spreads = []
    for cap in range(2):
        across = [[zero] * regs]
        for c in range(regs):
            drag_s[cap, c, at(0), :] = zero
            drag_s[cap, c, at(ext - 1), :] = zero
        for j in range(1, ext - 1):
            d0, d1 = drag_tile(state, rest, cap, j)
            turned = turned_prev(d1, lane)
            across.append([d1[c] - turned[c] for c in range(regs)])
            for c in range(regs):
                drag_s[cap, c, at(j), :] = d0[c]
                if j == 1:
                    kept[0, cap, c] = d0[c]
                if j == ext - 3:
                    kept[1, cap, c] = d0[c]
        across.append([zero] * regs)
        parts = []
        for j in range(1, ext):
            parts.append([
                (drag_s[cap, c, at(j), :] - drag_s[cap, c, at(j, -1), :]) + across[j][c] for c in range(regs)
            ])
        for k in range(bands):
            edge = packed_edge(parts[k][regs - 1], k, lane)
            held = packs[cap][k // WIDE_SLOTS]
            packs[cap][k // WIDE_SLOTS] = edge if held is None else held + edge
        spreads.append(parts)

    def put(block, north, south):
        p3[block] = jnp.where(g == 3, north, south)
        p2[block] = jnp.where((g == 2) | (g == 3), north, south)
        p1[block] = jnp.where(g == 1, north, south)
        mine[block] = jnp.where(g == 0, north, south)

    for k in range(bands):
        for c in range(regs - 1):
            put((tile(k), slice(c * LANES, (c + 1) * LANES)), spreads[0][k][c], spreads[1][k][c])
    for c in range(regs - 1):
        pair = [pack[c] if c < len(pack) else zero for pack in packs]
        put((tile(bands), slice(c * LANES, (c + 1) * LANES)), *pair)


def ice_late(g_ref, rd, ra, rb, nx, outer, h, vel, stress, wind, kept, p2_in, p1_in, p2, p1, fixed, *scratch):
    g = g_ref[0] & 3
    state, rest = scratch[:5], scratch[5:]
    ice_rows, cols = h.shape[1:]
    regs = cols // LANES + 1
    per = ice_rows // SUB
    ext = per + 2
    bands = per + 1
    lane = lane_iota()
    row = row_iota(LANES)
    zero = jnp.zeros((SUB, LANES), F32)
    count = 3
    for k in range(p2.shape[0] // SUB):
        p2[tile(k), :] = p2_in[tile(k), :]
        p1[tile(k), :] = p1_in[tile(k), :]

    def run(group):
        first = 0 if group == 1 else ext - count
        edge_tile = 0 if group == 1 else ext - 1
        flow_of = (ra, rb) if group == 1 else (rb, ra)
        outs = (p1, p2) if group == 1 else (p2, p1)

        def load(cap, jj):
            j = first + jj
            own = own_ice(h, vel, stress, wind, cap)
            if j == edge_tile:
                fields = [late_tile(rd, cap * NICE + f, lane, group == 1) for f in range(NICE)]
            else:
                fields = [
                    split(own[f][tile(j - 1), :]) + [outer[tile((cap * NICE + f) * per + j - 1), :]]
                    for f in range(NICE)
                ]
            for comp in range(2):
                n = comp * ext + j
                edge = wide_outer(nx[3 * cap, tile(n // WIDE_SLOTS), :], n % WIDE_SLOTS, lane)
                fields.append(split(flow_of[cap][tile(n), :]) + [edge])
            return fields

        ice_core(count, load, state, rest, lane)
        for cap in range(2):
            d0, d1 = drag_tile(state, rest, cap, 1)
            turned = turned_prev(d1, lane)
            bits = []
            for c in range(regs):
                across = d1[c] - turned[c]
                if group == 1:
                    here = (d0[c] - from_prev_row(d0[c], zero, row)) + across
                    change = jnp.where(row == 0, pltpu.roll(kept[0, cap, c] - d0[c], 1, 0), 0.0)
                    bits.append((here, change))
                else:
                    here = (d0[c] - from_prev_row(d0[c], kept[1, cap, c], row)) + across
                    bits.append((here, jnp.where(row == 0, -pltpu.roll(d0[c], 1, 0), 0.0)))
                if c + 1 < regs:
                    cut = slice(c * LANES, (c + 1) * LANES)
                    p, q = state[2][cap, c, at(1), :], state[3][cap, c, at(1), :]
                    fixed[cap, 0, :, cut] = state[0][cap, c, at(1), :]
                    fixed[cap, 1, :, cut] = state[1][cap, c, at(1), :]
                    fixed[cap, 2, :, cut] = p + q
                    fixed[cap, 3, :, cut] = p - q
                    fixed[cap, 4, :, cut] = state[4][cap, c, at(1), :]
            out = outs[cap]
            k = 0 if group == 1 else per - 1
            for c in range(regs - 1):
                cut = slice(c * LANES, (c + 1) * LANES)
                out[tile(k), cut] = bits[c][0]
                out[tile(k + 1), cut] = out[tile(k + 1), cut] + bits[c][1] if group == 1 else bits[c][1]
            for n, add in ((k, False), (k + 1, group == 1)):
                c = n // WIDE_SLOTS
                cut = slice(c * LANES, (c + 1) * LANES)
                edge = packed_edge(bits[regs - 1][n - k], n, lane)
                start = (2 * EDGE * (n % WIDE_SLOTS) - EDGE) % LANES
                inside = (lane - start) % LANES < 2 * EDGE if start else lane < 2 * EDGE
                old = out[tile(bands), cut]
                out[tile(bands), cut] = old + edge if add else jnp.where(inside, edge, old)

    @pl.when(g == 1)
    def _():
        run(1)

    @pl.when(g == 2)
    def _():
        run(2)


def ice_results(g_ref, u_s, v_s, p_s, q_s, s_s, fixed, vel_out, stress_out):
    g = g_ref[0] & 3
    per = vel_out.shape[2] // SUB
    regs = u_s.shape[1]
    for cap in range(2):
        for j in range(per):
            for c in range(regs - 1):
                cut = slice(c * LANES, (c + 1) * LANES)
                p, q = p_s[cap, c, at(j + 1), :], q_s[cap, c, at(j + 1), :]
                values = [u_s[cap, c, at(j + 1), :], v_s[cap, c, at(j + 1), :], p + q, p - q, s_s[cap, c, at(j + 1), :]]
                if j == 0 or j == per - 1:
                    late = g == (1 if j == 0 else 2)
                    values = [jnp.where(late, fixed[cap, f, :, cut], value) for f, value in enumerate(values)]
                for f, value in enumerate(values):
                    if f < 2:
                        vel_out[f, cap, tile(j), cut] = value
                    else:
                        stress_out[f - 2, cap, tile(j), cut] = value


def neighbour_sums(ref, j, lane):
    regs = ref.shape[0]
    here = [ref[c, at(j), :] for c in range(regs)]
    after, before = turned_next(here, lane), turned_prev(here, lane)
    return [
        (ref[c, at(j, -1), :] + ref[c, at(j, 1), :]) + (before[c] + after[c]) for c in range(regs)
    ]


def clear_ends(refs, count):
    zero = jnp.zeros((SUB, LANES), F32)
    for ref in refs:
        for c in range(ref.shape[0]):
            ref[c, at(-1), :] = zero
            ref[c, at(count), :] = zero


def ocean_before(g_ref, ra, rc, rd, nx, outer, base, gf, x0, g_s, invd, ra_out, gx_s, x_s, b_s):
    g = g_ref[0] & 3
    rows, cols = base.shape
    regs = cols // LANES + 1
    per = rows // SUB
    ext = per + 2
    lane = lane_iota()
    ocean_first = (outer.shape[0] // SUB - 2 * per) - NOC * per
    clear_ends((g_s, gx_s), ext)
    for j in range(ext):

        def field(i, ref):
            if j == 0 or j == ext - 1:
                n = 2 * NICE + i
                late = g == (1 if j == 0 else 2)
                pairs = zip(late_tile(rd, n, lane, j == 0), low_high(g, ra, rc, nx, n, lane, j == 0))
                return [jnp.where(late, x, y) for x, y in pairs]
            return split(ref[tile(j - 1), :]) + [outer[tile(ocean_first + i * per + j - 1), :]]

        for c, (b, depth, x) in enumerate(zip(field(0, base), field(1, gf), field(2, x0))):
            b_s[c, at(j), :] = b
            g_s[c, at(j), :] = depth
            gx_s[c, at(j), :] = depth * x
            x_s[c, at(j), :] = x
    for j in range(ext):
        around, products = neighbour_sums(g_s, j, lane), neighbour_sums(gx_s, j, lane)
        for c in range(regs):
            depth = g_s[c, at(j), :]
            diag = DAMP + depth * around[c]
            invd[c, at(j), :] = 1.0 / diag
            known = jnp.where(depth > 0.0, b_s[c, at(j), :], 0.0)
            ra_out[c, at(j), :] = known - (diag * x_s[c, at(j), :] - depth * products[c])


def ocean_basis(g_ref, gw, invd, ra, r1, r2, r3, mine, y0_out, y1_out, y2_out, sums,
                sp, u0_s, u1_s, u2_s):
    g = g_ref[0] & 3
    regs = gw.shape[0]
    ext = gw.shape[1] // SUB - 2
    slab = r1.shape[0] // SUB - 2
    lane = lane_iota()
    zero = jnp.zeros((SUB, LANES), F32)
    clear_ends((u0_s, u1_s, u2_s), ext)

    def strip(ref, k):
        n, i = k // WIDE_SLOTS, k % WIDE_SLOTS
        return split(ref[tile(k), :]) + [wide_outer(ref[tile(slab + 1), n * LANES : (n + 1) * LANES], i, lane)]

    def put(j, values):
        for c in range(regs):
            sp[c, at(j), :] = values[c]

    def clear(which):
        for j in which:
            put(j, [zero] * regs)

    def whole(slabs):
        clear([0])
        over = None
        for k, ref in enumerate(slabs):
            values = [strip(ref, t) for t in range(slab + 1)]
            for t in range(slab):
                value = values[t]
                if t == 0 and over is not None:
                    value = [x + y for x, y in zip(value, over)]
                put(1 + slab * k + t, value)
            over = values[slab]
        put(1 + slab * len(slabs), over)

    @pl.when(g == 0)
    def _():
        whole([mine, r1, r2, r3])

    @pl.when(g == 3)
    def _():
        whole([r3, r2, r1, mine])

    @pl.when(g == 1)
    def _():
        clear(range(2, ext))
        put(0, strip(r2, slab - 1))
        put(1, strip(r2, slab))

    @pl.when(g == 2)
    def _():
        clear(range(ext - 1))
        put(ext - 1, strip(r2, 0))

    acc = [[zero] * (regs - 1) for _ in range(6)]

    def add(k, c, left, right):
        acc[k][c] = acc[k][c] + left * right

    for j in range(ext):
        inside = 0 < j < ext - 1
        for c in range(regs):
            depth = gw[c, at(j), :]
            r0 = ra[c, at(j), :] + jnp.where(depth > 0.0, sp[c, at(j), :], 0.0)
            y0 = r0 * invd[c, at(j), :]
            u0_s[c, at(j), :] = depth * y0
            if inside and c + 1 < regs:
                y0_out[c, tile(j - 1), :] = y0
                add(0, c, r0, y0)
    for level, (source, target, before, here) in enumerate(
        ((u0_s, u1_s, y0_out, y1_out), (u1_s, u2_s, y1_out, y2_out))
    ):
        for j in range(ext):
            inside = 0 < j < ext - 1
            around = neighbour_sums(source, j, lane)
            for c in range(regs):
                depth = gw[c, at(j), :]
                w = depth * around[c]
                y = w * invd[c, at(j), :]
                target[c, at(j), :] = depth * y
                if inside and c + 1 < regs:
                    here[c, tile(j - 1), :] = y
                    add(2 * level + 1, c, before[c, tile(j - 1), :], w)
                    add(2 * level + 2, c, w, y)
    for j in range(1, ext - 1):
        around = neighbour_sums(u2_s, j, lane)
        for c in range(regs - 1):
            add(5, c, u2_s[c, at(j), :], around[c])
    lane_sums = []
    for k in range(6):
        total = acc[k][0]
        for c in range(1, regs - 1):
            total = total + acc[k][c]
        lane_sums.append(jnp.sum(total, axis=0, keepdims=True))
    stacked = jnp.concatenate(lane_sums + [jnp.zeros((2, LANES), F32)], axis=0)
    each = jnp.broadcast_to(jnp.sum(stacked, axis=1, keepdims=True), (SUB, LANES))
    sums[...] = jnp.sum(jnp.where(lane == row_iota(LANES), each, 0.0), axis=0, keepdims=True)


def combine(g_ref, parts, x0, y0, y1, y2, out):
    total = jnp.broadcast_to(jnp.sum(parts[...], axis=0), (SUB, LANES))
    lane = lane_iota()
    m = [
        jnp.broadcast_to(jnp.sum(jnp.where(lane == k, total, 0.0), axis=1, keepdims=True), (SUB, LANES))
        for k in range(6)
    ]

    def dot(left, right, image):
        value = None
        for i, a in enumerate(left):
            for j, b in enumerate(right):
                moment = m[i + j] - m[i + j + 1] if image else m[i + j]
                term = a * b * moment
                value = term if value is None else value + term
        return value

    z = [jnp.ones((SUB, LANES), F32)]
    p = z
    rz = m[0]
    coef = [0.0, 0.0, 0.0]
    for step in range(ITERS):
        alpha = rz / dot(p, p, True)
        for i, a in enumerate(p):
            coef[i] = coef[i] + alpha * a
        if step + 1 < ITERS:
            image = [a for a in p] + [jnp.zeros((SUB, LANES), F32)]
            for i, a in enumerate(p):
                image[i + 1] = image[i + 1] - a
            z = [(z[i] if i < len(z) else 0.0) - alpha * image[i] for i in range(len(image))]
            fresh = dot(z, z, False)
            beta = fresh / rz
            p = [z[i] + beta * p[i] if i < len(p) else z[i] for i in range(len(z))]
            rz = fresh
    for k in range(x0.shape[0] // SUB):
        t = tile(k)
        for c in range(y0.shape[0]):
            cut = slice(c * LANES, (c + 1) * LANES)
            move = coef[0] * y0[c, t, :] + coef[1] * y1[c, t, :] + coef[2] * y2[c, t, :]
            out[t, cut] = x0[t, cut] + move


def shards(
    base_rhs,
    depth,
    ssh_prev,
    currents,
    land_blocks,
    ice_thick,
    ice_blocks,
    ice_vel,
    ice_stress,
    wind,
):
    groups = lax.axis_size("grp")
    tiles = lax.axis_size("tile")
    assert groups == 4
    assert tiles % 2 == 0
    g = (lax.axis_index("grp") + groups * (lax.axis_index("tile") & 1)).astype(jnp.int32).reshape(1)
    rows, cols = base_rhs.shape
    ice_rows = ice_thick.shape[1]
    assert rows == groups * ice_rows
    slab = ice_rows + 2 * SUB
    strip = (2 * slab, cols)
    c, a, b, token = call(
        pack_rows,
        [(2 * (ice_rows + SUB), cols), strip, strip, (SUB, LANES)],
        [g, base_rhs, depth, ssh_prev, currents, land_blocks, ice_thick, ice_blocks, ice_vel, ice_stress, wind],
        scratch=[
            (2, 2, SUB, cols), (2, 2, SUB, cols),
            (land_blocks.shape, jnp.int32), (ice_blocks.shape, jnp.int32),
        ],
        sems=48,
        hbm=True,
    )
    rc = lax.ppermute(c, "grp", DIAGONAL)
    ra = lax.ppermute(a, "grp", FIRST)
    rb = lax.ppermute(b, "grp", SECOND)

    own = sum(own_count(rows, ice_rows))
    packed = (-(-own // SLOTS) * SUB, LANES)
    gf, h, inner, cross = call(
        pack_own,
        [(rows, cols), (2, ice_rows, cols), packed, packed],
        [g, token, base_rhs, depth, ssh_prev, currents, land_blocks, ice_thick, ice_blocks, ice_vel, ice_stress,
         wind],
    )
    inner = lax.ppermute(inner, "tile", [(i, i ^ 1) for i in range(tiles)])
    odd = range(1, tiles - 1, 2)
    cross = lax.ppermute(cross, "tile", [(i, i + 1) for i in odd] + [(i + 1, i) for i in odd])
    strip_tiles = 2 * (slab // SUB)
    narrow_rows = -(-strip_tiles // WIDE_SLOTS) * SUB
    tail = -(-narrow_rows * LANES // (SUB * cols)) * SUB
    outer, narrow, d = call(
        pack_narrow,
        [(own * SUB, LANES), (groups, narrow_rows, LANES), ((2 * NICE + 2) * SUB + tail, cols)],
        [g, inner, cross, h, gf, base_rhs, ssh_prev, ice_vel, ice_stress, wind],
    )
    nx = lax.all_to_all(narrow, "grp", 0, 0, tiled=True)
    d, nx = lax.optimization_barrier((d, nx))
    rd = lax.ppermute(d, "grp", FIRST)

    back = (ice_rows + 2 * SUB, cols)
    regs = cols // LANES + 1
    held = (2, regs, slab + 2 * SUB, LANES)
    *state, p3, p2, p1, mine, kept = call(
        ice_steps,
        [held] * 5 + [back] * 4 + [(2, 2, regs, SUB, LANES)],
        [g, ra, rb, rc, nx, outer, h, ice_vel, ice_stress, wind, currents],
        scratch=[held] * 11,
        mib=32,
        flops=20000000,
    )
    p2, p1, fixed = call(
        ice_late,
        [back, back, (2, 5, SUB, cols)],
        [g, rd, ra, rb, nx, outer, h, ice_vel, ice_stress, wind, kept, p2, p1],
        scratch=[(2, regs, 5 * SUB, LANES)] * 16,
        flops=20000000,
    )
    r3 = lax.ppermute(p3, "grp", [(3, 0), (0, 3)])
    r2 = lax.ppermute(p2, "grp", SECOND)
    r1 = lax.ppermute(p1, "grp", FIRST)
    velocity, stress = call(ice_results, [ice_vel.shape, ice_stress.shape], [g, *state, fixed], flops=10000000)

    field = (regs, rows + 4 * SUB, LANES)
    gw, invd, known = call(
        ocean_before,
        [field] * 3,
        [g, ra, rc, rd, nx, outer, base_rhs, gf, ssh_prev],
        scratch=[field] * 3,
        flops=20000000,
    )
    y0, y1, y2, sums = call(
        ocean_basis,
        [(regs - 1, rows, LANES)] * 3 + [(1, LANES)],
        [g, gw, invd, known, r1, r2, r3, mine],
        scratch=[field] * 4,
    )
    devices = groups * tiles
    shared = lax.all_to_all(
        jnp.broadcast_to(sums[None], (devices, 1, LANES)), ("grp", "tile"), 0, 0, tiled=True
    )
    (ssh,) = call(combine, [(rows, cols)], [g, shared, ssh_prev, y0, y1, y2])
    return ssh, velocity, stress


def solution(mesh):
    return jax.shard_map(
        shards,
        mesh=mesh,
        in_specs=(
            P("grp", "tile"),
            P("grp", "tile"),
            P("grp", "tile"),
            P(None, "grp", "tile"),
            P("grp", "tile"),
            P(None, "grp", "tile"),
            P(None, "grp", "tile"),
            P(None, None, "grp", "tile"),
            P(None, None, "grp", "tile"),
            P(None, None, "grp", "tile"),
        ),
        out_specs=(P("grp", "tile"), P(None, None, "grp", "tile"), P(None, None, "grp", "tile")),
        check_vma=False,
    )
```

```python
import jax
import jax.numpy as jnp
from jax import lax
from jax.experimental import pallas as pl
from jax.experimental.pallas import tpu as pltpu
from jax.sharding import PartitionSpec as P


BS = 8
NSUB = 8
ITERS = 3

DAMP = 0.05
RELAX = 0.2
STRENGTH = 0.5
DRAG = 1.0
STEP = 0.5

F32 = jnp.float32
SUB = 8
LANES = 128
EDGE = 16
SLOTS = LANES // EDGE
WIDE_SLOTS = LANES // (2 * EDGE)
GROUP = 4
SKEW = 1
NICE = 8
FIRST = [(0, 1), (1, 0), (2, 3), (3, 2)]
SECOND = [(0, 2), (2, 0), (1, 3), (3, 1)]
DIAGONAL = [(0, 3), (3, 0), (1, 2), (2, 1)]
NOC = 3


def vmem():
    return pl.BlockSpec(memory_space=pltpu.VMEM)


def smem():
    return pl.BlockSpec(memory_space=pltpu.SMEM)


def call(body, outs, ins, scratch=(), sems=0, hbm=False, mib=24, flops=1000000):
    shapes = tuple(jax.ShapeDtypeStruct(s, F32) for s in outs)
    other = pl.BlockSpec(memory_space=pltpu.HBM) if hbm else vmem()
    specs = [smem() if i == 0 else other for i in range(len(ins))]
    held = [pltpu.VMEM(*s) if isinstance(s[0], tuple) else pltpu.VMEM(s, F32) for s in scratch]
    if sems:
        held.append(pltpu.SemaphoreType.DMA((sems,)))
    return pl.pallas_call(
        body,
        out_shape=shapes,
        in_specs=specs,
        out_specs=tuple(vmem() for _ in outs),
        scratch_shapes=held,
        cost_estimate=pl.CostEstimate(flops=flops, bytes_accessed=4000000, transcendentals=0),
        compiler_params=pltpu.CompilerParams(vmem_limit_bytes=mib * 1024 * 1024),
    )(*([ins[0]] + [pltpu.with_memory_space_constraint(x, pltpu.HBM) for x in ins[1:]] if hbm else ins))


def tile(k):
    return slice(k * SUB, k * SUB + SUB)


def expanded_cols(blocks):
    count = blocks.shape[-1]
    row = lax.broadcasted_iota(jnp.int32, (count, count * BS), 0) * BS
    col = lax.broadcasted_iota(jnp.int32, (count, count * BS), 1)
    spread = ((col >= row) & (col < row + BS)).astype(F32)
    return jnp.dot(blocks.astype(F32), spread, preferred_element_type=F32)


def row_iota(cols):
    return lax.broadcasted_iota(jnp.int32, (SUB, cols), 0)


def lane_iota():
    return lax.broadcasted_iota(jnp.int32, (SUB, LANES), 1)


def from_prev_row(here, before, row):
    return pltpu.roll(jnp.where(row == SUB - 1, before, here), 1, 0)


def own_tile(cur, comp, first, j):
    last = cur.shape[1] // SUB - 1
    t = jnp.clip(first + j, 0, last)
    return cur[comp, pl.ds(pl.multiple_of(t * SUB, SUB), SUB), :]


def half_and_half(base, depth, last):
    row = row_iota(base.shape[1])
    return jnp.where(row >= SUB // 2 if last else row < SUB // 2, base, pltpu.roll(depth, SUB // 2, 0))


def halved(value, which, last):
    row = row_iota(value.shape[1])
    value = pltpu.roll(value, SUB // 2, 0) if which else value
    return jnp.where(row >= SUB // 2 if last else row < SUB // 2, value, 0.0)


def strip_tile(ref, n, low):
    if n < 2 * NICE:
        return ref[tile(n), :]
    if n == 2 * NICE + 2:
        return ref[tile(2 * NICE + 1), :]
    return halved(ref[tile(2 * NICE), :], n - 2 * NICE, low)


def pack_rows(g_ref, base, depth, x0, cur, land, thick, iceb, vel, stress, wind,
              c, a, b, token, thick_s, depth_s, land_s, iceb_s, sems):
    g = g_ref[0] & 3
    rows, cols = base.shape
    ice_rows = thick.shape[1]
    slab = ice_rows + 2 * SUB
    token[...] = jnp.zeros((SUB, LANES), F32)

    def run(slabs, halos):
        copies = []

        def copy(src, dst):
            made = pltpu.make_async_copy(src, dst, sems.at[len(copies)])
            made.start()
            copies.append(made)

        for out, dest in slabs:
            start = ice_rows * dest - SUB
            first, last = max(start, 0), min(start + slab, rows)
            for comp in range(2):
                begin = comp * (last - first)
                copy(cur.at[comp, first:last, :], out.at[begin : begin + last - first, :])
        if halos:
            copy(land, land_s)
            copy(iceb, iceb_s)
        for i, (out, last) in enumerate(halos):
            r = slice(ice_rows - SUB, ice_rows) if last else slice(0, SUB)
            ro = slice(rows - SUB, rows) if last else slice(0, SUB)
            for cap in range(2):
                copy(thick.at[cap, r, :], thick_s.at[i, cap])
                n = cap * NICE + 1
                pieces = [vel.at[0, cap, r, :], vel.at[1, cap, r, :]]
                pieces += [stress.at[k, cap, r, :] for k in range(3)]
                pieces += [wind.at[k, cap, r, :] for k in range(2)]
                for piece in pieces:
                    copy(piece, out.at[tile(n), :])
                    n += 1
            copy(depth.at[ro, :], depth_s.at[i, 0])
            copy(base.at[ro, :], depth_s.at[i, 1])
            copy(x0.at[ro, :], out.at[tile(2 * NICE + 1), :])
            for k in range(2 * NICE + 2, out.shape[0] // SUB):
                out[tile(k), :] = jnp.zeros((SUB, cols), F32)
        for made in copies:
            made.wait()
        if halos:
            wet = expanded_cols(land_s[...])
            covers = [expanded_cols(iceb_s[cap]) for cap in range(2)]
        for i, (out, last) in enumerate(halos):
            for cap in range(2):
                k = covers[cap].shape[0] - 1 if last else 0
                out[tile(cap * NICE), :] = thick_s[i, cap] * covers[cap][k : k + 1, :]
            k = wet.shape[0] - 1 if last else 0
            out[tile(2 * NICE), :] = half_and_half(depth_s[i, 1], depth_s[i, 0] * wet[k : k + 1, :], last)

    @pl.when(g == 0)
    def _():
        run([(c, 3), (a, 1), (b, 2)], [])

    @pl.when(g == 3)
    def _():
        run([(c, 0), (a, 2), (b, 1)], [])

    @pl.when(g == 1)
    def _():
        run([], [(a, False), (c, True)])

    @pl.when(g == 2)
    def _():
        run([], [(a, True), (c, False)])


def pack_own(g_ref, token, base, depth, x0, cur, land, thick, iceb, vel, stress, wind, gf, h, inner, cross):
    cols = base.shape[1]
    even = g_ref[0] < 4
    lane = lane_iota()
    slot = lane // EDGE
    state = {"n": 0, "l": None, "r": None}

    def emit(first, last):
        n = state["n"]
        s = n % SLOTS
        both = jnp.where(lane < EDGE, first, last)
        both = pltpu.roll(both, EDGE * s, 1) if s else both
        if s == 0:
            state["l"] = state["r"] = both
        else:
            state["l"] = jnp.where(slot == s, both, state["l"])
            state["r"] = jnp.where(slot == s - 1, both, state["r"])
        if s == SLOTS - 1:
            k = n // SLOTS
            inner[tile(k), :] = jnp.where(even, state["r"], state["l"])
            cross[tile(k), :] = jnp.where(even, state["l"], state["r"])
        state["n"] = n + 1

    def emit_all(ref):
        for k in range(ref.shape[0] // SUB):
            emit(ref[tile(k), :LANES], ref[tile(k), cols - LANES :])

    wet = expanded_cols(land[...])
    for k in range(depth.shape[0] // SUB):
        gf[tile(k), :] = depth[tile(k), :] * wet[k : k + 1, :]
    for cap in range(2):
        cover = expanded_cols(iceb[cap])
        for k in range(thick.shape[1] // SUB):
            h[cap, tile(k), :] = thick[cap, tile(k), :] * cover[k : k + 1, :]
    for cap in range(2):
        for ref in own_ice(h, vel, stress, wind, cap):
            emit_all(ref)
    for ref in (base, gf, x0):
        emit_all(ref)
    for comp in range(2):
        emit_all(cur.at[comp])
    while state["n"] % SLOTS:
        emit(jnp.zeros((SUB, LANES), F32), jnp.zeros((SUB, LANES), F32))


def own_ice(h, vel, stress, wind, cap):
    fields = [h.at[cap], vel.at[0, cap], vel.at[1, cap]]
    fields += [stress.at[i, cap] for i in range(3)]
    return fields + [wind.at[i, cap] for i in range(2)]


def own_count(rows, ice_rows):
    return 2 * NICE * (ice_rows // SUB), NOC * (rows // SUB), 2 * (rows // SUB)


def halo_tiles(rows, ice_rows, last):
    ice_tiles, ocean_tiles = ice_rows // SUB, rows // SUB
    picked = [n * ice_tiles + (ice_tiles - 1 if last else 0) for n in range(2 * NICE)]
    start = 2 * NICE * ice_tiles
    return picked + [start + i * ocean_tiles + (ocean_tiles - 1 if last else 0) for i in range(NOC)]


def pack_narrow(g_ref, inner, cross, h, gf, base, x0, vel, stress, wind, outer, narrow, d):
    g = g_ref[0] & 3
    rows, cols = base.shape
    ice_rows = h.shape[1]
    lane = lane_iota()
    count = sum(own_count(rows, ice_rows))
    batch = 32
    for n in range(0, count, batch):
        made = [outer_columns(g_ref[0] < 4, inner, cross, i, lane) for i in range(n, min(n + batch, count))]
        for i, value in enumerate(made):
            outer[tile(n + i), :] = value
    packed = narrow.shape[1] // SUB

    def pack(put, tiles):
        for k in range(packed):
            value = None
            for i in range(WIDE_SLOTS):
                n = k * WIDE_SLOTS + i
                if n < len(tiles):
                    one = tiles[n]()
                    one = pltpu.roll(one, i * 2 * EDGE, 1) if i else one
                    value = one if value is None else value + one
            put(k, jnp.zeros((SUB, LANES), F32) if value is None else value)

    def picked(n):
        return lambda: outer[tile(n), :]

    def slab(dest):
        start = sum(own_count(rows, ice_rows)[:2])
        per = rows // SUB
        tiles = []
        for comp in range(2):
            for j in range(ice_rows // SUB + 2):
                t = ice_rows // SUB * dest - 1 + j
                inside = 0 <= t < per
                tiles.append(picked(start + comp * per + t) if inside else lambda: jnp.zeros((SUB, LANES), F32))
        return tiles

    def halo(last):
        return [picked(n) for n in halo_tiles(rows, ice_rows, last)]

    def send(dest, tiles):
        def put(k, value):
            narrow[dest, tile(k), :] = value

        pack(put, tiles)

    def strip(last):
        r = slice(ice_rows - SUB, ice_rows) if last else slice(0, SUB)
        ro = slice(rows - SUB, rows) if last else slice(0, SUB)
        n = 0
        for cap in range(2):
            for ref in own_ice(h, vel, stress, wind, cap):
                d[tile(n), :] = ref[r, :]
                n += 1
        d[tile(n), :] = half_and_half(base[ro, :], gf[ro, :], last)
        d[tile(n + 1), :] = x0[ro, :]
        n += 2
        per = cols // LANES

        def put(k, value):
            c = k % per
            d[tile(n + k // per), c * LANES : (c + 1) * LANES] = value

        pack(put, halo(last))

    @pl.when(g == 0)
    def _():
        send(0, [])
        send(1, slab(1))
        send(2, slab(2))
        send(3, slab(3))
        strip(True)

    @pl.when(g == 1)
    def _():
        send(0, halo(False))
        send(1, [])
        send(2, halo(True))
        send(3, [])

    @pl.when(g == 2)
    def _():
        send(0, [])
        send(1, halo(False))
        send(2, [])
        send(3, halo(True))

    @pl.when(g == 3)
    def _():
        send(0, slab(0))
        send(1, slab(1))
        send(2, slab(2))
        send(3, [])
        strip(False)


def wide_outer(value, i, lane):
    value = pltpu.roll(value, LANES - 2 * EDGE * i, 1) if i else value
    return jnp.where((lane < EDGE) | (lane >= LANES - EDGE), value, 0.0)


def late_tile(rd, n, lane, low):
    per = rd.shape[1] // LANES
    k, i = n // WIDE_SLOTS, n % WIDE_SLOTS
    tail = rd[tile(2 * NICE + 2 + k // per), (k % per) * LANES : (k % per + 1) * LANES]
    return split(strip_tile(rd, n, low)) + [wide_outer(tail, i, lane)]


def low_high(g, ra, rc, nx, n, lane, low):
    k, i = n // WIDE_SLOTS, n % WIDE_SLOTS
    pieces = [(2, rc, 1), (3, ra, 2)] if low else [(0, ra, 1), (1, rc, 2)]
    inner = jnp.zeros((SUB, ra.shape[1]), F32)
    packed = jnp.zeros((SUB, LANES), F32)
    for group, ref, source in pieces:
        inner = jnp.where(g == group, strip_tile(ref, n, low), inner)
        packed = jnp.where(g == group, nx[source, tile(k), :], packed)
    return split(inner) + [wide_outer(packed, i, lane)]


def outer_columns(even, inner, cross, n, lane):
    s, k = n % SLOTS, n // SLOTS
    from_right = jnp.where(even, inner[tile(k), :], cross[tile(k), :])
    from_left = jnp.where(even, cross[tile(k), :], inner[tile(k), :])
    both = jnp.where(lane // EDGE == s, from_right, from_left)
    both = pltpu.roll(both, LANES - EDGE * s, 1) if s else both
    return jnp.where((lane < EDGE) | (lane >= LANES - EDGE), both, 0.0)


def split(value):
    return [value[:, c * LANES : (c + 1) * LANES] for c in range(value.shape[1] // LANES)]


def turned_next(regs, lane):
    n = len(regs)
    return [pltpu.roll(jnp.where(lane == 0, regs[(c + 1) % n], regs[c]), LANES - 1, 1) for c in range(n)]


def turned_prev(regs, lane):
    n = len(regs)
    return [pltpu.roll(jnp.where(lane == LANES - 1, regs[c - 1], regs[c]), 1, 1) for c in range(n)]


KEEP = 1.0 / (1.0 + RELAX)


def at(j, shift=0):
    return slice(SUB * (j + 1) + shift, SUB * (j + 2) + shift)


def ice_core(count, load, state, rest, lane):
    u_s, v_s, p_s, q_s, s_s = state
    un_s, vn_s, qp_s, sp_s, a_s, m_s, w_s, fx_s, fy_s, f0_s, f1_s = rest
    regs = u_s.shape[1]
    zero = jnp.zeros((SUB, LANES), F32)
    for cap in range(2):
        for c in range(regs):
            for ref in (p_s, s_s):
                ref[cap, c, at(-1), :] = zero
            for ref in (u_s, v_s):
                ref[cap, c, at(count), :] = zero
        for j in range(count):
            fields = load(cap, j)
            for c in range(regs):
                hh, u, v, s0, s1, s2, w0, w1, f0, f1 = (f[c] for f in fields)
                u_s[cap, c, at(j), :] = u
                v_s[cap, c, at(j), :] = v
                p_s[cap, c, at(j), :] = 0.5 * (s0 + s1)
                q_s[cap, c, at(j), :] = 0.5 * (s0 - s1)
                s_s[cap, c, at(j), :] = s2
                inv = jnp.where(hh > 0.0, 1.0 / (hh + (1.0 + STEP * DRAG)), 0.0)
                quick = STEP * inv
                a_s[cap, c, at(j), :] = hh * (RELAX * STRENGTH * KEEP)
                m_s[cap, c, at(j), :] = (hh + 1.0) * inv
                w_s[cap, c, at(j), :] = quick
                fx_s[cap, c, at(j), :] = quick * (w0 + DRAG * f0)
                fy_s[cap, c, at(j), :] = quick * (w1 + DRAG * f1)
                f0_s[cap, c, at(j), :] = f0
                f1_s[cap, c, at(j), :] = f1
    for j in range(count):
        for cap in range(2):
            for ref, source in ((un_s, u_s), (vn_s, v_s)):
                turned = turned_next([source[cap, c, at(j), :] for c in range(regs)], lane)
                for c in range(regs):
                    ref[cap, c, at(j), :] = turned[c]

    def stress_tile(cap, j):
        qs, ss = [], []
        for c in range(regs):
            u, v = u_s[cap, c, at(j), :], v_s[cap, c, at(j), :]
            ux = u_s[cap, c, at(j, 1), :] - u
            vx = v_s[cap, c, at(j, 1), :] - v
            uy = un_s[cap, c, at(j), :] - u
            vy = vn_s[cap, c, at(j), :] - v
            es = uy + vx
            half = ux * ux + vy * vy
            a = a_s[cap, c, at(j), :]
            ratio = a * lax.rsqrt((half + half) + (es * es + 1.0))
            low = 0.5 * a
            q = q_s[cap, c, at(j), :] * KEEP + (ratio * vy - low)
            s = s_s[cap, c, at(j), :] * KEEP + ratio * es
            p_s[cap, c, at(j), :] = p_s[cap, c, at(j), :] * KEEP + (ratio * ux - low)
            q_s[cap, c, at(j), :] = q
            s_s[cap, c, at(j), :] = s
            qs.append(q)
            ss.append(s)
        for ref, turned in ((qp_s, turned_prev(qs, lane)), (sp_s, turned_prev(ss, lane))):
            for c in range(regs):
                ref[cap, c, at(j), :] = turned[c]

    def velocity_tile(cap, j):
        us, vs = [], []
        for c in range(regs):
            s = s_s[cap, c, at(j), :]
            force_x = (p_s[cap, c, at(j), :] - p_s[cap, c, at(j, -1), :]) + (s - sp_s[cap, c, at(j), :])
            force_y = (q_s[cap, c, at(j), :] - qp_s[cap, c, at(j), :]) + (s - s_s[cap, c, at(j, -1), :])
            m, quick = m_s[cap, c, at(j), :], w_s[cap, c, at(j), :]
            u = m * u_s[cap, c, at(j), :] + (quick * force_x + fx_s[cap, c, at(j), :])
            v = m * v_s[cap, c, at(j), :] + (quick * force_y + fy_s[cap, c, at(j), :])
            u_s[cap, c, at(j), :] = u
            v_s[cap, c, at(j), :] = v
            us.append(u)
            vs.append(v)
        for ref, turned in ((un_s, turned_next(us, lane)), (vn_s, turned_next(vs, lane))):
            for c in range(regs):
                ref[cap, c, at(j), :] = turned[c]

    def subcycle(_, carry):
        for j in range(count + SKEW):
            for cap in range(2):
                if j < count:
                    stress_tile(cap, j)
                if j >= SKEW:
                    velocity_tile(cap, j - SKEW)
        return carry

    lax.fori_loop(0, NSUB, subcycle, 0)


def drag_tile(state, rest, cap, j):
    u_s, v_s = state[:2]
    m_s, f0_s, f1_s = rest[5], rest[9], rest[10]
    d0, d1 = [], []
    for c in range(u_s.shape[1]):
        iced = m_s[cap, c, at(j), :] > 0.0
        d0.append(jnp.where(iced, DRAG * (u_s[cap, c, at(j), :] - f0_s[cap, c, at(j), :]), 0.0))
        d1.append(jnp.where(iced, DRAG * (v_s[cap, c, at(j), :] - f1_s[cap, c, at(j), :]), 0.0))
    return d0, d1


def tail_regs(per, inner):
    used = -(-(per + 1) // WIDE_SLOTS) + 1
    return -(-used // inner) * inner


def stacked_rows(values):
    row = row_iota(LANES)
    total = jnp.where(row == 0, values[0], 0.0)
    for c in range(1, len(values)):
        total = total + jnp.where(row == c, pltpu.roll(values[c], c, 0), 0.0)
    return total


def packed_edge(edge, k, lane):
    edge = jnp.where((lane < EDGE) | (lane >= LANES - EDGE), edge, 0.0)
    i = k % WIDE_SLOTS
    return pltpu.roll(edge, 2 * EDGE * i, 1) if i else edge


def ice_steps(g_ref, ra, rb, rc, nx, outer, h, vel, stress, wind, cur,
              u_s, v_s, p_s, q_s, s_s, p3, p2, p1, mine, kept, *rest):
    g = g_ref[0] & 3
    state = (u_s, v_s, p_s, q_s, s_s)
    ice_rows, cols = h.shape[1:]
    rows = cur.shape[1]
    regs = cols // LANES + 1
    per = ice_rows // SUB
    ext = per + 2
    lane = lane_iota()
    zero = jnp.zeros((SUB, LANES), F32)
    flow_first = sum(own_count(rows, ice_rows)[:2])

    def flow(cap, comp, j):
        n = comp * ext + j
        t = tile(n)
        k, i = n // WIDE_SLOTS, n % WIDE_SLOTS
        far = j - cap
        diag = rc[tile(comp * (per + 1) + far), :] if 0 <= far <= per else jnp.zeros((SUB, cols), F32)
        here = jnp.clip(per * g - 1 + j, 0, rows // SUB - 1)
        own = own_tile(cur, comp, per * g - 1, j)
        spot = pl.multiple_of((flow_first + comp * (rows // SUB) + here) * SUB, SUB)
        own_outer = outer[pl.ds(spot, SUB), :]
        if cap == 0:
            inner = jnp.where(g == 0, own, jnp.where(g == 1, ra[t, :], jnp.where(g == 2, rb[t, :], diag)))
            edge = jnp.where(g == 0, own_outer, wide_outer(nx[0, tile(k), :], i, lane))
        else:
            inner = jnp.where(g == 3, own, jnp.where(g == 2, ra[t, :], jnp.where(g == 1, rb[t, :], diag)))
            edge = jnp.where(g == 3, own_outer, wide_outer(nx[3, tile(k), :], i, lane))
        return split(inner) + [edge]

    flows = {}

    def load(cap, j):
        own = own_ice(h, vel, stress, wind, cap)
        if j % GROUP == 0:
            flows.clear()
            for i in range(j, min(j + GROUP, ext)):
                flows[i] = [flow(cap, comp, i) for comp in range(2)]
        if j == 0 or j == ext - 1:
            fields = [low_high(g, ra, rc, nx, cap * NICE + f, lane, j == 0) for f in range(NICE)]
        else:
            fields = [
                split(own[f][tile(j - 1), :]) + [outer[tile((cap * NICE + f) * per + j - 1), :]]
                for f in range(NICE)
            ]
        return fields + flows[j]

    ice_core(ext, load, state, rest, lane)
    drag_s = rest[0]
    bands = per + 1
    packs = [[None] * -(-bands // WIDE_SLOTS) for _ in range(2)]
    spreads = []
    for cap in range(2):
        across = [[zero] * regs]
        for c in range(regs):
            drag_s[cap, c, at(0), :] = zero
            drag_s[cap, c, at(ext - 1), :] = zero
        for j in range(1, ext - 1):
            d0, d1 = drag_tile(state, rest, cap, j)
            turned = turned_prev(d1, lane)
            across.append([d1[c] - turned[c] for c in range(regs)])
            for c in range(regs):
                drag_s[cap, c, at(j), :] = d0[c]
                if j == 1:
                    kept[0, cap, c] = d0[c]
                if j == ext - 3:
                    kept[1, cap, c] = d0[c]
        across.append([zero] * regs)
        parts = []
        for j in range(1, ext):
            parts.append([
                (drag_s[cap, c, at(j), :] - drag_s[cap, c, at(j, -1), :]) + across[j][c] for c in range(regs)
            ])
        for k in range(bands):
            edge = packed_edge(parts[k][regs - 1], k, lane)
            held = packs[cap][k // WIDE_SLOTS]
            packs[cap][k // WIDE_SLOTS] = edge if held is None else held + edge
        spreads.append(parts)

    def put(block, north, south):
        p3[block] = jnp.where(g == 3, north, south)
        p2[block] = jnp.where((g == 2) | (g == 3), north, south)
        p1[block] = jnp.where(g == 1, north, south)
        mine[block] = jnp.where(g == 0, north, south)

    for k in range(per):
        for c in range(regs - 1):
            put((tile(k), slice(c * LANES, (c + 1) * LANES)), spreads[0][k][c], spreads[1][k][c])
    for cap in range(2):
        packs[cap].append(stacked_rows(spreads[cap][per][: regs - 1]))
    for c in range(tail_regs(per, regs - 1)):
        pair = [pack[c] if c < len(pack) else zero for pack in packs]
        put((tile(per + c // (regs - 1)), slice(c % (regs - 1) * LANES, (c % (regs - 1) + 1) * LANES)), *pair)


def ice_late(g_ref, rd, ra, rb, nx, outer, h, vel, stress, wind, kept, p2_in, p1_in, p2, p1, fixed, *scratch):
    g = g_ref[0] & 3
    state, rest = scratch[:5], scratch[5:]
    ice_rows, cols = h.shape[1:]
    regs = cols // LANES + 1
    per = ice_rows // SUB
    ext = per + 2
    lane = lane_iota()
    row = row_iota(LANES)
    zero = jnp.zeros((SUB, LANES), F32)
    count = 3
    for k in range(p2.shape[0] // SUB):
        p2[tile(k), :] = p2_in[tile(k), :]
        p1[tile(k), :] = p1_in[tile(k), :]

    def run(group):
        first = 0 if group == 1 else ext - count
        edge_tile = 0 if group == 1 else ext - 1
        flow_of = (ra, rb) if group == 1 else (rb, ra)
        outs = (p1, p2) if group == 1 else (p2, p1)

        def load(cap, jj):
            j = first + jj
            own = own_ice(h, vel, stress, wind, cap)
            if j == edge_tile:
                fields = [late_tile(rd, cap * NICE + f, lane, group == 1) for f in range(NICE)]
            else:
                fields = [
                    split(own[f][tile(j - 1), :]) + [outer[tile((cap * NICE + f) * per + j - 1), :]]
                    for f in range(NICE)
                ]
            for comp in range(2):
                n = comp * ext + j
                edge = wide_outer(nx[3 * cap, tile(n // WIDE_SLOTS), :], n % WIDE_SLOTS, lane)
                fields.append(split(flow_of[cap][tile(n), :]) + [edge])
            return fields

        ice_core(count, load, state, rest, lane)
        for cap in range(2):
            d0, d1 = drag_tile(state, rest, cap, 1)
            turned = turned_prev(d1, lane)
            bits = []
            for c in range(regs):
                across = d1[c] - turned[c]
                if group == 1:
                    here = (d0[c] - from_prev_row(d0[c], zero, row)) + across
                    change = jnp.where(row == 0, pltpu.roll(kept[0, cap, c] - d0[c], 1, 0), 0.0)
                    bits.append((here, change))
                else:
                    here = (d0[c] - from_prev_row(d0[c], kept[1, cap, c], row)) + across
                    bits.append((here, jnp.where(row == 0, -pltpu.roll(d0[c], 1, 0), 0.0)))
                if c + 1 < regs:
                    cut = slice(c * LANES, (c + 1) * LANES)
                    p, q = state[2][cap, c, at(1), :], state[3][cap, c, at(1), :]
                    fixed[cap, 0, :, cut] = state[0][cap, c, at(1), :]
                    fixed[cap, 1, :, cut] = state[1][cap, c, at(1), :]
                    fixed[cap, 2, :, cut] = p + q
                    fixed[cap, 3, :, cut] = p - q
                    fixed[cap, 4, :, cut] = state[4][cap, c, at(1), :]
            out = outs[cap]
            k = 0 if group == 1 else per - 1

            def spot(c):
                c, t = c % (regs - 1), c // (regs - 1)
                return tile(per + t), slice(c * LANES, (c + 1) * LANES)

            for c in range(regs - 1):
                cut = slice(c * LANES, (c + 1) * LANES)
                out[tile(k), cut] = bits[c][0]
                if group == 1:
                    out[tile(k + 1), cut] = out[tile(k + 1), cut] + bits[c][1]
            if group == 2:
                out[spot(-(-(per + 1) // WIDE_SLOTS))] = stacked_rows([b[1] for b in bits[: regs - 1]])
            for n, add in ((k, False), (k + 1, group == 1)):
                c = n // WIDE_SLOTS
                edge = packed_edge(bits[regs - 1][n - k], n, lane)
                start = (2 * EDGE * (n % WIDE_SLOTS) - EDGE) % LANES
                inside = (lane - start) % LANES < 2 * EDGE if start else lane < 2 * EDGE
                old = out[spot(c)]
                out[spot(c)] = old + edge if add else jnp.where(inside, edge, old)

    @pl.when(g == 1)
    def _():
        run(1)

    @pl.when(g == 2)
    def _():
        run(2)


def ice_results(g_ref, u_s, v_s, p_s, q_s, s_s, fixed, vel_out, stress_out):
    g = g_ref[0] & 3
    per = vel_out.shape[2] // SUB
    regs = u_s.shape[1]
    for cap in range(2):
        for j in range(per):
            for c in range(regs - 1):
                cut = slice(c * LANES, (c + 1) * LANES)
                p, q = p_s[cap, c, at(j + 1), :], q_s[cap, c, at(j + 1), :]
                values = [u_s[cap, c, at(j + 1), :], v_s[cap, c, at(j + 1), :], p + q, p - q, s_s[cap, c, at(j + 1), :]]
                if j == 0 or j == per - 1:
                    late = g == (1 if j == 0 else 2)
                    values = [jnp.where(late, fixed[cap, f, :, cut], value) for f, value in enumerate(values)]
                for f, value in enumerate(values):
                    if f < 2:
                        vel_out[f, cap, tile(j), cut] = value
                    else:
                        stress_out[f - 2, cap, tile(j), cut] = value


def neighbour_sums(ref, j, lane):
    regs = ref.shape[0]
    here = [ref[c, at(j), :] for c in range(regs)]
    after, before = turned_next(here, lane), turned_prev(here, lane)
    return [
        (ref[c, at(j, -1), :] + ref[c, at(j, 1), :]) + (before[c] + after[c]) for c in range(regs)
    ]


def clear_ends(refs, count):
    zero = jnp.zeros((SUB, LANES), F32)
    for ref in refs:
        for c in range(ref.shape[0]):
            ref[c, at(-1), :] = zero
            ref[c, at(count), :] = zero


def ocean_before(g_ref, ra, rc, rd, nx, outer, base, gf, x0, g_s, invd, ra_out, gx_s, x_s, b_s):
    g = g_ref[0] & 3
    rows, cols = base.shape
    regs = cols // LANES + 1
    per = rows // SUB
    ext = per + 2
    lane = lane_iota()
    ocean_first = (outer.shape[0] // SUB - 2 * per) - NOC * per
    clear_ends((g_s, gx_s), ext)
    for j in range(ext):

        def field(i, ref):
            if j == 0 or j == ext - 1:
                n = 2 * NICE + i
                late = g == (1 if j == 0 else 2)
                pairs = zip(late_tile(rd, n, lane, j == 0), low_high(g, ra, rc, nx, n, lane, j == 0))
                return [jnp.where(late, x, y) for x, y in pairs]
            return split(ref[tile(j - 1), :]) + [outer[tile(ocean_first + i * per + j - 1), :]]

        for c, (b, depth, x) in enumerate(zip(field(0, base), field(1, gf), field(2, x0))):
            b_s[c, at(j), :] = b
            g_s[c, at(j), :] = depth
            gx_s[c, at(j), :] = depth * x
            x_s[c, at(j), :] = x
    for j in range(ext):
        around, products = neighbour_sums(g_s, j, lane), neighbour_sums(gx_s, j, lane)
        for c in range(regs):
            depth = g_s[c, at(j), :]
            diag = DAMP + depth * around[c]
            invd[c, at(j), :] = 1.0 / diag
            known = jnp.where(depth > 0.0, b_s[c, at(j), :], 0.0)
            ra_out[c, at(j), :] = known - (diag * x_s[c, at(j), :] - depth * products[c])


def ocean_basis(g_ref, gw, invd, ra, r1, r2, r3, mine, y0_out, y1_out, y2_out, sums,
                sp, u0_s, u1_s, u2_s):
    g = g_ref[0] & 3
    regs = gw.shape[0]
    ext = gw.shape[1] // SUB - 2
    inner = regs - 1
    slab = (gw.shape[1] // SUB - 4) // 4
    row = row_iota(LANES)
    lane = lane_iota()
    zero = jnp.zeros((SUB, LANES), F32)
    clear_ends((u0_s, u1_s, u2_s), ext)

    def strip(ref, k):
        def spot(c):
            return ref[tile(slab + c // inner), c % inner * LANES : (c % inner + 1) * LANES]

        edge = wide_outer(spot(k // WIDE_SLOTS), k % WIDE_SLOTS, lane)
        if k < slab:
            return split(ref[tile(k), :]) + [edge]
        below = spot(-(-(slab + 1) // WIDE_SLOTS))
        return [jnp.where(row == 0, pltpu.roll(below, SUB - c, 0) if c else below, 0.0) for c in range(inner)] + [edge]

    def put(j, values):
        for c in range(regs):
            sp[c, at(j), :] = values[c]

    def clear(which):
        for j in which:
            put(j, [zero] * regs)

    def whole(slabs):
        clear([0])
        over = None
        for k, ref in enumerate(slabs):
            values = [strip(ref, t) for t in range(slab + 1)]
            for t in range(slab):
                value = values[t]
                if t == 0 and over is not None:
                    value = [x + y for x, y in zip(value, over)]
                put(1 + slab * k + t, value)
            over = values[slab]
        put(1 + slab * len(slabs), over)

    @pl.when(g == 0)
    def _():
        whole([mine, r1, r2, r3])

    @pl.when(g == 3)
    def _():
        whole([r3, r2, r1, mine])

    @pl.when(g == 1)
    def _():
        clear(range(2, ext))
        put(0, strip(r2, slab - 1))
        put(1, strip(r2, slab))

    @pl.when(g == 2)
    def _():
        clear(range(ext - 1))
        put(ext - 1, strip(r2, 0))

    acc = [[zero] * (regs - 1) for _ in range(6)]

    def add(k, c, left, right):
        acc[k][c] = acc[k][c] + left * right

    for j in range(ext):
        inside = 0 < j < ext - 1
        for c in range(regs):
            depth = gw[c, at(j), :]
            r0 = ra[c, at(j), :] + jnp.where(depth > 0.0, sp[c, at(j), :], 0.0)
            y0 = r0 * invd[c, at(j), :]
            u0_s[c, at(j), :] = depth * y0
            if inside and c + 1 < regs:
                y0_out[c, tile(j - 1), :] = y0
                add(0, c, r0, y0)
    for level, (source, target, before, here) in enumerate(
        ((u0_s, u1_s, y0_out, y1_out), (u1_s, u2_s, y1_out, y2_out))
    ):
        for j in range(ext):
            inside = 0 < j < ext - 1
            around = neighbour_sums(source, j, lane)
            for c in range(regs):
                depth = gw[c, at(j), :]
                w = depth * around[c]
                y = w * invd[c, at(j), :]
                target[c, at(j), :] = depth * y
                if inside and c + 1 < regs:
                    here[c, tile(j - 1), :] = y
                    add(2 * level + 1, c, before[c, tile(j - 1), :], w)
                    add(2 * level + 2, c, w, y)
    for j in range(1, ext - 1):
        around = neighbour_sums(u2_s, j, lane)
        for c in range(regs - 1):
            add(5, c, u2_s[c, at(j), :], around[c])
    lane_sums = []
    for k in range(6):
        total = acc[k][0]
        for c in range(1, regs - 1):
            total = total + acc[k][c]
        lane_sums.append(jnp.sum(total, axis=0, keepdims=True))
    stacked = jnp.concatenate(lane_sums + [jnp.zeros((2, LANES), F32)], axis=0)
    each = jnp.broadcast_to(jnp.sum(stacked, axis=1, keepdims=True), (SUB, LANES))
    sums[...] = jnp.sum(jnp.where(lane == row_iota(LANES), each, 0.0), axis=0, keepdims=True)


def combine(g_ref, parts, x0, y0, y1, y2, out):
    total = jnp.broadcast_to(jnp.sum(parts[...], axis=0), (SUB, LANES))
    lane = lane_iota()
    m = [
        jnp.broadcast_to(jnp.sum(jnp.where(lane == k, total, 0.0), axis=1, keepdims=True), (SUB, LANES))
        for k in range(6)
    ]

    def dot(left, right, image):
        value = None
        for i, a in enumerate(left):
            for j, b in enumerate(right):
                moment = m[i + j] - m[i + j + 1] if image else m[i + j]
                term = a * b * moment
                value = term if value is None else value + term
        return value

    z = [jnp.ones((SUB, LANES), F32)]
    p = z
    rz = m[0]
    coef = [0.0, 0.0, 0.0]
    for step in range(ITERS):
        alpha = rz / dot(p, p, True)
        for i, a in enumerate(p):
            coef[i] = coef[i] + alpha * a
        if step + 1 < ITERS:
            image = [a for a in p] + [jnp.zeros((SUB, LANES), F32)]
            for i, a in enumerate(p):
                image[i + 1] = image[i + 1] - a
            z = [(z[i] if i < len(z) else 0.0) - alpha * image[i] for i in range(len(image))]
            fresh = dot(z, z, False)
            beta = fresh / rz
            p = [z[i] + beta * p[i] if i < len(p) else z[i] for i in range(len(z))]
            rz = fresh
    for k in range(x0.shape[0] // SUB):
        t = tile(k)
        for c in range(y0.shape[0]):
            cut = slice(c * LANES, (c + 1) * LANES)
            move = coef[0] * y0[c, t, :] + coef[1] * y1[c, t, :] + coef[2] * y2[c, t, :]
            out[t, cut] = x0[t, cut] + move


def shards(
    base_rhs,
    depth,
    ssh_prev,
    currents,
    land_blocks,
    ice_thick,
    ice_blocks,
    ice_vel,
    ice_stress,
    wind,
):
    groups = lax.axis_size("grp")
    tiles = lax.axis_size("tile")
    assert groups == 4
    assert tiles % 2 == 0
    g = (lax.axis_index("grp") + groups * (lax.axis_index("tile") & 1)).astype(jnp.int32).reshape(1)
    rows, cols = base_rhs.shape
    ice_rows = ice_thick.shape[1]
    assert rows == groups * ice_rows
    slab = ice_rows + 2 * SUB
    strip = (2 * slab, cols)
    c, a, b, token = call(
        pack_rows,
        [(2 * (ice_rows + SUB), cols), strip, strip, (SUB, LANES)],
        [g, base_rhs, depth, ssh_prev, currents, land_blocks, ice_thick, ice_blocks, ice_vel, ice_stress, wind],
        scratch=[
            (2, 2, SUB, cols), (2, 2, SUB, cols),
            (land_blocks.shape, jnp.int32), (ice_blocks.shape, jnp.int32),
        ],
        sems=48,
        hbm=True,
    )
    rc = lax.ppermute(c, "grp", DIAGONAL)
    ra = lax.ppermute(a, "grp", FIRST)
    rb = lax.ppermute(b, "grp", SECOND)

    own = sum(own_count(rows, ice_rows))
    packed = (-(-own // SLOTS) * SUB, LANES)
    gf, h, inner, cross = call(
        pack_own,
        [(rows, cols), (2, ice_rows, cols), packed, packed],
        [g, token, base_rhs, depth, ssh_prev, currents, land_blocks, ice_thick, ice_blocks, ice_vel, ice_stress,
         wind],
    )
    inner = lax.ppermute(inner, "tile", [(i, i ^ 1) for i in range(tiles)])
    odd = range(1, tiles - 1, 2)
    cross = lax.ppermute(cross, "tile", [(i, i + 1) for i in odd] + [(i + 1, i) for i in odd])
    strip_tiles = 2 * (slab // SUB)
    narrow_rows = -(-strip_tiles // WIDE_SLOTS) * SUB
    tail = -(-narrow_rows * LANES // (SUB * cols)) * SUB
    outer, narrow, d = call(
        pack_narrow,
        [(own * SUB, LANES), (groups, narrow_rows, LANES), ((2 * NICE + 2) * SUB + tail, cols)],
        [g, inner, cross, h, gf, base_rhs, ssh_prev, ice_vel, ice_stress, wind],
    )
    nx = lax.all_to_all(narrow, "grp", 0, 0, tiled=True)
    d, nx = lax.optimization_barrier((d, nx))
    rd = lax.ppermute(d, "grp", FIRST)

    regs = cols // LANES + 1
    back = (ice_rows + tail_regs(ice_rows // SUB, regs - 1) // (regs - 1) * SUB, cols)
    held = (2, regs, slab + 2 * SUB, LANES)
    *state, p3, p2, p1, mine, kept = call(
        ice_steps,
        [held] * 5 + [back] * 4 + [(2, 2, regs, SUB, LANES)],
        [g, ra, rb, rc, nx, outer, h, ice_vel, ice_stress, wind, currents],
        scratch=[held] * 11,
        mib=32,
        flops=20000000,
    )
    p2, p1, fixed = call(
        ice_late,
        [back, back, (2, 5, SUB, cols)],
        [g, rd, ra, rb, nx, outer, h, ice_vel, ice_stress, wind, kept, p2, p1],
        scratch=[(2, regs, 5 * SUB, LANES)] * 16,
        flops=20000000,
    )
    r3 = lax.ppermute(p3, "grp", [(3, 0), (0, 3)])
    r2 = lax.ppermute(p2, "grp", SECOND)
    r1 = lax.ppermute(p1, "grp", FIRST)
    velocity, stress = call(ice_results, [ice_vel.shape, ice_stress.shape], [g, *state, fixed], flops=10000000)

    field = (regs, rows + 4 * SUB, LANES)
    gw, invd, known = call(
        ocean_before,
        [field] * 3,
        [g, ra, rc, rd, nx, outer, base_rhs, gf, ssh_prev],
        scratch=[field] * 3,
        flops=20000000,
    )
    y0, y1, y2, sums = call(
        ocean_basis,
        [(regs - 1, rows, LANES)] * 3 + [(1, LANES)],
        [g, gw, invd, known, r1, r2, r3, mine],
        scratch=[field] * 4,
    )
    devices = groups * tiles
    shared = lax.all_to_all(
        jnp.broadcast_to(sums[None], (devices, 1, LANES)), ("grp", "tile"), 0, 0, tiled=True
    )
    (ssh,) = call(combine, [(rows, cols)], [g, shared, ssh_prev, y0, y1, y2])
    return ssh, velocity, stress


def solution(mesh):
    return jax.shard_map(
        shards,
        mesh=mesh,
        in_specs=(
            P("grp", "tile"),
            P("grp", "tile"),
            P("grp", "tile"),
            P(None, "grp", "tile"),
            P("grp", "tile"),
            P(None, "grp", "tile"),
            P(None, "grp", "tile"),
            P(None, None, "grp", "tile"),
            P(None, None, "grp", "tile"),
            P(None, None, "grp", "tile"),
        ),
        out_specs=(P("grp", "tile"), P(None, None, "grp", "tile"), P(None, None, "grp", "tile")),
        check_vma=False,
    )
```
